32 devices in a mesh: rep: 16 (over z, y, core), shard: 2 (over x).
Axes of the slice: x: 2, y: 2, z: 4, core: 2. Of those that a mesh axis runs over, the one named last changes fastest.
Arguments:
- tokens: bfloat16 [32768, 768], P(('rep', 'shard')), may hold values from -6 to 6
- routes: int32 [32768, 2], P(('rep', 'shard')), may hold values from 0 to 3, all different within a row; in each aligned block of 1024 rows (0 to 1023, 1024 to 2047, ...) at most 640 rows name the same one
- pic_block: int32 [32], P(('rep', 'shard')), may hold values from 0 to 3
- norm1_gain: bfloat16 [768], P('shard'), may hold values from 0.099609375 to 1.8984375
- w_query: bfloat16 [768, 768], P('shard'), may hold values from -0.21875 to 0.21875
- w_key: bfloat16 [768, 768], P('shard'), may hold values from -0.21875 to 0.21875
- w_value: bfloat16 [768, 768], P('shard'), may hold values from -0.21875 to 0.21875
- w_out: bfloat16 [768, 768], P('shard'), may hold values from -0.875 to 0.875
- norm2_gain: bfloat16 [768], P('shard'), may hold values from 0.099609375 to 1.8984375
- router: bfloat16 [768, 4], P('shard'), may hold values from -0.21875 to 0.21875
- expert_gate: bfloat16 [4, 768, 2048], P(None, 'shard'), may hold values from -0.21875 to 0.21875
- expert_up: bfloat16 [4, 768, 2048], P(None, 'shard'), may hold values from -0.21875 to 0.21875
- expert_down: bfloat16 [4, 2048, 768], P(None, 'shard'), may hold values from -0.125 to 0.125
- shared_gate: bfloat16 [768, 2048], P('shard'), may hold values from -0.21875 to 0.21875
- shared_up: bfloat16 [768, 2048], P('shard'), may hold values from -0.21875 to 0.21875
- shared_down: bfloat16 [2048, 768], P('shard'), may hold values from -0.125 to 0.125
- cotangent: bfloat16 [32768, 768], P(('rep', 'shard')), may hold values from -6 to 6
Outputs:
- output: bfloat16 [32768, 768], P(('rep', 'shard'))
- input_grad: float32 [32768, 768], P(('rep', 'shard'))
- grad_norm1_gain: float32 [768], P('shard')
- grad_w_query: float32 [768, 768], P('shard')
- grad_w_key: float32 [768, 768], P('shard')
- grad_w_value: float32 [768, 768], P('shard')
- grad_w_out: float32 [768, 768], P('shard')
- grad_norm2_gain: float32 [768], P('shard')
- grad_router: float32 [768, 4], P('shard')
- grad_expert_gate: float32 [4, 768, 2048], P(None, 'shard')
- grad_expert_up: float32 [4, 768, 2048], P(None, 'shard')
- grad_expert_down: float32 [4, 2048, 768], P(None, 'shard')
- grad_shared_gate: float32 [768, 2048], P('shard')
- grad_shared_up: float32 [768, 2048], P('shard')
- grad_shared_down: float32 [2048, 768], P('shard')
The draws below stay inside these ranges and needn't reach their ends.
Inputs may be any that keep to these rules, and one draw needn't show every extreme that they name: `routes`: each row names two different experts; among the 1024 rows of one device no expert is named by more than 640 rows, and in every draw some expert is named by exactly 640 rows of some device.
All inputs are finite; a program needn't handle non-finite values.
Results may differ from the reference program's by a relative error of at most 0.015.
Values may be sent and summed in bfloat16 or wider, within the bound.
No kernel may reach another device: no remote copies, remote signals or barrier semaphores. Data moves between devices by JAX's collectives and lax.ppermute only.
A program may use at most 768 MiB of HBM per device.

```python
import math
import jax
import jax.numpy as jnp
import numpy as np
from jax import lax

D = 768
HEADS = 12
HEAD_DIM = 64
FF = 2048
EXPERTS = 4
TOP = 2
SEQ_LEN = 1024
PIC = 256
TOK_DEV = 1024
CAP = 640
SEQS = 32
TOKENS = 32768


def place_ends(result, own_key, smallest, high):
    extent = result.shape
    place = [jax.random.randint(jax.random.fold_in(own_key, axis), (), 0, extent[axis]) for axis in range(len(extent))]
    result = result.at[tuple(place)].set(smallest)
    longest = extent.index(max(extent))
    place[longest] = (place[longest] + 1) % extent[longest]
    return result.at[tuple(place)].set(high)


def spiked(entries, stream_key, source, target, blocks, factor):
    owner, partner = [(jnp.arange(entries.shape[dim]) // (entries.shape[dim] // blocks)).reshape([-1 if axis == dim else 1 for axis in range(entries.ndim)]) for dim in (source, target)]
    chosen = jax.random.permutation(stream_key, blocks)[partner]
    strong = (owner == chosen) | (owner == (partner + blocks // 2) % blocks)
    return jnp.where(strong, factor * entries, entries)


def steps_of(own_key, extent, shards, low, top_value):
    gain = 1.0
    for dim, parts in shards:
        draws = jax.random.uniform(jax.random.fold_in(jax.random.fold_in(own_key, 6), dim), (parts,), jnp.float32, low / len(shards), top_value / len(shards))
        gain = gain * jnp.repeat(jnp.exp(draws), extent[dim] // parts).reshape((-1,) + (1,) * (len(extent) - 1 - dim))
    return gain


def routed_block(own_key, own, number, rows, amount, top, limit, slope):
    sequence = jax.random.permutation(own_key, amount)
    crowded, common = portions_of(amount, rows * top, limit, slope, True), portions_of(amount, rows * top, limit, slope, False)
    places = jnp.arange(amount)

    def named(tallies, rotation):
        used = int((tallies > 0).sum())
        fixed = max(1, used // 4)
        shifted = fixed + (places - fixed + rotation * (used - fixed)) % max(1, amount - fixed)
        return jnp.zeros((amount,), jnp.int32).at[sequence[jnp.where(places < fixed, places, shifted)]].set(jnp.asarray(tallies, jnp.int32))

    tallies = jnp.where(number % 4 == 0, named(crowded, number // 4), named(common, number - number // 4 - 1))
    mixed = jax.random.permutation(jax.random.fold_in(own, 3), amount)
    source_of, taker = mixed[0:amount // 2 * 2:2], mixed[1:amount // 2 * 2:2]
    room = jnp.minimum(tallies[source_of] - 1, limit - tallies[taker]) // 2
    room = jnp.where((source_of == sequence[0]) | (taker == sequence[0]) | (tallies[taker] == 0), 0, jnp.maximum(room, 0))
    shifted = jax.random.randint(jax.random.fold_in(own, 4), (amount // 2,), 0, 1 << 20) % (room + 1)
    tallies = tallies.at[source_of].add(-shifted).at[taker].add(shifted)
    members = jnp.searchsorted(jnp.cumsum(tallies), jnp.arange(rows * top), side="right").astype(jnp.int32)
    table = members.reshape(top, rows).T
    table = table[jax.random.permutation(jax.random.fold_in(own, 1), rows)]
    rotation = jax.random.randint(jax.random.fold_in(own, 2), (rows, 1), 0, top)
    return jnp.take_along_axis(table, (jnp.arange(top)[None, :] + rotation) % top, axis=1)


def portions_of(number_of, total, most, slope, full):
    portions = [(1 << 20) // math.isqrt(rank ** slope) + 1 for rank in range(1, number_of + 1)]
    largest = most if full else min(most, max(-(-total // number_of), total * portions[0] // sum(portions)))
    least = 1 if total - largest >= number_of - 1 else 0
    counts, rest = [largest] + [least] * (number_of - 1), total - largest - least * (number_of - 1)
    while rest > 0:
        candidates = [i for i in range(1, number_of) if counts[i] < largest] or [i for i in range(1, number_of) if counts[i] < most]
        mass, remaining = sum([portions[i] for i in candidates]), rest
        for i in candidates:
            extra = min(most - counts[i], max(1, remaining * portions[i] // mass), rest)
            counts[i] = counts[i] + extra
            rest = rest - extra
    return np.array(counts)


def centred(key, shape, width, most, pieces=(), held_as=jnp.bfloat16):
    entries = jax.random.normal(key, shape, jnp.float32) * width
    if len(pieces) > 0:
        entries = steps_of(key, shape, pieces, -0.22, 0.18) * entries
    return jnp.clip(entries, min=-most, max=most).astype(held_as)


def bell_draw_with(rng, shape, spread, bound, shards, heavy, held_as=jnp.bfloat16):
    result = spread * jax.random.normal(rng, shape, jnp.float32)
    if shards:
        result = result * steps_of(rng, shape, shards, -0.22, 0.18)
    return jnp.clip(spiked(result, jax.random.fold_in(rng, 3), *heavy), -bound, bound).astype(held_as)


def setup_inputs(seed: int = 0) -> dict:
    key_list = jax.random.split(jax.random.key(seed), 18)
    tokens = centred(key_list[0], (TOKENS, D), 1.0, 6.0, ((0, 32),))
    routes_keys = jax.random.split(jax.random.fold_in(key_list[1], 1), TOKENS // TOK_DEV)
    routes_turns = jax.random.permutation(jax.random.fold_in(key_list[1], 3), TOKENS // TOK_DEV)
    routes = jax.vmap(lambda own, number: routed_block(jax.random.fold_in(key_list[1], 2), own, number, TOK_DEV, EXPERTS, TOP, CAP, 1))(routes_keys, routes_turns).reshape((TOKENS, TOP))
    pic_block = place_ends(jax.random.randint(key_list[2], (SEQS,), 0, SEQ_LEN // PIC), jax.random.fold_in(key_list[2], 1), 0, (SEQ_LEN // PIC) - 1).astype(jnp.int32)
    norm1_gain = jnp.clip(1.0 + 0.18 * jax.random.normal(key_list[3], (D,), jnp.float32), 0.099609375, 1.8984375).astype(jnp.bfloat16)
    w_query = centred(key_list[4], (D, D), D ** -0.5, 0.21875, ((0, 2),))
    w_key = centred(key_list[5], (D, D), D ** -0.5, 0.21875, ((0, 2),))
    w_value = centred(key_list[6], (D, D), D ** -0.5, 0.21875, ((0, 2),))
    w_out = centred(key_list[7], (D, D), (D // 16) ** -0.5, 0.875, ((0, 2),))
    norm2_gain = jnp.clip(1.0 + 0.18 * jax.random.normal(key_list[8], (D,), jnp.float32), 0.099609375, 1.8984375).astype(jnp.bfloat16)
    router = centred(key_list[9], (D, EXPERTS), D ** -0.5, 0.21875, ((0, 2),))
    expert_gate = centred(key_list[10], (EXPERTS, D, FF), D ** -0.5, 0.21875, ((1, 2),))
    expert_up = centred(key_list[11], (EXPERTS, D, FF), D ** -0.5, 0.21875, ((1, 2),))
    expert_down = centred(key_list[12], (EXPERTS, FF, D), FF ** -0.5, 0.125, ((1, 2),))
    shared_gate = centred(key_list[13], (D, FF), D ** -0.5, 0.21875, ((0, 2),))
    shared_up = centred(key_list[14], (D, FF), D ** -0.5, 0.21875, ((0, 2),))
    shared_down = centred(key_list[15], (FF, D), FF ** -0.5, 0.125, ((0, 2),))
    cotangent = bell_draw_with(key_list[16], (TOKENS, D), 1.0, 6.0, ((0, 32),), (0, 1, 32, 2.75))
    return dict(tokens=tokens, routes=routes, pic_block=pic_block, norm1_gain=norm1_gain, w_query=w_query, w_key=w_key, w_value=w_value, w_out=w_out, norm2_gain=norm2_gain, router=router, expert_gate=expert_gate, expert_up=expert_up, expert_down=expert_down, shared_gate=shared_gate, shared_up=shared_up, shared_down=shared_down, cotangent=cotangent)


@jax.custom_vjp
def low(v):
    return lax.optimization_barrier(v.astype(jnp.bfloat16)).astype(jnp.float32)

@jax.custom_vjp
def low_back(v):
    return v

def low_keep(v):
    return (low(v), None)

def low_pass(kept, grad):
    return (grad,)

def back_keep(v):
    return (v, None)

def back_low(kept, grad):
    return (low(grad),)
low.defvjp(low_keep, low_pass)
low_back.defvjp(back_keep, back_low)

def matmul(left, right):
    return jnp.dot(left, right, precision=lax.Precision.HIGHEST)

def rotary_tables(length, head_dim):
    halfway = head_dim // 2
    freqs_base = 10000.0 ** (-jnp.arange(halfway, dtype=jnp.float32) / halfway)
    angles = jnp.arange(length, dtype=jnp.float32)[:, None] * freqs_base[None, :]
    cosine_table = jnp.concatenate([jnp.cos(angles), jnp.cos(angles)], axis=1)
    sine_table = jnp.concatenate([jnp.sin(angles), jnp.sin(angles)], axis=1)
    return (cosine_table, sine_table)

def turn_half(values):
    halfway = values.shape[-1] // 2
    return jnp.concatenate([-values[..., halfway:], values[..., :halfway]], axis=-1)

def rotate(values, cosine_table, sine_table):
    return values * cosine_table[:, None, :] + turn_half(values) * sine_table[:, None, :]

def allowed_mask(row_start, block_rows, length, picture_block):
    position = jnp.arange(length)
    row_ids = row_start + jnp.arange(block_rows)
    in_picture = position // PIC == picture_block
    row_picture = row_ids // PIC == picture_block
    return (position[None, :] <= row_ids[:, None]) | row_picture[:, None] & in_picture[None, :]

def layer_sequence(inputs, route, picture_block, params):
    gain_first, query_full, key_full, value_full, out_full, gain_second, router_full, gate_full, up_full, down_full, common_gate, common_up, common_down = params
    length = inputs.shape[0]
    inv_one = lax.rsqrt(lax.optimization_barrier(jnp.mean(inputs * inputs, axis=-1, keepdims=True)) + 1e-05)
    normed_one = low(inputs * inv_one * gain_first)
    cosine_table, sine_table = rotary_tables(length, HEAD_DIM)
    query = low(rotate(low_back(matmul(normed_one, query_full)).reshape(length, HEADS, HEAD_DIM), cosine_table, sine_table))
    keys = low(rotate(low_back(matmul(normed_one, key_full)).reshape(length, HEADS, HEAD_DIM), cosine_table, sine_table))
    values = low(low_back(matmul(normed_one, value_full))).reshape(length, HEADS, HEAD_DIM)
    scores = low_back(jnp.einsum('qhd,khd->hqk', query, keys, precision=lax.Precision.HIGHEST)) * 0.125
    allowed = allowed_mask(0, length, length, picture_block)
    scores = jnp.where(allowed[None], scores, -1e+30)
    probs = low(jax.nn.softmax(scores, axis=-1))
    mixed = jnp.einsum('hqk,khd->qhd', probs, values, precision=lax.Precision.HIGHEST).reshape(length, D)
    mixed = low(low_back(mixed))
    resid = inputs + low_back(matmul(mixed, out_full))
    inv_two = lax.rsqrt(lax.optimization_barrier(jnp.mean(resid * resid, axis=-1, keepdims=True)) + 1e-05)
    normed_two = low(resid * inv_two * gain_second)
    logits = low_back(matmul(normed_two, router_full))
    picked = route[:, :, None] == jnp.arange(EXPERTS)[None, None, :]
    chosen = lax.optimization_barrier(jnp.sum(jnp.where(picked, logits[:, None, :], 0.0), axis=-1))
    gates = jax.nn.softmax(chosen, axis=-1)
    combine = lax.optimization_barrier(jnp.sum(jnp.where(picked, gates[:, :, None], 0.0), axis=1))
    total = resid
    for expert_index in range(EXPERTS):
        gate_pre = low_back(matmul(normed_two, gate_full[expert_index]))
        up_pre = low_back(matmul(normed_two, up_full[expert_index]))
        hidden = low(jax.nn.silu(gate_pre) * up_pre)
        expert_out = low_back(matmul(hidden, down_full[expert_index]))
        total = total + combine[:, expert_index:expert_index + 1] * expert_out
    common_gate_pre = low_back(matmul(normed_two, common_gate))
    common_up_pre = low_back(matmul(normed_two, common_up))
    common_hid = low(jax.nn.silu(common_gate_pre) * common_up_pre)
    total = total + low_back(matmul(common_hid, common_down))
    return total

def reference(tokens, routes, pic_block, norm1_gain, w_query, w_key, w_value, w_out, norm2_gain, router, expert_gate, expert_up, expert_down, shared_gate, shared_up, shared_down, cotangent):
    params = tuple((weight.astype(jnp.float32) for weight in (norm1_gain, w_query, w_key, w_value, w_out, norm2_gain, router, expert_gate, expert_up, expert_down, shared_gate, shared_up, shared_down)))
    inputs = tokens.astype(jnp.float32).reshape(SEQS, SEQ_LEN, D)
    seq_routes = routes.reshape(SEQS, SEQ_LEN, TOP)
    layer_step = jax.checkpoint(layer_sequence)

    def forward(inputs_all, params_all):

        def scan_step(carried, scan_item):
            return (carried, layer_step(scan_item[0], scan_item[1], scan_item[2], params_all))
        unused, outputs = lax.scan(scan_step, None, (inputs_all, seq_routes, pic_block))
        return outputs
    outputs, pullback = jax.vjp(forward, inputs, params)
    grad_inputs, grad_params = pullback(cotangent.astype(jnp.float32).reshape(SEQS, SEQ_LEN, D))
    return (outputs.reshape(TOKENS, D).astype(jnp.bfloat16), grad_inputs.reshape(TOKENS, D), grad_params[0], grad_params[1], grad_params[2], grad_params[3], grad_params[4], grad_params[5], grad_params[6], grad_params[7], grad_params[8], grad_params[9], grad_params[10], grad_params[11], grad_params[12])
```

```python
import functools

import jax
import jax.numpy as jnp
from jax import lax
from jax.experimental import pallas as pl
from jax.experimental.pallas import tpu as pltpu
from jax.sharding import PartitionSpec as P

D = 768
HEADS = 12
HEAD_DIM = 64
PIC = 256
CAP = 640
PAIR = 2 * HEAD_DIM
PAIRS = HEADS // 2
QB = 256
EPS = 1e-05
BF = jnp.bfloat16
F32 = jnp.float32
ALL = ("rep", "shard")
MIB = 1 << 20


def nn(a, b):
    return lax.dot_general(a, b, (((1,), (0,)), ((), ())), preferred_element_type=F32)


def nt(a, b):
    return lax.dot_general(a, b, (((1,), (1,)), ((), ())), preferred_element_type=F32)


def resident(shape):
    zeros = (0,) * len(shape)
    return pl.BlockSpec(shape, lambda *_: zeros, pipeline_mode=pl.Buffered(1))


def rotary_tables(length):
    halfway = HEAD_DIM // 2
    freqs_base = 10000.0 ** (-jnp.arange(halfway, dtype=F32) / halfway)
    angles = jnp.arange(length, dtype=F32)[:, None] * freqs_base[None, :]
    cosine = jnp.cos(angles)
    sine = jnp.sin(angles)
    zero = jnp.zeros_like(sine)
    cos_t = jnp.concatenate([cosine] * 4, axis=1)
    left = jnp.concatenate([-sine, zero, -sine, zero], axis=1)
    right = jnp.concatenate([zero, sine, zero, sine], axis=1)
    return cos_t, left, right


def turned(v, left, right):
    return pltpu.roll(v, 96, 1) * left + pltpu.roll(v, 32, 1) * right


def head_masks(rows):
    lane = lax.broadcasted_iota(jnp.int32, (rows, PAIR), 1)
    return lane < HEAD_DIM, lane >= HEAD_DIM


def attend_forward_body(pic, tok, gain, wqkv, cos_t, left, right, q_o, k_o, v_o, mix_o, lse_o, xn):
    length = tok.shape[0]

    @pl.when(pl.program_id(0) == 0)
    def _():
        for lo in range(0, length, QB):
            x = tok[lo : lo + QB, :].astype(F32)
            inv = lax.rsqrt(jnp.mean(x * x, axis=1, keepdims=True) + EPS)
            xn[lo : lo + QB, :] = (x * inv * gain[...]).astype(BF)

    for lo in range(0, length, QB):
        rows = slice(lo, lo + QB)
        qkv = nn(xn[rows, :], wqkv[...])
        q, k = qkv[:, :PAIR], qkv[:, PAIR : 2 * PAIR]
        c_, l_, r_ = cos_t[rows, :], left[rows, :], right[rows, :]
        q_o[rows, :] = (q * c_ + turned(q, l_, r_)).astype(BF) * jnp.asarray(0.125, BF)
        k_o[rows, :] = (k * c_ + turned(k, l_, r_)).astype(BF)
        v_o[rows, :] = qkv[:, 2 * PAIR :].astype(BF)
    masks = head_masks(QB)
    row = lax.broadcasted_iota(jnp.int32, (QB, QB), 0)
    col = lax.broadcasted_iota(jnp.int32, (QB, QB), 1)
    causal = col <= row
    for block in range(length // QB):
        rows = slice(block * QB, (block + 1) * QB)
        allowed = causal | (pic[0] == block)
        q = q_o[rows, :]
        outs = []
        for head in range(2):
            qm = jnp.where(masks[head], q, jnp.zeros_like(q))
            s_d = jnp.where(allowed, nt(qm, k_o[rows, :]), -1e30)
            top = jnp.max(s_d, axis=1, keepdims=True)
            if block:
                s_o = nt(qm, k_o[: block * QB, :])
                top = jnp.maximum(top, jnp.max(s_o, axis=1, keepdims=True))
            p_d = jnp.exp(s_d - top)
            total = jnp.sum(p_d, axis=1, keepdims=True)
            acc = nn(p_d.astype(BF), v_o[rows, :])
            if block:
                p_o = jnp.exp(s_o - top)
                total = total + jnp.sum(p_o, axis=1, keepdims=True)
                acc = acc + nn(p_o.astype(BF), v_o[: block * QB, :])
            outs.append(acc / total)
            lse = jnp.broadcast_to(top + jnp.log(total), (QB, PAIR))
            lse_o[0, head : head + 1, rows] = jnp.transpose(lse)[0:1, :]
        mix_o[rows, :] = jnp.where(masks[0], outs[0], outs[1]).astype(BF)


def attend_forward(pic_block, tokens, gain, wqkv, tables):
    length = tokens.shape[0]
    pair = pl.BlockSpec((length, PAIR), lambda p: (0, p))
    wide = jax.ShapeDtypeStruct((length, D), BF)
    return pl.pallas_call(
        attend_forward_body,
        grid=(PAIRS,),
        in_specs=[
            pl.BlockSpec(memory_space=pltpu.SMEM),
            resident((length, D)),
            resident((1, D)),
            pl.BlockSpec((D, 3 * PAIR), lambda p: (0, p)),
            resident((length, PAIR)),
            resident((length, PAIR)),
            resident((length, PAIR)),
        ],
        out_specs=[pair, pair, pair, pair, pl.BlockSpec((1, 8, length), lambda p: (p, 0, 0))],
        out_shape=[wide, wide, wide, wide, jax.ShapeDtypeStruct((PAIRS, 8, length), F32)],
        scratch_shapes=[pltpu.VMEM((length, D), BF)],
        compiler_params=pltpu.CompilerParams(vmem_limit_bytes=48 * MIB),
        name="attend_forward",
    )(pic_block, tokens, gain, wqkv, *tables)


def attend_backward_body(
    pic, tok, gain, wqkv, wout, cos_t, left, right, q_i, k_i, v_i, mix_i, lse_i, dres, dres_f,
    gqkv_o, gout_o, igrad_o, ggain_o,
    xn_t, dxn, dmix, dqkv, dk_s, dv_s, k_t,
):
    length = tok.shape[0]
    step = pl.program_id(0)

    @pl.when(step == 0)
    def _():
        for lo in range(0, length, QB):
            x = tok[lo : lo + QB, :].astype(F32)
            inv = lax.rsqrt(jnp.mean(x * x, axis=1, keepdims=True) + EPS)
            xn_t[:, lo : lo + QB] = jnp.transpose((x * inv * gain[...]).astype(BF))

    dm = nt(dres[...], wout[...]).astype(BF)
    dmix[...] = dm
    mixed = mix_i[...]
    gout_o[...] = nn(jnp.transpose(mixed), dres[...]).astype(BF)
    prod = jnp.transpose(dm.astype(F32) * mixed.astype(F32))
    delta = (
        jnp.sum(prod[:HEAD_DIM, :], axis=0, keepdims=True),
        jnp.sum(prod[HEAD_DIM:, :], axis=0, keepdims=True),
    )
    k_t[...] = jnp.transpose(k_i[...])
    masks = head_masks(QB)
    key_row = lax.broadcasted_iota(jnp.int32, (QB, QB), 0)
    query_col = lax.broadcasted_iota(jnp.int32, (QB, QB), 1)
    causal = key_row <= query_col
    for block in reversed(range(length // QB)):
        rows = slice(block * QB, (block + 1) * QB)
        first = block == length // QB - 1
        allowed = causal | (pic[0] == block)
        q = q_i[rows, :]
        dm = dmix[rows, :]
        dq_t = []
        parts = {"d": [], "o": []}
        for head in range(2):
            qm = jnp.where(masks[head], q, jnp.zeros_like(q))
            dmm = jnp.where(masks[head], dm, jnp.zeros_like(dm))
            lse = lse_i[0, head : head + 1, rows]
            cent = delta[head][:, rows]
            half = slice(head * HEAD_DIM, (head + 1) * HEAD_DIM)
            dq = None
            for part, keys in (("d", rows), ("o", slice(0, block * QB))):
                if part == "o" and block == 0:
                    continue
                st = nt(k_i[keys, :], qm)
                pt = jnp.exp(st - lse)
                if part == "d":
                    pt = jnp.where(allowed, pt, 0.0)
                dpt = nt(v_i[keys, :], dmm)
                dst = (pt * (dpt - cent)).astype(BF)
                parts[part].append((nn(dst, qm), nn(pt.astype(BF), dmm)))
                add = nn(k_t[half, keys], dst)
                dq = add if dq is None else dq + add
            dq_t.append(dq)
        for part, keys in (("d", rows), ("o", slice(0, block * QB))):
            if not parts[part]:
                continue
            dk = parts[part][0][0] + parts[part][1][0]
            dv = parts[part][0][1] + parts[part][1][1]
            if first:
                dk_s[keys, :] = dk
                dv_s[keys, :] = dv
            else:
                dk_s[keys, :] = dk_s[keys, :] + dk
                dv_s[keys, :] = dv_s[keys, :] + dv
        dq = jnp.transpose(jnp.concatenate(dq_t, axis=0)) * 0.125
        c_, l_, r_ = cos_t[rows, :], left[rows, :], right[rows, :]
        dqkv[rows, :PAIR] = (dq * c_ - turned(dq, l_, r_)).astype(BF)
        dk = dk_s[rows, :]
        dqkv[rows, PAIR : 2 * PAIR] = (dk * c_ - turned(dk, l_, r_)).astype(BF)
        dqkv[rows, 2 * PAIR :] = dv_s[rows, :].astype(BF)
    gqkv_o[...] = nn(xn_t[...], dqkv[...]).astype(BF)
    add = nt(dqkv[...], wqkv[...])

    @pl.when(step == 0)
    def _():
        dxn[...] = add

    @pl.when(step > 0)
    def _():
        dxn[...] = dxn[...] + add

    @pl.when(step == PAIRS - 1)
    def _():
        total = jnp.zeros((1, D), F32)
        for lo in range(0, length, QB):
            rows = slice(lo, lo + QB)
            x = tok[rows, :].astype(F32)
            inv = lax.rsqrt(jnp.mean(x * x, axis=1, keepdims=True) + EPS)
            n = x * inv
            up = dxn[rows, :]
            total = total + jnp.sum(up * n, axis=0, keepdims=True)
            u = up * gain[...]
            igrad_o[rows, :] = dres_f[rows, :] + inv * (u - n * jnp.mean(u * n, axis=1, keepdims=True))
        ggain_o[...] = total


def attend_backward(pic_block, tokens, gain, wqkv, wout, tables, q, k, v, mixed, lse, dres, dres_f):
    length = tokens.shape[0]
    pair = pl.BlockSpec((length, PAIR), lambda p: (0, p))
    return pl.pallas_call(
        attend_backward_body,
        grid=(PAIRS,),
        in_specs=[
            pl.BlockSpec(memory_space=pltpu.SMEM),
            resident((length, D)),
            resident((1, D)),
            pl.BlockSpec((D, 3 * PAIR), lambda p: (0, p)),
            pl.BlockSpec((PAIR, D), lambda p: (p, 0)),
            resident((length, PAIR)),
            resident((length, PAIR)),
            resident((length, PAIR)),
            pair, pair, pair, pair,
            pl.BlockSpec((1, 8, length), lambda p: (p, 0, 0)),
            resident((length, D)),
            resident((length, D)),
        ],
        out_specs=[
            pl.BlockSpec((D, 3 * PAIR), lambda p: (0, p)),
            pl.BlockSpec((PAIR, D), lambda p: (p, 0)),
            resident((length, D)),
            resident((1, D)),
        ],
        out_shape=[
            jax.ShapeDtypeStruct((D, 3 * D), BF),
            jax.ShapeDtypeStruct((D, D), BF),
            jax.ShapeDtypeStruct((length, D), F32),
            jax.ShapeDtypeStruct((1, D), F32),
        ],
        scratch_shapes=[
            pltpu.VMEM((D, length), BF),
            pltpu.VMEM((length, D), F32),
            pltpu.VMEM((length, PAIR), BF),
            pltpu.VMEM((length, 3 * PAIR), BF),
            pltpu.VMEM((length, PAIR), F32),
            pltpu.VMEM((length, PAIR), F32),
            pltpu.VMEM((PAIR, length), BF),
        ],
        compiler_params=pltpu.CompilerParams(vmem_limit_bytes=56 * MIB),
        name="attend_backward",
    )(pic_block, tokens, gain, wqkv, wout, *tables, q, k, v, mixed, lse, dres, dres_f)


def middle_body(shard, tok, mixed, wout, gain, router_t, routes_t, resid_o, n2_o, n2p_o, comb_o):
    r = tok[...].astype(F32) + nn(mixed[...], wout[...])
    resid_o[...] = r
    inv = lax.rsqrt(jnp.mean(r * r, axis=1, keepdims=True) + EPS)
    n2 = (r * inv * gain[...]).astype(BF)
    n2_o[...] = n2
    half = D // 2
    swapped = jnp.concatenate([n2[:, half:], n2[:, :half]], axis=1)
    n2p_o[...] = jnp.where(shard[0] == 0, n2, swapped)
    logits = nt(router_t[...], n2)
    expert = lax.broadcasted_iota(jnp.int32, logits.shape, 0)
    picks = [expert == routes_t[k : k + 1, :] for k in range(2)]
    chosen = [jnp.sum(jnp.where(p, logits, 0.0), axis=0, keepdims=True) for p in picks]
    top = jnp.maximum(chosen[0], chosen[1])
    weights = [jnp.exp(v - top) for v in chosen]
    total = weights[0] + weights[1]
    gates = [w / total for w in weights]
    comb_o[...] = jnp.where(picks[0], gates[0], 0.0) + jnp.where(picks[1], gates[1], 0.0)


def middle(shard, tokens, mixed, wout, gain, router_t, routes_t):
    length = tokens.shape[0]
    block = 256
    rows = pl.BlockSpec((block, D), lambda i: (i, 0))
    cols = pl.BlockSpec((8, block), lambda i: (0, i))
    return pl.pallas_call(
        middle_body,
        grid=(length // block,),
        in_specs=[
            pl.BlockSpec(memory_space=pltpu.SMEM),
            rows,
            rows,
            resident((D, D)),
            resident((1, D)),
            resident((8, D)),
            cols,
        ],
        out_specs=[rows, rows, rows, cols],
        out_shape=[
            jax.ShapeDtypeStruct((length, D), F32),
            jax.ShapeDtypeStruct((length, D), BF),
            jax.ShapeDtypeStruct((length, D), BF),
            jax.ShapeDtypeStruct((8, length), F32),
        ],
        compiler_params=pltpu.CompilerParams(vmem_limit_bytes=40 * MIB),
        name="middle",
    )(shard, tokens, mixed, wout, gain, router_t, routes_t)


def join_body(shard, dy, resid, gain, dlog, router_t, *refs):
    outs, dxs = refs[:6], refs[6:12]
    out_o, dres_o, dlow_o, ggain_o = refs[12:]
    r = resid[...]
    total = r
    for part in outs:
        total = total + part[...].astype(F32)
    out_o[...] = total.astype(BF)
    up = dxs[0][...].astype(F32)
    for part in dxs[1:]:
        up = up + part[...].astype(F32)
    half = D // 2
    swapped = jnp.concatenate([up[:, half:], up[:, :half]], axis=1)
    up = jnp.where(shard[0] == 0, up, swapped)
    up = up + nn(dlog[...], router_t[...])
    inv = lax.rsqrt(jnp.mean(r * r, axis=1, keepdims=True) + EPS)
    n = r * inv
    add = jnp.sum(up * n, axis=0, keepdims=True)

    @pl.when(pl.program_id(0) == 0)
    def _():
        ggain_o[...] = add

    @pl.when(pl.program_id(0) > 0)
    def _():
        ggain_o[...] = ggain_o[...] + add

    u = up * gain[...]
    d = dy[...].astype(F32) + inv * (u - n * jnp.mean(u * n, axis=1, keepdims=True))
    dres_o[...] = d
    dlow_o[...] = d.astype(BF)


def join(shard, dy, resid, gain, dlog, router_t, outs, dxs):
    length = dy.shape[0]
    block = 256
    rows = pl.BlockSpec((block, D), lambda i: (i, 0))

    def part_spec(part):
        if part.ndim == 3:
            return pl.BlockSpec((None, block, D), lambda i: (0, i, 0))
        return rows

    return pl.pallas_call(
        join_body,
        grid=(length // block,),
        in_specs=[
            pl.BlockSpec(memory_space=pltpu.SMEM),
            rows,
            rows,
            resident((1, D)),
            pl.BlockSpec((block, 128), lambda i: (i, 0)),
            resident((128, D)),
        ]
        + [part_spec(p) for p in outs]
        + [part_spec(p) for p in dxs],
        out_specs=[rows, rows, rows, pl.BlockSpec((1, D), lambda i: (0, 0))],
        out_shape=[
            jax.ShapeDtypeStruct((length, D), BF),
            jax.ShapeDtypeStruct((length, D), F32),
            jax.ShapeDtypeStruct((length, D), BF),
            jax.ShapeDtypeStruct((1, D), F32),
        ],
        compiler_params=pltpu.CompilerParams(vmem_limit_bytes=40 * MIB),
        name="join",
    )(shard, dy, resid, gain, dlog, router_t, *outs, *dxs)


def ffn_body(routed, steps, chunk, where, tok, dy, *refs):
    if routed:
        slot_row, slot_col, gate_row = refs[:3]
        refs = refs[3:]
    g_own, g_oth, u_own, u_oth, d_own, d_oth = refs[:6]
    refs = refs[6:]
    out_o, dx_o = refs[:2]
    refs = refs[2:]
    if routed:
        dgate_o = refs[0]
        refs = refs[1:]
    kg_o, sg_o, ku_o, su_o, kd_o, sd_o = refs[:6]
    refs = refs[6:]
    wg, wu, wd, y_acc, dx_acc, hid_s, dg_s, du_s, x_t, de_t = refs[:10]
    refs = refs[10:]
    i = pl.program_id(0)
    srcs, length = tok.shape[0], tok.shape[1]
    rows_all = y_acc.shape[0]
    hold = rows_all // srcs
    half = D // 2
    if routed:
        x_s, de_s, dys, gate_s = refs
    tile = 128

    @pl.when(i == 0)
    def _():
        for src in range(srcs):
            if routed:
                for lo in range(0, hold, tile):
                    slot = lax.broadcasted_iota(jnp.int32, (tile, length), 0) + lo
                    mine = slot == slot_row[src : src + 1, :]
                    pick = jnp.where(mine, 1.0, 0.0).astype(BF)
                    rows = slice(src * hold + lo, src * hold + lo + tile)
                    x = nn(pick, tok[src]).astype(BF)
                    d_raw = nn(pick, dy[src])
                    gate = jnp.sum(jnp.where(mine, gate_row[src : src + 1, :], 0.0), axis=1, keepdims=True)
                    gate_s[rows, :] = jnp.broadcast_to(gate, (tile, 128))
                    d_e = (d_raw * gate).astype(BF)
                    x_s[rows, :] = x
                    dys[rows, :] = d_raw.astype(BF)
                    de_s[rows, :] = d_e
                    x_t[:, rows] = jnp.transpose(x)
                    de_t[:, rows] = jnp.transpose(d_e)
            else:
                for lo in range(0, hold, 256):
                    rows = slice(src * hold + lo, src * hold + lo + 256)
                    x_t[:, rows] = jnp.transpose(tok[src, lo : lo + 256, :])
                    de_t[:, rows] = jnp.transpose(dy[src, lo : lo + 256, :])

    wg[:half, :] = g_own[...]
    wg[half:, :] = g_oth[...]
    wu[:half, :] = u_own[...]
    wu[half:, :] = u_oth[...]

    @pl.when(i < steps // 2)
    def _():
        wd[...] = d_own[...]

    @pl.when(i >= steps // 2)
    def _():
        wd[...] = d_oth[...]

    def piece(j, first):
        rows = pl.ds(pl.multiple_of(j * chunk, chunk), chunk)
        if routed:
            x, de = x_s[rows, :], de_s[rows, :]
        else:
            per = length // chunk
            inner = pl.ds(pl.multiple_of((j % per) * chunk, chunk), chunk)
            x, de = tok[j // per, inner, :], dy[j // per, inner, :]
        g = nn(x, wg[...])
        u = nn(x, wu[...])
        dh = nt(de, wd[...])
        s = 1.0 / (1.0 + jnp.exp(-g))
        act = g * s
        hid = (act * u).astype(BF)
        du = (dh * act).astype(BF)
        dg = (dh * u * s * (1.0 + g * (1.0 - s))).astype(BF)
        hid_s[rows, :] = hid
        dg_s[rows, :] = dg
        du_s[rows, :] = du
        y = nn(hid, wd[...])
        dx = nt(dg, wg[...]) + nt(du, wu[...])
        if first:
            y_acc[rows, :] = y
            dx_acc[rows, :] = dx
        else:
            y_acc[rows, :] = y_acc[rows, :] + y
            dx_acc[rows, :] = dx_acc[rows, :] + dx

    @pl.when(i == 0)
    def _():
        @pl.loop(0, rows_all // chunk)
        def _(j):
            piece(j, True)

    @pl.when(i > 0)
    def _():
        @pl.loop(0, rows_all // chunk)
        def _(j):
            piece(j, False)

    gg = nn(x_t[...], dg_s[...])
    kg_o[...] = gg[:half, :].astype(BF)
    sg_o[...] = gg[half:, :].astype(BF)
    gu = nn(x_t[...], du_s[...])
    ku_o[...] = gu[:half, :].astype(BF)
    su_o[...] = gu[half:, :].astype(BF)
    gd = jnp.transpose(nn(de_t[...], hid_s[...])).astype(BF)

    @pl.when(i < steps // 2)
    def _():
        kd_o[...] = gd

    @pl.when(i >= steps // 2)
    def _():
        sd_o[...] = gd

    @pl.when(i == steps - 1)
    def _():
        for src in range(srcs):
            if routed:
                total = jnp.zeros((1, length), F32)
                for lo in range(0, hold, tile):
                    rows = slice(src * hold + lo, src * hold + lo + tile)
                    y = y_acc[rows, :]
                    dgate = jnp.sum(dys[rows, :].astype(F32) * y, axis=1, keepdims=True)
                    slot = lax.broadcasted_iota(jnp.int32, (tile, length), 0) + lo
                    mine = slot == slot_row[src : src + 1, :]
                    total = total + jnp.sum(jnp.where(mine, dgate, 0.0), axis=0, keepdims=True)
                    x_s[rows, :] = (y * gate_s[rows, 0:1]).astype(BF)
                    de_s[rows, :] = dx_acc[rows, :].astype(BF)
                dgate_o[src : src + 1, :] = total
                held = slice(src * hold, (src + 1) * hold)
                for lo in range(0, length, tile):
                    slot = lax.broadcasted_iota(jnp.int32, (tile, hold), 1)
                    mine = slot == slot_col[src * length + lo : src * length + lo + tile, :]
                    pick = jnp.where(mine, 1.0, 0.0).astype(BF)
                    out_o[src, lo : lo + tile, :] = nn(pick, x_s[held, :]).astype(BF)
                    dx_o[src, lo : lo + tile, :] = nn(pick, de_s[held, :]).astype(BF)
            else:
                held = slice(src * hold, (src + 1) * hold)
                out_o[src] = y_acc[held, :].astype(BF)
                dx_o[src] = dx_acc[held, :].astype(BF)


def ffn(where, tok, dy, gate, up, down, gate_oth, up_oth, down_oth, route=None):
    routed = route is not None
    srcs, length = tok.shape[0], tok.shape[1]
    block = 512
    half = D // 2
    if routed:
        total_cols = gate_oth.shape[1]
        steps = total_cols // block
        rows_all = srcs * CAP
        chunk = 256
    else:
        total_cols = gate_oth.shape[1]
        steps = total_cols // block
        rows_all = srcs * length
        chunk = 256
    per = steps // 2

    def compact(i, w):
        return jnp.where(i < per, w[0] * per + i, (1 - w[0]) * per + i - per)

    if routed:
        gate_spec = pl.BlockSpec((None, half, block), lambda i, w: (w[2], 0, compact(i, w)))
        down_spec = pl.BlockSpec((None, block, D), lambda i, w: (w[2], jnp.minimum(i, per - 1), 0))
    else:
        cores = gate.shape[1] // total_cols
        gate_spec = pl.BlockSpec((half, block), lambda i, w: (0, compact(i, w) * cores + w[1]))
        down_spec = pl.BlockSpec((block, D), lambda i, w: (w[1], 0))
    gate_oth_spec = pl.BlockSpec((half, block), lambda i, w: (0, compact(i, w)))
    first_half = pl.BlockSpec((block, D), lambda i, w: (jnp.minimum(i, per - 1), 0))
    last_half = pl.BlockSpec((block, D), lambda i, w: (jnp.maximum(i - per, 0), 0))
    in_specs = [resident((srcs, length, D)), resident((srcs, length, D))]
    operands = [tok, dy]
    if routed:
        slot_row, slot_col, gate_row = route
        in_specs += [resident(slot_row.shape), resident(slot_col.shape), resident(gate_row.shape)]
        operands += [slot_row, slot_col, gate_row]
    in_specs += [gate_spec, gate_oth_spec, gate_spec, gate_oth_spec, down_spec, last_half]
    operands += [gate, gate_oth, up, up_oth, down, down_oth]
    wide = jax.ShapeDtypeStruct((srcs, length, D), BF)
    out_specs = [resident((srcs, length, D)), resident((srcs, length, D))]
    out_shape = [wide, wide]
    if routed:
        out_specs.append(resident((srcs, length)))
        out_shape.append(jax.ShapeDtypeStruct((srcs, length), F32))
    col_grad = jax.ShapeDtypeStruct((half, total_cols), BF)
    row_grad = jax.ShapeDtypeStruct((total_cols // 2, D), BF)
    out_specs += [gate_oth_spec] * 4 + [first_half, last_half]
    out_shape += [col_grad] * 4 + [row_grad] * 2
    scratch = [
        pltpu.VMEM((D, block), BF),
        pltpu.VMEM((D, block), BF),
        pltpu.VMEM((block, D), BF),
        pltpu.VMEM((rows_all, D), F32),
        pltpu.VMEM((rows_all, D), F32),
        pltpu.VMEM((rows_all, block), BF),
        pltpu.VMEM((rows_all, block), BF),
        pltpu.VMEM((rows_all, block), BF),
        pltpu.VMEM((D, rows_all), BF),
        pltpu.VMEM((D, rows_all), BF),
    ]
    if routed:
        scratch += [
            pltpu.VMEM((rows_all, D), BF),
            pltpu.VMEM((rows_all, D), BF),
            pltpu.VMEM((rows_all, D), BF),
            pltpu.VMEM((rows_all, 128), F32),
        ]
    flops = 9 * 2 * rows_all * D * block * steps
    return pl.pallas_call(
        functools.partial(ffn_body, routed, steps, chunk),
        grid_spec=pltpu.PrefetchScalarGridSpec(
            num_scalar_prefetch=1,
            grid=(steps,),
            in_specs=in_specs,
            out_specs=out_specs,
            scratch_shapes=scratch,
        ),
        out_shape=out_shape,
        compiler_params=pltpu.CompilerParams(vmem_limit_bytes=60 * MIB),
        cost_estimate=pl.CostEstimate(flops=flops, transcendentals=0, bytes_accessed=20 * MIB),
        name="ffn_routed" if routed else "ffn_shared",
    )(where, *operands)


def on_device(
    tokens,
    routes,
    pic_block,
    norm1_gain,
    w_query,
    w_key,
    w_value,
    w_out,
    norm2_gain,
    router,
    expert_gate,
    expert_up,
    expert_down,
    shared_gate,
    shared_up,
    shared_down,
    cotangent,
):
    reps = lax.axis_size("rep")
    shards = lax.axis_size("shard")
    rep = lax.axis_index("rep")
    shard = lax.axis_index("shard")
    core = rep % 2
    length = tokens.shape[0]
    half = D // 2
    experts = router.shape[1]

    def swap(value, rep_bit, shard_bit):
        perm = [
            (r * shards + s, (r ^ rep_bit) * shards + (s ^ shard_bit))
            for r in range(reps)
            for s in range(shards)
        ]
        return lax.ppermute(value, ALL, perm)

    def over_core(value):
        return swap(value, 1, 0)

    def over_x(value):
        return swap(value, 0, 1)

    def in_order(index, mine, theirs, axis):
        return jnp.where(
            index == 0,
            jnp.concatenate([mine, theirs], axis=axis),
            jnp.concatenate([theirs, mine], axis=axis),
        )

    extra = jnp.concatenate([norm1_gain[:, None], norm2_gain[:, None], router], axis=1)
    extra = jnp.pad(extra, ((0, 0), (0, 256 - extra.shape[1])))
    small = jnp.concatenate([w_query, w_key, w_value, w_out, extra], axis=1)
    width = small.shape[1] // 2
    got = over_x(lax.dynamic_slice_in_dim(small, core * width, width, axis=1))
    small_oth = in_order(core, got, over_core(got), 1)
    small_full = in_order(shard, small, small_oth, 0)
    wqkv = small_full[:, : 3 * D].reshape(D, 3, PAIRS, PAIR).transpose(0, 2, 1, 3).reshape(D, 3 * D)
    wout = small_full[:, 3 * D : 4 * D]
    gain_one = small_full[:, 4 * D].astype(F32).reshape(1, D)
    gain_two = small_full[:, 4 * D + 1].astype(F32).reshape(1, D)
    router_t = jnp.transpose(small_full[:, 4 * D + 2 : 4 * D + 2 + experts])
    router_t8 = jnp.pad(router_t, ((0, 8 - experts), (0, 0)))
    router_t128 = jnp.pad(router_t, ((0, 128 - experts), (0, 0)))

    def later(value, after):
        return lax.optimization_barrier((value, after))[0]

    def shared_cols(weight):
        return jnp.concatenate(
            [
                lax.dynamic_slice_in_dim(weight, s * 1024 + core * 512, 512, axis=1)
                for s in range(shards)
            ],
            axis=1,
        )

    shared_send = [
        shared_cols(shared_gate),
        shared_cols(shared_up),
        lax.dynamic_slice_in_dim(shared_down, core * 512, 512, axis=0),
    ]
    shared_oth = [over_x(later(v, got)) for v in shared_send]
    per_core = experts // 2
    expert_oth = []
    previous = shared_oth[0]
    for j in range(per_core):
        sends = [
            lax.dynamic_index_in_dim(weight, core * per_core + j, 0, keepdims=False)
            for weight in (expert_gate, expert_up, expert_down)
        ]
        gots = [over_x(later(v, previous)) for v in sends]
        previous = gots[0]
        expert_oth.append(gots)

    def slot_tables(picks):
        expert_ids = jnp.arange(8)[:, None, None]
        picked = jnp.any(picks.T[None] == expert_ids, axis=1)
        earlier = jnp.arange(length)[:, None] < jnp.arange(length)[None, :]
        rank = jnp.dot(picked.astype(BF), earlier.astype(BF), preferred_element_type=F32)
        return jnp.where(picked, rank.astype(jnp.int32), -1)

    routes_oth = over_core(routes)
    slots = jnp.stack([slot_tables(routes), slot_tables(routes_oth)])
    dy_both = jnp.stack([cotangent, over_core(cotangent)])
    tables = rotary_tables(length)
    routes_t = jnp.pad(routes.T, ((0, 6), (0, 0)))

    q, k, v, mixed, lse = attend_forward(pic_block, tokens, gain_one, wqkv, tables)
    shard_s = shard.astype(jnp.int32).reshape(1)
    resid, n2, n2p, comb = middle(shard_s, tokens, mixed, wout, gain_two, router_t8, routes_t)
    n2_both = jnp.stack([n2p, over_core(n2p)])
    combs = jnp.stack([comb, over_core(comb)])

    def where_of(expert):
        return jnp.stack([shard, core, expert]).astype(jnp.int32)

    res = ffn(where_of(core), n2_both, dy_both, shared_gate, shared_up, shared_down, *shared_oth)
    outs, dxs, grads = [res[0]], [res[1]], [res[2:]]
    dgates = []
    for j in range(per_core):
        expert = core * per_core + j
        slot_row = lax.dynamic_index_in_dim(slots, expert, 1, keepdims=False)
        gate_row = lax.dynamic_index_in_dim(combs, expert, 1, keepdims=False)
        route = (slot_row, slot_row.reshape(-1, 1), gate_row)
        res = ffn(
            where_of(expert), n2_both, dy_both, expert_gate, expert_up, expert_down,
            *expert_oth[j], route=route,
        )
        outs.append(res[0])
        dxs.append(res[1])
        dgates.append(res[2])
        grads.append(res[3:])
    out_parts, dx_parts = [], []
    for part in outs:
        out_parts += [part, over_core(part[1])]
    for part in dxs:
        dx_parts += [part, over_core(part[1])]
    dgates = jnp.stack(dgates)
    dgate = in_order(core, dgates[:, 0], over_core(dgates[:, 1]), 0)
    comb_e = comb[:experts]
    dlog_t = (comb_e * (dgate - jnp.sum(comb_e * dgate, axis=0, keepdims=True))).astype(BF)
    dlog = jnp.pad(dlog_t.T, ((0, 0), (0, 128 - experts)))
    output, d_resid, d_low, ggain_two = join(
        shard_s, cotangent, resid, gain_two, dlog, router_t128, out_parts, dx_parts
    )
    grad_router = jnp.dot(dlog_t, n2, preferred_element_type=F32)
    gqkv, gout, input_grad, ggain_one = attend_backward(
        pic_block, tokens, gain_one, wqkv, wout, tables, q, k, v, mixed, lse, d_low, d_resid
    )

    groups = [[r for r in range(reps) if r % 2 == c] for c in range(2)]

    def reduce_rep(value):
        piece = lax.psum_scatter(
            value, "rep", scatter_dimension=0, tiled=True, axis_index_groups=groups
        )
        return lax.all_gather(piece, "rep", axis=0, tiled=True, axis_index_groups=groups)

    def summed(keep, send):
        return (keep.astype(F32) + over_x(send).astype(F32)).astype(BF)

    finals = []
    for keep_g, send_g, keep_u, send_u, keep_d, send_d in grads:
        trio = []
        for keep, send in ((keep_g, send_g), (keep_u, send_u), (keep_d, send_d)):
            mine = reduce_rep(summed(keep, send))
            trio.append((mine, over_core(mine)))
        finals.append(trio)

    def shared_out(mine, theirs, axis):
        blocks = mine.shape[axis] // 512
        parts = []
        for b in range(blocks):
            cut = functools.partial(lax.slice_in_dim, start_index=b * 512, limit_index=(b + 1) * 512, axis=axis)
            parts.append(in_order(core, cut(mine), cut(theirs), axis))
        return jnp.concatenate(parts, axis=axis).astype(F32)

    shared_grads = [
        shared_out(*finals[0][0], 1),
        shared_out(*finals[0][1], 1),
        shared_out(*finals[0][2], 0),
    ]
    expert_grads = []
    for m in range(3):
        mine = jnp.stack([finals[1 + j][m][0] for j in range(per_core)])
        theirs = jnp.stack([finals[1 + j][m][1] for j in range(per_core)])
        expert_grads.append(in_order(core, mine, theirs, 0).astype(F32))

    extra_grad = jnp.concatenate([ggain_one, ggain_two, grad_router], axis=0).astype(BF)
    extra_grad = jnp.pad(extra_grad.T, ((0, 0), (0, 128 - extra_grad.shape[0])))
    tail = jnp.concatenate([gqkv, gout, extra_grad], axis=1)
    tail = tail.reshape(shards, reps, half // reps, tail.shape[1]).transpose(1, 0, 2, 3)
    tail = tail.reshape(D, -1)
    piece = lax.psum_scatter(tail, ALL, scatter_dimension=0, tiled=True)
    full = lax.all_gather(piece, "rep", axis=0, tiled=True).astype(F32)
    gq = full[:, : 3 * D].reshape(half, PAIRS, 3, PAIR).transpose(2, 0, 1, 3).reshape(3, half, D)
    g_out = full[:, 3 * D : 4 * D]
    return (
        output,
        input_grad,
        full[:, 4 * D],
        gq[0],
        gq[1],
        gq[2],
        g_out,
        full[:, 4 * D + 1],
        full[:, 4 * D + 2 : 4 * D + 2 + experts],
        expert_grads[0],
        expert_grads[1],
        expert_grads[2],
        shared_grads[0],
        shared_grads[1],
        shared_grads[2],
    )


def solution(mesh):
    both = P(("rep", "shard"), None)
    rows = P("shard", None)
    vec = P("shard")
    mid = P(None, "shard", None)
    return jax.shard_map(
        on_device,
        mesh=mesh,
        in_specs=(
            both, both, P(("rep", "shard")),
            vec, rows, rows, rows, rows, vec, rows, mid, mid, mid, rows, rows, rows,
            both,
        ),
        out_specs=(both, both, vec, rows, rows, rows, rows, vec, rows, mid, mid, mid, rows, rows, rows),
        check_vma=False,
    )
```

```python
import functools

import jax
import jax.numpy as jnp
from jax import lax
from jax.experimental import pallas as pl
from jax.experimental.pallas import tpu as pltpu
from jax.sharding import PartitionSpec as P

D = 768
HEADS = 12
HEAD_DIM = 64
PIC = 256
CAP = 640
PAIR = 2 * HEAD_DIM
PAIRS = HEADS // 2
QB = 256
EPS = 1e-05
BF = jnp.bfloat16
F32 = jnp.float32
ALL = ("rep", "shard")
MIB = 1 << 20
CHEAP = pl.CostEstimate(flops=1, transcendentals=0, bytes_accessed=1)
DEAR = pl.CostEstimate(flops=1 << 36, transcendentals=0, bytes_accessed=1)
HUGE = pl.CostEstimate(flops=1 << 38, transcendentals=0, bytes_accessed=1)
FAIR = pl.CostEstimate(flops=1 << 34, transcendentals=0, bytes_accessed=1)


def nn(a, b):
    return lax.dot_general(a, b, (((1,), (0,)), ((), ())), preferred_element_type=F32)


def nt(a, b):
    return lax.dot_general(a, b, (((1,), (1,)), ((), ())), preferred_element_type=F32)


def resident(shape):
    zeros = (0,) * len(shape)
    return pl.BlockSpec(shape, lambda *_: zeros, pipeline_mode=pl.Buffered(1))


def rotary_tables(length):
    halfway = HEAD_DIM // 2
    freqs_base = 10000.0 ** (-jnp.arange(halfway, dtype=F32) / halfway)
    angles = jnp.arange(length, dtype=F32)[:, None] * freqs_base[None, :]
    cosine = jnp.cos(angles)
    sine = jnp.sin(angles)
    zero = jnp.zeros_like(sine)
    cos_t = jnp.concatenate([cosine] * 4, axis=1)
    left = jnp.concatenate([-sine, zero, -sine, zero], axis=1)
    right = jnp.concatenate([zero, sine, zero, sine], axis=1)
    return cos_t, left, right


def turned(v, left, right):
    return pltpu.roll(v, 96, 1) * left + pltpu.roll(v, 32, 1) * right


def head_masks(rows):
    lane = lax.broadcasted_iota(jnp.int32, (rows, PAIR), 1)
    return lane < HEAD_DIM, lane >= HEAD_DIM


def attend_forward_body(
    where, pic, tok, gain, wq, wk, wv, mine, theirs, cos_t, left, right,
    q_o, k_o, v_o, mix_o, lse_o, w_o,
    xn,
):
    length = tok.shape[0]
    half = D // 2
    step = pl.program_id(0)

    @pl.when(step == 0)
    def _():
        for lo in range(0, length, QB):
            x = tok[lo : lo + QB, :].astype(F32)
            inv = lax.rsqrt(jnp.mean(x * x, axis=1, keepdims=True) + EPS)
            xn[lo : lo + QB, :] = (x * inv * gain[...]).astype(BF)

    own = pl.ds(pl.multiple_of(where[0] * half, half), half)
    quarter = half // 2
    first = pl.ds(pl.multiple_of((1 - where[0]) * half + where[1] * quarter, quarter), quarter)
    second = pl.ds(pl.multiple_of((1 - where[0]) * half + (1 - where[1]) * quarter, quarter), quarter)
    for m, w in enumerate((wq, wk, wv)):
        cols = slice(m * PAIR, (m + 1) * PAIR)
        w_o[own, cols] = w[...]
        w_o[first, cols] = mine[m]
        w_o[second, cols] = theirs[m]
    for lo in range(0, length, QB):
        rows = slice(lo, lo + QB)
        qkv = nn(xn[rows, :], w_o[...])
        q, k = qkv[:, :PAIR], qkv[:, PAIR : 2 * PAIR]
        c_, l_, r_ = cos_t[rows, :], left[rows, :], right[rows, :]
        q_o[rows, :] = (q * c_ + turned(q, l_, r_)).astype(BF) * jnp.asarray(0.125, BF)
        k_o[rows, :] = (k * c_ + turned(k, l_, r_)).astype(BF)
        v_o[rows, :] = qkv[:, 2 * PAIR :].astype(BF)
    masks = head_masks(QB)
    row = lax.broadcasted_iota(jnp.int32, (QB, QB), 0)
    col = lax.broadcasted_iota(jnp.int32, (QB, QB), 1)
    causal = col <= row
    for block in range(length // QB):
        rows = slice(block * QB, (block + 1) * QB)
        allowed = causal | (pic[0] == block)
        q = q_o[rows, :]
        outs = []
        for head in range(2):
            qm = jnp.where(masks[head], q, jnp.zeros_like(q))
            s_d = jnp.where(allowed, nt(qm, k_o[rows, :]), -1e30)
            top = jnp.max(s_d, axis=1, keepdims=True)
            if block:
                s_o = nt(qm, k_o[: block * QB, :])
                top = jnp.maximum(top, jnp.max(s_o, axis=1, keepdims=True))
            p_d = jnp.exp(s_d - top)
            total = jnp.sum(p_d, axis=1, keepdims=True)
            acc = nn(p_d.astype(BF), v_o[rows, :])
            if block:
                p_o = jnp.exp(s_o - top)
                total = total + jnp.sum(p_o, axis=1, keepdims=True)
                acc = acc + nn(p_o.astype(BF), v_o[: block * QB, :])
            outs.append(acc / total)
            lse = jnp.broadcast_to(top + jnp.log(total), (QB, PAIR))
            lse_o[0, head : head + 1, rows] = jnp.transpose(lse)[0:1, :]
        mix_o[rows, :] = jnp.where(masks[0], outs[0], outs[1]).astype(BF)


def attend_forward(where, pic_block, tokens, gain, weights, mine, theirs, tables):
    length = tokens.shape[0]
    half = D // 2
    pair = pl.BlockSpec((length, PAIR), lambda p: (0, p))
    wide = jax.ShapeDtypeStruct((length, D), BF)
    weight = pl.BlockSpec((half, PAIR), lambda p: (0, p))
    part = pl.BlockSpec((4, half // 2, PAIR), lambda p: (0, 0, p))
    return pl.pallas_call(
        attend_forward_body,
        cost_estimate=DEAR,
        grid=(PAIRS,),
        in_specs=[
            pl.BlockSpec(memory_space=pltpu.SMEM),
            pl.BlockSpec(memory_space=pltpu.SMEM),
            resident((length, D)),
            resident((1, D)),
            weight,
            weight,
            weight,
            part,
            part,
            resident((length, PAIR)),
            resident((length, PAIR)),
            resident((length, PAIR)),
        ],
        out_specs=[
            pair, pair, pair, pair,
            pl.BlockSpec((1, 8, length), lambda p: (p, 0, 0)),
            pl.BlockSpec((D, 3 * PAIR), lambda p: (0, p)),
        ],
        out_shape=[
            wide, wide, wide, wide,
            jax.ShapeDtypeStruct((PAIRS, 8, length), F32),
            jax.ShapeDtypeStruct((D, 3 * D), BF),
        ],
        scratch_shapes=[pltpu.VMEM((length, D), BF)],
        compiler_params=pltpu.CompilerParams(vmem_limit_bytes=48 * MIB),
        name="attend_forward",
    )(where, pic_block, tokens, gain, *weights, mine, theirs, *tables)


def attend_backward_body(
    last, where, pic, tok, gain, wqkv, wout, cos_t, left, right, q_i, k_i, v_i, mix_i, lse_i, dres, *refs
):
    if last:
        dres_f, dxn_i, keep_o, send_o, gout_o, igrad_o, ggain_o = refs[:7]
        refs = refs[7:]
    else:
        keep_o, send_o, gout_o, dxn_o = refs[:4]
        refs = refs[4:]
    xn_t, dxn, dmix, dqkv, dk_s, dv_s, k_t = refs
    length = tok.shape[0]
    half = D // 2
    step = pl.program_id(0)

    @pl.when(step == 0)
    def _():
        for lo in range(0, length, QB):
            x = tok[lo : lo + QB, :].astype(F32)
            inv = lax.rsqrt(jnp.mean(x * x, axis=1, keepdims=True) + EPS)
            n_t = jnp.transpose((x * inv * gain[...]).astype(BF))
            spot = pl.multiple_of(where[0] * half, half)
            xn_t[pl.ds(spot, half), lo : lo + QB] = n_t[:half, :]
            xn_t[pl.ds(half - spot, half), lo : lo + QB] = n_t[half:, :]

    dm = nt(dres[...], wout[...]).astype(BF)
    dmix[...] = dm
    mixed = mix_i[...]
    gout_o[...] = nn(jnp.transpose(mixed), dres[...]).astype(BF)
    prod = jnp.transpose(dm.astype(F32) * mixed.astype(F32))
    delta = (
        jnp.sum(prod[:HEAD_DIM, :], axis=0, keepdims=True),
        jnp.sum(prod[HEAD_DIM:, :], axis=0, keepdims=True),
    )
    k_t[...] = jnp.transpose(k_i[...])
    masks = head_masks(QB)
    key_row = lax.broadcasted_iota(jnp.int32, (QB, QB), 0)
    query_col = lax.broadcasted_iota(jnp.int32, (QB, QB), 1)
    causal = key_row <= query_col
    for block in reversed(range(length // QB)):
        rows = slice(block * QB, (block + 1) * QB)
        first = block == length // QB - 1
        allowed = causal | (pic[0] == block)
        q = q_i[rows, :]
        dm = dmix[rows, :]
        dq_t = []
        parts = {"d": [], "o": []}
        for head in range(2):
            qm = jnp.where(masks[head], q, jnp.zeros_like(q))
            dmm = jnp.where(masks[head], dm, jnp.zeros_like(dm))
            lse = lse_i[0, head : head + 1, rows]
            cent = delta[head][:, rows]
            lanes = slice(head * HEAD_DIM, (head + 1) * HEAD_DIM)
            dq = None
            for part, keys in (("d", rows), ("o", slice(0, block * QB))):
                if part == "o" and block == 0:
                    continue
                st = nt(k_i[keys, :], qm)
                pt = jnp.exp(st - lse)
                if part == "d":
                    pt = jnp.where(allowed, pt, 0.0)
                dpt = nt(v_i[keys, :], dmm)
                dst = (pt * (dpt - cent)).astype(BF)
                parts[part].append((nn(dst, qm), nn(pt.astype(BF), dmm)))
                add = nn(k_t[lanes, keys], dst)
                dq = add if dq is None else dq + add
            dq_t.append(dq)
        for part, keys in (("d", rows), ("o", slice(0, block * QB))):
            if not parts[part]:
                continue
            dk = parts[part][0][0] + parts[part][1][0]
            dv = parts[part][0][1] + parts[part][1][1]
            if first:
                dk_s[keys, :] = dk
                dv_s[keys, :] = dv
            else:
                dk_s[keys, :] = dk_s[keys, :] + dk
                dv_s[keys, :] = dv_s[keys, :] + dv
        dq = jnp.transpose(jnp.concatenate(dq_t, axis=0)) * 0.125
        c_, l_, r_ = cos_t[rows, :], left[rows, :], right[rows, :]
        dqkv[rows, :PAIR] = (dq * c_ - turned(dq, l_, r_)).astype(BF)
        dk = dk_s[rows, :]
        dqkv[rows, PAIR : 2 * PAIR] = (dk * c_ - turned(dk, l_, r_)).astype(BF)
        dqkv[rows, 2 * PAIR :] = dv_s[rows, :].astype(BF)
    gqkv = nn(xn_t[...], dqkv[...]).astype(BF)
    keep_o[...] = gqkv[:half, :]
    send_o[...] = gqkv[half:, :]
    add = nt(dqkv[...], wqkv[...])

    @pl.when(step == 0)
    def _():
        if last:
            dxn[...] = dxn_i[...] + add
        else:
            dxn[...] = add

    @pl.when(step > 0)
    def _():
        dxn[...] = dxn[...] + add

    @pl.when(step == pl.num_programs(0) - 1)
    def _():
        if not last:
            dxn_o[...] = dxn[...]
            return
        total = jnp.zeros((1, D), F32)
        for lo in range(0, length, QB):
            rows = slice(lo, lo + QB)
            x = tok[rows, :].astype(F32)
            inv = lax.rsqrt(jnp.mean(x * x, axis=1, keepdims=True) + EPS)
            n = x * inv
            up = dxn[rows, :]
            total = total + jnp.sum(up * n, axis=0, keepdims=True)
            u = up * gain[...]
            igrad_o[rows, :] = dres_f[rows, :] + inv * (u - n * jnp.mean(u * n, axis=1, keepdims=True))
        ggain_o[...] = total


def attend_backward(where, pic_block, tokens, gain, wqkv, wout, tables, q, k, v, mixed, lse, dres, more=None):
    length = tokens.shape[0]
    half = D // 2
    last = more is not None
    early = 2 * PAIRS // 3
    count = PAIRS - early if last else early
    off = early if last else 0
    pair = pl.BlockSpec((length, PAIR), lambda p: (0, p + off))
    grad = pl.BlockSpec((half, 3 * PAIR), lambda p: (0, p))
    wide = jax.ShapeDtypeStruct((length, D), F32)
    out_specs = [grad, grad, pl.BlockSpec((PAIR, D), lambda p: (p, 0)), resident((length, D))]
    out_shape = [
        jax.ShapeDtypeStruct((half, 3 * PAIR * count), BF),
        jax.ShapeDtypeStruct((half, 3 * PAIR * count), BF),
        jax.ShapeDtypeStruct((PAIR * count, D), BF),
        wide,
    ]
    if last:
        out_specs.append(resident((1, D)))
        out_shape.append(jax.ShapeDtypeStruct((1, D), F32))
    return pl.pallas_call(
        functools.partial(attend_backward_body, last),
        cost_estimate=DEAR,
        grid=(count,),
        in_specs=[
            pl.BlockSpec(memory_space=pltpu.SMEM),
            pl.BlockSpec(memory_space=pltpu.SMEM),
            resident((length, D)),
            resident((1, D)),
            pl.BlockSpec((D, 3 * PAIR), lambda p: (0, p + off)),
            pl.BlockSpec((PAIR, D), lambda p: (p + off, 0)),
            resident((length, PAIR)),
            resident((length, PAIR)),
            resident((length, PAIR)),
            pair, pair, pair, pair,
            pl.BlockSpec((1, 8, length), lambda p: (p + off, 0, 0)),
            resident((length, D)),
        ]
        + ([resident((length, D))] * 2 if last else []),
        out_specs=out_specs,
        out_shape=out_shape,
        scratch_shapes=[
            pltpu.VMEM((D, length), BF),
            pltpu.VMEM((length, D), F32),
            pltpu.VMEM((length, PAIR), BF),
            pltpu.VMEM((length, 3 * PAIR), BF),
            pltpu.VMEM((length, PAIR), F32),
            pltpu.VMEM((length, PAIR), F32),
            pltpu.VMEM((PAIR, length), BF),
        ],
        compiler_params=pltpu.CompilerParams(vmem_limit_bytes=56 * MIB),
        name="attend_backward_2" if last else "attend_backward_1",
    )(where, pic_block, tokens, gain, wqkv, wout, *tables, q, k, v, mixed, lse, dres, *(more or ()))


def middle_body(
    shard, tok, mixed, w_own, w_mine, w_theirs, gain, router_t, routes_t,
    resid_o, n2_o, n2p_o, comb_o, wout,
):
    @pl.when(pl.program_id(0) == 0)
    def _():
        half = D // 2
        quarter = half // 2
        other = (1 - shard[0]) * half
        wout[pl.ds(pl.multiple_of(shard[0] * half, half), half), :] = w_own[...]
        first = pl.multiple_of(other + shard[1] * quarter, quarter)
        second = pl.multiple_of(other + (1 - shard[1]) * quarter, quarter)
        wout[pl.ds(first, quarter), :] = w_mine[...]
        wout[pl.ds(second, quarter), :] = w_theirs[...]

    r = tok[...].astype(F32) + nn(mixed[...], wout[...])
    resid_o[...] = r
    inv = lax.rsqrt(jnp.mean(r * r, axis=1, keepdims=True) + EPS)
    n2 = (r * inv * gain[...]).astype(BF)
    n2_o[...] = n2
    half = D // 2
    swapped = jnp.concatenate([n2[:, half:], n2[:, :half]], axis=1)
    n2p_o[...] = jnp.where(shard[0] == 0, n2, swapped)
    logits = nt(router_t[...], n2)
    expert = lax.broadcasted_iota(jnp.int32, logits.shape, 0)
    picks = [expert == routes_t[k : k + 1, :] for k in range(2)]
    chosen = [jnp.sum(jnp.where(p, logits, 0.0), axis=0, keepdims=True) for p in picks]
    top = jnp.maximum(chosen[0], chosen[1])
    weights = [jnp.exp(v - top) for v in chosen]
    total = weights[0] + weights[1]
    gates = [w / total for w in weights]
    comb_o[...] = jnp.where(picks[0], gates[0], 0.0) + jnp.where(picks[1], gates[1], 0.0)


def middle(where, tokens, mixed, w_own, w_mine, w_theirs, gain, router_t, routes_t):
    length = tokens.shape[0]
    block = 256
    rows = pl.BlockSpec((block, D), lambda i: (i, 0))
    cols = pl.BlockSpec((8, block), lambda i: (0, i))
    return pl.pallas_call(
        middle_body,
        cost_estimate=CHEAP,
        grid=(length // block,),
        in_specs=[
            pl.BlockSpec(memory_space=pltpu.SMEM),
            rows,
            rows,
            resident((D // 2, D)),
            pl.BlockSpec((None, D // 4, D), lambda i: (3, 0, 0), pipeline_mode=pl.Buffered(1)),
            pl.BlockSpec((None, D // 4, D), lambda i: (3, 0, 0), pipeline_mode=pl.Buffered(1)),
            resident((1, D)),
            resident((8, D)),
            cols,
        ],
        out_specs=[rows, rows, rows, cols, resident((D, D))],
        out_shape=[
            jax.ShapeDtypeStruct((length, D), F32),
            jax.ShapeDtypeStruct((length, D), BF),
            jax.ShapeDtypeStruct((length, D), BF),
            jax.ShapeDtypeStruct((8, length), F32),
            jax.ShapeDtypeStruct((D, D), BF),
        ],
        compiler_params=pltpu.CompilerParams(vmem_limit_bytes=40 * MIB),
        name="middle",
    )(where, tokens, mixed, w_own, w_mine, w_theirs, gain, router_t, routes_t)


def join_body(shard, dy, resid, gain, dlog, router_t, *refs):
    parts = refs[:-4]
    out_o, dres_o, dlow_o, ggain_o = refs[-4:]
    r = resid[...]
    total = r
    for part in parts:
        total = total + part[0].astype(F32)
    out_o[...] = total.astype(BF)
    up = parts[0][1].astype(F32)
    for part in parts[1:]:
        up = up + part[1].astype(F32)
    half = D // 2
    swapped = jnp.concatenate([up[:, half:], up[:, :half]], axis=1)
    up = jnp.where(shard[0] == 0, up, swapped)
    up = up + nn(dlog[...], router_t[...])
    inv = lax.rsqrt(jnp.mean(r * r, axis=1, keepdims=True) + EPS)
    n = r * inv
    add = jnp.sum(up * n, axis=0, keepdims=True)

    @pl.when(pl.program_id(0) == 0)
    def _():
        ggain_o[...] = add

    @pl.when(pl.program_id(0) > 0)
    def _():
        ggain_o[...] = ggain_o[...] + add

    u = up * gain[...]
    d = dy[...].astype(F32) + inv * (u - n * jnp.mean(u * n, axis=1, keepdims=True))
    dres_o[...] = d
    dlow_o[...] = d.astype(BF)


def join(shard, dy, resid, gain, dlog, router_t, parts):
    length = dy.shape[0]
    block = 256
    rows = pl.BlockSpec((block, D), lambda i: (i, 0))

    return pl.pallas_call(
        join_body,
        cost_estimate=CHEAP,
        grid=(length // block,),
        in_specs=[
            pl.BlockSpec(memory_space=pltpu.SMEM),
            rows,
            rows,
            resident((1, D)),
            pl.BlockSpec((block, 128), lambda i: (i, 0)),
            resident((128, D)),
        ]
        + [pl.BlockSpec((2, block, D), lambda i: (0, i, 0))] * len(parts),
        out_specs=[rows, rows, rows, pl.BlockSpec((1, D), lambda i: (0, 0))],
        out_shape=[
            jax.ShapeDtypeStruct((length, D), BF),
            jax.ShapeDtypeStruct((length, D), F32),
            jax.ShapeDtypeStruct((length, D), BF),
            jax.ShapeDtypeStruct((1, D), F32),
        ],
        compiler_params=pltpu.CompilerParams(vmem_limit_bytes=40 * MIB),
        name="join",
    )(shard, dy, resid, gain, dlog, router_t, *parts)


def ffn_body(routed, steps, chunk, before, where, tok_a, tok_b, dy_a, dy_b, *refs):
    tok, dy = (tok_a, tok_b), (dy_a, dy_b)
    if routed:
        slot_row, slot_col, gate_row = refs[:3]
        refs = refs[3:]
    g_own, u_own, d_own = refs[:3]
    per = steps // 2
    gu_oth = refs[3 : 3 + 2 * per]
    d_oth = refs[3 + 2 * per : 3 + 4 * per]
    refs = refs[3 + 4 * per :]
    if before:
        theirs_i = refs[0]
        refs = refs[1:]
    sides = refs[:2]
    refs = refs[2:]
    if routed:
        dgate_o = refs[0]
        refs = refs[1:]
    keep, send, hold_y, push_y = refs[:4]
    refs = refs[4:]
    wg, wu, wd, y_acc, dx_acc, hid_s, dg_s, du_s, x_t, de_t = refs[:10]
    refs = refs[10:]
    i = pl.program_id(0)
    srcs, length = 2, tok_a.shape[0]
    rows_all = y_acc.shape[0]
    hold = rows_all // srcs
    half = D // 2
    if routed:
        x_s, de_s, dys, gate_s = refs
    tile = 128

    @pl.when(i == 0)
    def _():
        for src in range(srcs):
            if routed:
                for lo in range(0, hold, tile):
                    slot = lax.broadcasted_iota(jnp.int32, (tile, length), 0) + lo
                    mine = slot == slot_row[src : src + 1, :]
                    pick = jnp.where(mine, 1.0, 0.0).astype(BF)
                    rows = slice(src * hold + lo, src * hold + lo + tile)
                    x = nn(pick, tok[src][...]).astype(BF)
                    d_raw = nn(pick, dy[src][...])
                    gate = jnp.sum(jnp.where(mine, gate_row[src : src + 1, :], 0.0), axis=1, keepdims=True)
                    gate_s[rows, :] = jnp.broadcast_to(gate, (tile, 128))
                    d_e = (d_raw * gate).astype(BF)
                    x_s[rows, :] = x
                    dys[rows, :] = d_raw.astype(BF)
                    de_s[rows, :] = d_e
                    x_t[:, rows] = jnp.transpose(x)
                    de_t[:, rows] = jnp.transpose(d_e)
            else:
                for lo in range(0, hold, 256):
                    rows = slice(src * hold + lo, src * hold + lo + 256)
                    x_t[:, rows] = jnp.transpose(tok[src][lo : lo + 256, :])
                    de_t[:, rows] = jnp.transpose(dy[src][lo : lo + 256, :])

    wg[:half, :] = g_own[...]
    wu[:half, :] = u_own[...]
    part = half // 2
    block = wd.shape[0]
    for p in range(per):

        @pl.when(i // 2 == p)
        def _(p=p):
            for k in range(2):
                spot = pl.ds(pl.multiple_of(half + (where[4] ^ k) * part, part), part)
                ref = gu_oth[2 * p + k]
                for h in range(2):
                    lanes = slice(h * 256, (h + 1) * 256)
                    wg[spot, lanes] = ref[2 * h * part : (2 * h + 1) * part, :]
                    wu[spot, lanes] = ref[(2 * h + 1) * part : (2 * h + 2) * part, :]

    @pl.when(i % 2 == 0)
    def _():
        wd[...] = d_own[...]

    for p in range(per):

        @pl.when(i == 2 * p + 1)
        def _(p=p):
            for k in range(2):
                spot = pl.ds(pl.multiple_of((where[4] ^ k) * (block // 2), block // 2), block // 2)
                for h in range(3):
                    wd[spot, h * 256 : (h + 1) * 256] = d_oth[2 * p + k][h * 256 : (h + 1) * 256, :]

    def piece(j, src, first):
        inner = pl.ds(pl.multiple_of(j * chunk, chunk), chunk)
        if routed:
            rows = inner
            x, de = x_s[rows, :], de_s[rows, :]
        else:
            rows = pl.ds(pl.multiple_of(src * length + j * chunk, chunk), chunk)
            x, de = tok[src][inner, :], dy[src][inner, :]
        g = nn(x, wg[...])
        u = nn(x, wu[...])
        dh = nt(de, wd[...])
        s = 1.0 / (1.0 + jnp.exp(-g))
        act = g * s
        hid = (act * u).astype(BF)
        du = (dh * act).astype(BF)
        dg = (dh * u * s * (1.0 + g * (1.0 - s))).astype(BF)
        hid_s[rows, :] = hid
        dg_s[rows, :] = dg
        du_s[rows, :] = du
        y = nn(hid, wd[...])
        dx = nt(dg, wg[...]) + nt(du, wu[...])
        if first:
            y_acc[rows, :] = y
            dx_acc[rows, :] = dx
        else:
            y_acc[rows, :] = y_acc[rows, :] + y
            dx_acc[rows, :] = dx_acc[rows, :] + dx

    for first in (True, False):

        @pl.when((i == 0) == first)
        def _(first=first):
            for src in range(1 if routed else srcs):

                @pl.loop(0, (rows_all if routed else length) // chunk)
                def _(j, src=src, first=first):
                    piece(j, src, first)

    gg = nn(x_t[...], dg_s[...]).astype(BF)
    gu = nn(x_t[...], du_s[...]).astype(BF)
    gd = nn(de_t[...], hid_s[...]).astype(BF)
    for p in range(per):

        def put(side, tile, value, p=p):
            count = keep.shape[0]
            number = 6 * p + tile
            if number < count:
                (keep, send)[side][number] = value
            else:
                top, low = value[: half // 2, :], value[half // 2 :, :]
                hold_y[side, number - count] = jnp.where(where[4] == 0, top, low)
                push_y[side, number - count] = jnp.where(where[4] == 0, low, top)

        @pl.when(i == 2 * p)
        def _(put=put):
            put(0, 0, gg[:half, :])
            put(0, 1, gu[:half, :])
            put(0, 2, gd[:half, :])
            put(0, 3, gd[half:, :])
            put(1, 4, gg[half:, :])
            put(1, 5, gu[half:, :])

        @pl.when(i == 2 * p + 1)
        def _(put=put):
            put(0, 4, gg[:half, :])
            put(0, 5, gu[:half, :])
            put(1, 0, gg[half:, :])
            put(1, 1, gu[half:, :])
            put(1, 2, gd[:half, :])
            put(1, 3, gd[half:, :])

    @pl.when(i == steps - 1)
    def _():
        for src in range(srcs):
            if routed:
                total = jnp.zeros((1, length), F32)
                for lo in range(0, hold, tile):
                    rows = slice(src * hold + lo, src * hold + lo + tile)
                    y = y_acc[rows, :]
                    dgate = jnp.sum(dys[rows, :].astype(F32) * y, axis=1, keepdims=True)
                    slot = lax.broadcasted_iota(jnp.int32, (tile, length), 0) + lo
                    mine = slot == slot_row[src : src + 1, :]
                    total = total + jnp.sum(jnp.where(mine, dgate, 0.0), axis=0, keepdims=True)
                    x_s[rows, :] = (y * gate_s[rows, 0:1]).astype(BF)
                    de_s[rows, :] = dx_acc[rows, :].astype(BF)
                dgate_o[src : src + 1, :] = total
                held = slice(src * hold, (src + 1) * hold)
                for lo in range(0, length, tile):
                    slot = lax.broadcasted_iota(jnp.int32, (tile, hold), 1)
                    mine = slot == slot_col[src * length + lo : src * length + lo + tile, :]
                    pick = jnp.where(mine, 1.0, 0.0).astype(BF)
                    sides[src][0, lo : lo + tile, :] = nn(pick, x_s[held, :]).astype(BF)
                    sides[src][1, lo : lo + tile, :] = nn(pick, de_s[held, :]).astype(BF)
            else:
                held = slice(src * hold, (src + 1) * hold)
                for n, acc in enumerate((y_acc, dx_acc)):
                    total = acc[held, :]
                    if before and src == 1:
                        total = total + theirs_i[n].astype(F32)
                    sides[src][n] = total.astype(BF)


def ffn(where, toks, dys, gate, up, down, others, route=None, only=None, before=None):
    routed = route is not None
    srcs, length = 2, toks[0].shape[0]
    block = 512
    half = D // 2
    per = len(others) // 2
    total, start = (2, only) if only is not None else (per, 0)
    steps = 2 * per
    rows_all = srcs * (CAP if routed else length)
    chunk = 256

    def column(i, w):
        return (i % 2 + w[0] - 2 * w[0] * (i % 2)) * total + i // 2 + start

    if routed:
        gate_spec = pl.BlockSpec((None, half, block), lambda i, w: (w[2], 0, column(i, w)))
        down_spec = pl.BlockSpec((None, block, D), lambda i, w: (w[2], i // 2 + start, 0))
    else:
        gate_spec = pl.BlockSpec((half, block), lambda i, w: (0, column(i, w) * 2 + w[1]))
        down_spec = pl.BlockSpec((block, D), lambda i, w: (w[1], 0))
    def shard_block(i, w):
        return i % 2 + w[0] - 2 * w[0] * (i % 2)

    def gu_spec(p):
        first, last = 2 * p, 2 * p + 1
        return pl.BlockSpec((2 * half, 256), lambda i, w: (shard_block(jnp.clip(i, first, last), w), 0))

    d_spec = pl.BlockSpec((2 * half, 256), lambda i, w: (2, 0), pipeline_mode=pl.Buffered(1))
    in_specs = [resident((length, D))] * 4
    operands = [*toks, *dys]
    if routed:
        in_specs += [resident(r.shape) for r in route]
        operands += list(route)
    in_specs += [gate_spec, gate_spec, down_spec] + [gu_spec(n // 2) for n in range(2 * per)] + [d_spec] * (2 * per)
    operands += [gate, up, down, *others, *others]
    if before is not None:
        in_specs.append(resident(before.shape))
        operands.append(before)
    wide = jax.ShapeDtypeStruct((srcs, length, D), BF)
    out_specs = [resident((srcs, length, D)), resident((srcs, length, D))]
    out_shape = [wide, wide]
    if routed:
        out_specs.append(resident((srcs, length)))
        out_shape.append(jax.ShapeDtypeStruct((srcs, length), F32))
    for shape in ((3 * per, half, block), (2, 3 * per, half // 2, block)):
        out_specs += [resident(shape)] * 2
        out_shape += [jax.ShapeDtypeStruct(shape, BF)] * 2
    scratch = [
        pltpu.VMEM((D, block), BF),
        pltpu.VMEM((D, block), BF),
        pltpu.VMEM((block, D), BF),
        pltpu.VMEM((rows_all, D), F32),
        pltpu.VMEM((rows_all, D), F32),
        pltpu.VMEM((rows_all, block), BF),
        pltpu.VMEM((rows_all, block), BF),
        pltpu.VMEM((rows_all, block), BF),
        pltpu.VMEM((D, rows_all), BF),
        pltpu.VMEM((D, rows_all), BF),
    ]
    if routed:
        scratch += [
            pltpu.VMEM((rows_all, D), BF),
            pltpu.VMEM((rows_all, D), BF),
            pltpu.VMEM((rows_all, D), BF),
            pltpu.VMEM((rows_all, 128), F32),
        ]
    return pl.pallas_call(
        functools.partial(ffn_body, routed, steps, chunk, before is not None),
        cost_estimate=DEAR,
        grid_spec=pltpu.PrefetchScalarGridSpec(
            num_scalar_prefetch=1,
            grid=(steps,),
            in_specs=in_specs,
            out_specs=out_specs,
            scratch_shapes=scratch,
        ),
        out_shape=out_shape,
        compiler_params=pltpu.CompilerParams(vmem_limit_bytes=63 * MIB),
        name="ffn_routed" if routed else "ffn_shared",
    )(where, *operands)


def add(a, b):
    return a[...].astype(F32) + b[...].astype(F32)


def small_call(body, name, where, grid, ins, outs, cost=CHEAP):
    return pl.pallas_call(
        body,
        cost_estimate=cost,
        grid_spec=pltpu.PrefetchScalarGridSpec(
            num_scalar_prefetch=1,
            grid=grid,
            in_specs=[pl.BlockSpec(block, index) for _, block, index in ins],
            out_specs=[pl.BlockSpec(block, index) for _, block, index in outs],
        ),
        out_shape=[jax.ShapeDtypeStruct(shape, BF) for shape, _, _ in outs],
        compiler_params=pltpu.CompilerParams(vmem_limit_bytes=32 * MIB),
        name=name,
    )(where, *[array for array, _, _ in ins])


def sum_x(where, keep, got, cost=CHEAP):
    tiles, rows, cols = keep.shape
    block = (1, rows // 2, cols)

    def mine(t, w):
        return (t, w[4], 0)

    def other(t, w):
        return (t, 1 - w[4], 0)

    def body(w, k_m, g_m, k_o, g_o, send, hold):
        hold[...] = add(k_m, g_m).astype(BF)
        send[...] = add(k_o, g_o).astype(BF)

    ins = [(keep, block, mine), (got, block, mine), (keep, block, other), (got, block, other)]
    shape = (tiles, rows // 2, cols)
    here = (shape, block, lambda t, w: (t, 0, 0))
    return small_call(body, "sum_x", where, (tiles,), ins, [here, here], cost)


def sum_y(where, keep, got, cost=CHEAP):
    tiles, rows, cols = keep.shape
    step = 3 if tiles % 3 == 0 else 1
    block = (step, rows // 4, cols)

    def body(w, *refs):
        for k in range(4):
            refs[8 + k][...] = add(refs[k], refs[4 + k]).astype(BF)

    spots = [lambda t, w, k=k: (t, w[5] ^ k, 0) for k in range(4)]
    ins = [(keep, block, s) for s in spots] + [(got, block, s) for s in spots]
    here = ((tiles, rows // 4, cols), block, lambda t, w: (t, 0, 0))
    return small_call(body, "sum_y", where, (tiles // step,), ins, [here] * 4, cost)


def sum_z(where, parts, cost=CHEAP):
    shape = parts[0].shape
    step = 3 if shape[0] % 3 == 0 else 1
    block = (step,) + shape[1:]

    def body(w, a, b, c, d, out):
        out[...] = (add(a, b) + add(c, d)).astype(BF)

    def at(t, w):
        return (t, 0, 0)

    ins = [(p, block, at) for p in parts]
    return small_call(body, "sum_z", where, (shape[0] // step,), ins, [(shape, block, at)], cost)[0]


def pack(where, gate, up, down, units, per, cost=CHEAP):
    half = D // 2
    part = half // 2
    routed = gate.ndim == 3

    def body(w, *refs):
        for n in range(len(units)):
            g, u, d = refs[3 * n : 3 * n + 3]
            out = refs[3 * len(units) + n]

            @pl.when(pl.program_id(0) < 2)
            def _(g=g, u=u, out=out):
                for h in range(2):
                    for m, ref in enumerate((g, u)):
                        spot = (2 * h + m) * part
                        out[spot : spot + part, :] = ref[:, h * 256 : (h + 1) * 256]

            @pl.when(pl.program_id(0) == 2)
            def _(d=d, out=out):
                for h in range(3):
                    out[h * 256 : (h + 1) * 256, :] = d[:, h * 256 : (h + 1) * 256]

    in_specs = []
    for p, flip in units:

        def col_block(b, p=p):
            return jnp.minimum(b, 1) * per + p

        if routed:
            col = pl.BlockSpec((None, part, 512), lambda b, w, c=col_block, f=flip: (w[2], w[4] ^ f, c(b)))
            row = pl.BlockSpec((None, 256, D), lambda b, w, p=p, f=flip: (w[2], p * 2 + (w[4] ^ f), 0))
        else:
            col = pl.BlockSpec((part, 512), lambda b, w, c=col_block, f=flip: (w[4] ^ f, c(b) * 2 + w[1]))
            row = pl.BlockSpec((256, D), lambda b, w, f=flip: (w[1] * 2 + (w[4] ^ f), 0))
        in_specs += [col, col, row]
    out = pl.BlockSpec((2 * half, 256), lambda b, w: (b, 0))
    return pl.pallas_call(
        body,
        cost_estimate=cost,
        grid_spec=pltpu.PrefetchScalarGridSpec(
            num_scalar_prefetch=1, grid=(3,), in_specs=in_specs, out_specs=[out] * len(units)
        ),
        out_shape=[jax.ShapeDtypeStruct((6 * half, 256), BF)] * len(units),
        name="pack",
    )(where, *[gate, up, down] * len(units))


def pair_first(where, keep, got, hold, got_y, cost=CHEAP):
    tiles, rows, cols = keep.shape
    block = (1, rows // 2, cols)
    both = (2, 1, rows // 2, cols)

    def mine(t, w):
        return (t, w[4], 0)

    def other(t, w):
        return (t, 1 - w[4], 0)

    def two(t, w):
        return (0, t, 0, 0)

    def body(w, k_m, g_m, k_o, g_o, h, g, y_send, y_keep, x_send, x_keep):
        y_keep[...] = add(k_m, g_m).astype(BF)
        y_send[...] = add(k_o, g_o).astype(BF)
        total = add(h, g).astype(BF)
        x_keep[...] = total[0]
        x_send[...] = total[1]

    ins = [(keep, block, mine), (got, block, mine), (keep, block, other), (got, block, other)]
    ins += [(hold, both, two), (got_y, both, two)]
    here = ((tiles, rows // 2, cols), block, lambda t, w: (t, 0, 0))
    return small_call(body, "pair_first", where, (tiles,), ins, [here] * 4, cost)


def pair_second(where, a, b, c, d, cost=CHEAP):
    tiles, rows, cols = a.shape
    block = (3, rows // 4, cols)

    def body(w, *refs):
        for k in range(4):
            a_, b_, c_, d_ = refs[4 * k : 4 * k + 4]
            refs[16 + k][0] = add(a_, b_).astype(BF)
            refs[16 + k][1] = add(c_, d_).astype(BF)

    ins = []
    for k in range(4):
        ins += [(x, block, lambda t, w, k=k: (t, w[5] ^ k, 0)) for x in (a, b, c, d)]
    out = ((2, tiles) + block[1:], (2,) + block, lambda t, w: (0, t, 0, 0))
    return small_call(body, "pair_second", where, (tiles // 3,), ins, [out] * 4, cost)


def pair_scatter(where, a, b, c, d):
    tiles, rows, cols = a.shape
    block = (tiles, rows // 4, cols)

    def body(w, a_, b_, c_, d_, out):
        out[0] = add(a_, b_).astype(BF)
        out[1] = add(c_, d_).astype(BF)

    ins = [(x, block, lambda t, w: (0, t, 0)) for x in (a, b, c, d)]
    out = ((4, 2) + block, (None, 2) + block, lambda t, w: (t, 0, 0, 0, 0))
    return small_call(body, "pair_scatter", where, (4,), ins, [out])[0]


def pair_third(where, parts, cost=CHEAP):
    shape = parts[0].shape
    block = (None,) + shape[1:]

    def body(w, a, b, c, d, out):
        out[...] = (add(a, b) + add(c, d)).astype(BF)

    def at(n, w):
        return (n, 0, 0, 0)

    return small_call(body, "pair_third", where, (2,), [(p, block, at) for p in parts], [(shape, block, at)], cost)[0]


def attention_pack(where, first_keep, first_send, last_keep, last_send, gout_low, gout_high, gain_a, gain_b, router_g):
    half = D // 2
    wide = 2 * D + 128

    def body(w, lk, ls, hk, hs, gl, gh, ga, gb, gr, other, mine, rows, turned_rows):
        rows[...] = jnp.zeros(rows.shape, F32)
        rows[0:1, :] = ga[...]
        rows[1:2, :] = gb[...]
        rows[2 : 2 + gr.shape[0], :] = gr[...]
        turned_rows[...] = jnp.transpose(rows[...]).astype(BF)
        split = lk.shape[1]
        cut = wide - split
        rest = hk.shape[1] - cut
        for side, (low, high) in enumerate(((lk, hk), (ls, hs))):
            spot = pl.multiple_of((w[0] ^ side) * half, half)
            more = turned_rows[pl.ds(spot, half), :]
            for core in range(2):

                @pl.when(w[1] == core)
                def _(core=core, low=low, high=high, side=side, more=more):
                    first, last = (mine, other) if core == 0 else (other, mine)
                    first[side, :, :split] = low[...]
                    first[side, :, split:] = high[:, :cut]
                    last[side, :, :rest] = high[:, cut:]
                    last[side, :, rest + D : rest + D + 128] = more
                    last[side, :, rest + D + 128 :] = jnp.zeros((half, wide - rest - D - 128), BF)

            for core in range(2):
                for part in range(2):

                    @pl.when((w[1] == core) & ((w[0] ^ side) == part))
                    def _(core=core, part=part, side=side):
                        last = (other, mine)[core]
                        if part == 0:
                            last[side, :, rest : rest + D] = gl[:half, :]
                        else:
                            count = gl.shape[0] - half
                            last[side, :count, rest : rest + D] = gl[half:, :]
                            last[side, count:, rest : rest + D] = gh[...]

    last_core = (first_keep, first_send, last_keep, last_send, gout_low, gout_high, gain_a, gain_b, router_g)
    out = resident((2, half, wide))
    return pl.pallas_call(
        body,
        cost_estimate=CHEAP,
        grid_spec=pltpu.PrefetchScalarGridSpec(
            num_scalar_prefetch=1,
            grid=(1,),
            in_specs=[resident(v.shape) for v in last_core],
            out_specs=[out, out],
            scratch_shapes=[pltpu.VMEM((128, D), F32), pltpu.VMEM((D, 128), BF)],
        ),
        out_shape=[jax.ShapeDtypeStruct((2, half, wide), BF)] * 2,
        compiler_params=pltpu.CompilerParams(vmem_limit_bytes=40 * MIB),
        name="attention_pack",
    )(where, *last_core)


def attention_sum(where, mine, got):
    block = (1,) + mine.shape[1:]

    def body(w, a, b, c, d, keep, send):
        keep[...] = add(a, b).astype(BF)
        send[...] = add(c, d).astype(BF)

    ins = [(v, block, lambda t, w, n=n: (n, 0, 0)) for n in range(2) for v in (mine, got)]
    out = (block, block, lambda t, w: (0, 0, 0))
    return small_call(body, "attention_sum", where, (1,), ins, [out, out])


def attention_unpack(where, mine, theirs):
    half, wide = mine.shape[1:]

    def body(w, m, t, *outs):
        for core in range(2):

            @pl.when(w[1] == core)
            def _(core=core):
                both = (m, t) if core == 0 else (t, m)

                def cols(lo):
                    return both[lo // wide][0, :, lo % wide : lo % wide + 128].astype(F32)

                for pair in range(PAIRS):
                    for n in range(3):
                        outs[n][:, pair * PAIR : (pair + 1) * PAIR] = cols((3 * pair + n) * PAIR)
                for n in range(D // 128):
                    outs[3][:, n * 128 : (n + 1) * 128] = cols(3 * D + n * 128)
                outs[4][...] = cols(4 * D)

    shapes = [(half, D)] * 4 + [(half, 128)]
    return pl.pallas_call(
        body,
        cost_estimate=CHEAP,
        grid_spec=pltpu.PrefetchScalarGridSpec(
            num_scalar_prefetch=1,
            grid=(1,),
            in_specs=[resident(mine.shape)] * 2,
            out_specs=[resident(v) for v in shapes],
        ),
        out_shape=[jax.ShapeDtypeStruct(v, F32) for v in shapes],
        compiler_params=pltpu.CompilerParams(vmem_limit_bytes=40 * MIB),
        name="attention_unpack",
    )(where, mine, theirs)


def assemble(where, pieces):
    tiles, rows, cols = pieces[0].shape
    block = (tiles, rows, cols)

    def body(w, *refs):
        for k in range(8):

            @pl.when(pl.program_id(0) == k)
            def _(k=k):
                refs[8][...] = refs[k][...]

    ins = [(p, block, lambda t, w: (0, 0, 0)) for p in pieces]
    out = ((tiles, 8 * rows, cols), block, lambda t, w: (0, t ^ (w[4] * 4 + w[5]), 0))
    return small_call(body, "assemble", where, (8,), ins, [out])[0]


def place(where, j, full, shapes, before, cost=CHEAP):
    paired = isinstance(full, (list, tuple))
    count, _, rows, block = (full[0] if paired else full).shape[1:]
    half = 8 * rows
    routed = j is not None

    def core(t, w):
        return t + w[1] - 2 * t * w[1]

    def column(o, w):
        o = jnp.minimum(o, 1)
        return o + w[0] - 2 * o * w[0]

    def pick(o):
        return jnp.where(o == 0, 0, 3 - o)

    if paired:
        operands = list(full)

        def mine(t, p, o, w):
            return (0, jnp.where(t == 0, p, count - 1), jnp.where(t == 0, pick(o), 1), 0, 0)

        def theirs(t, p, o, w):
            return (0, jnp.where(t == 0, 0, p), jnp.where(t == 0, 0, pick(o)), 0, 0)

        tiles = [pl.BlockSpec((8, None, 2, rows, block), index) for index in (mine, theirs)]
    else:
        operands = [full.reshape((8, 2) + full.shape[1:])]
        tiles = [
            pl.BlockSpec((8, None, None, 2, rows, block), lambda t, p, o, w: (0, core(t, w), p, pick(o), 0, 0))
        ]

    def body(w, *refs):
        for which in range(len(tiles)):
            if paired:

                @pl.when(pl.program_id(0) == which)
                def _(which=which):
                    write(refs[which], *refs[-3:])

            else:
                write(refs[which], *refs[-3:])

    def write(tile, g_o, u_o, d_o):
        step = pl.program_id(2)

        @pl.when(step < 2)
        def _():
            for r in range(8):
                spot = ((r % 2) * 4 + r // 2) * rows
                g_o[spot : spot + rows, :] = tile[r, 0].astype(F32)
                u_o[spot : spot + rows, :] = tile[r, 1].astype(F32)

        @pl.when(step == 2)
        def _():
            for m in range(2):
                parts = [tile[(n % 4) * 2 + n // 4, m] for n in range(8)]
                d_o[:, m * half : (m + 1) * half] = jnp.transpose(jnp.concatenate(parts, axis=0)).astype(F32)

    if routed:
        col = pl.BlockSpec((None, half, block), lambda t, p, o, w: (core(t, w) * 2 + j, 0, column(o, w) * count + p))
        row = pl.BlockSpec((None, block, D), lambda t, p, o, w: (core(t, w) * 2 + j, p, 0))
    else:
        col = pl.BlockSpec((half, block), lambda t, p, o, w: (0, column(o, w) * 2 + core(t, w)))
        row = pl.BlockSpec((block, D), lambda t, p, o, w: (core(t, w), 0))
    before = before or ()
    return pl.pallas_call(
        body,
        cost_estimate=cost,
        grid_spec=pltpu.PrefetchScalarGridSpec(
            num_scalar_prefetch=1,
            grid=(2, count, 3),
            in_specs=tiles + [pl.BlockSpec(memory_space=pl.ANY)] * len(before),
            out_specs=[col, col, row],
        ),
        out_shape=[jax.ShapeDtypeStruct(s, F32) for s in shapes],
        input_output_aliases={1 + len(tiles) + k: k for k in range(len(before))},
        compiler_params=pltpu.CompilerParams(vmem_limit_bytes=40 * MIB),
        name="place",
    )(where, *operands, *before)


def on_device(
    tokens,
    routes,
    pic_block,
    norm1_gain,
    w_query,
    w_key,
    w_value,
    w_out,
    norm2_gain,
    router,
    expert_gate,
    expert_up,
    expert_down,
    shared_gate,
    shared_up,
    shared_down,
    cotangent,
):
    reps = lax.axis_size("rep")
    shards = lax.axis_size("shard")
    rep = lax.axis_index("rep")
    shard = lax.axis_index("shard")
    core = rep % 2
    quarter = (rep // 2) % 4
    length = tokens.shape[0]
    half = D // 2
    experts = router.shape[1]
    per_core = experts // 2

    def swap(value, rep_bit, shard_bit):
        perm = [
            (r * shards + s, (r ^ rep_bit) * shards + (s ^ shard_bit))
            for r in range(reps)
            for s in range(shards)
        ]
        return lax.ppermute(value, ALL, perm)

    def over_core(value):
        return swap(value, 1, 0)

    def over_x(value):
        return swap(value, 0, 1)

    def over_y(value):
        return swap(value, 2, 0)

    def over_z(value, bits):
        return swap(value, 4 * bits, 0)

    def in_order(index, mine, theirs, axis):
        return jnp.where(
            index == 0,
            jnp.concatenate([mine, theirs], axis=axis),
            jnp.concatenate([theirs, mine], axis=axis),
        )

    def later(value, after):
        return lax.optimization_barrier((value, after))[0]

    held = [None]

    def in_turn(call, *args, need=()):
        if held[0] is not None or need:
            args, _, _ = lax.optimization_barrier((args, held[0], need))
        result = call(*args)
        held[0] = result[0] if isinstance(result, (list, tuple)) else result
        return result

    def where_of(expert):
        return jnp.stack(
            [shard, core, expert, quarter, quarter % 2, (rep // 4) % 4]
        ).astype(jnp.int32)

    where = where_of(core * per_core)

    rows_c = functools.partial(lax.dynamic_slice_in_dim, start_index=core * (half // 2), slice_size=half // 2, axis=0)
    tiny = jnp.concatenate([norm1_gain[None], norm2_gain[None], router.T], axis=0)
    tiny = jnp.pad(tiny, ((0, 8 - tiny.shape[0]), (0, 0)))
    tiny_got = over_x(tiny)
    small_mine = over_x(later(jnp.stack([rows_c(w_query), rows_c(w_key), rows_c(w_value), rows_c(w_out)]), tiny_got))
    tiny_full = in_order(shard, tiny, tiny_got, 1)
    gain_one = tiny_full[0:1].astype(F32)
    gain_two = tiny_full[1:2].astype(F32)
    router_t = tiny_full[2 : 2 + experts]
    router_t8 = jnp.pad(router_t, ((0, 8 - experts), (0, 0)))
    router_t128 = jnp.pad(router_t, ((0, 128 - experts), (0, 0)))

    experts_w = (expert_gate, expert_up, expert_down)
    shared_w = (shared_gate, shared_up, shared_down)

    def fetch(weights, units, per, expert, cost=CHEAP, need=()):
        call = functools.partial(pack, units=units, per=per, cost=cost)
        return [over_x(v) for v in in_turn(call, where_of(expert), *weights, need=need)]

    def slot_tables(picks):
        expert_ids = jnp.arange(8)[:, None, None]
        picked = jnp.any(picks.T[None] == expert_ids, axis=1)
        earlier = jnp.arange(length)[:, None] < jnp.arange(length)[None, :]
        rank = jnp.dot(picked.astype(BF), earlier.astype(BF), preferred_element_type=F32)
        return jnp.where(picked, rank.astype(jnp.int32), -1)

    routes_oth = over_core(routes)
    slots = jnp.stack([slot_tables(routes), slot_tables(routes_oth)])
    dys = (cotangent, over_core(cotangent))
    tables = rotary_tables(length)
    routes_t = jnp.pad(routes.T, ((0, 6), (0, 0)))

    first_w = fetch(experts_w, ((0, 0), (1, 0)), 2, core * per_core)
    small_theirs = over_core(later(small_mine, held[0]))
    q, k, v, mixed, lse, wqkv = in_turn(
        attend_forward, where, pic_block, tokens, gain_one, (w_query, w_key, w_value), small_mine, small_theirs, tables,
    )
    first_w = [later(v, q) for v in first_w]
    first_w = (first_w[0], over_y(first_w[0]), first_w[1], over_y(first_w[1]))
    second_w = fetch(experts_w, ((0, 0), (1, 0), (1, 1)), 2, core * per_core + 1)
    resid, n2, n2p, comb, wout = in_turn(
        middle, where, tokens, mixed, w_out, small_mine, small_theirs, gain_two, router_t8, routes_t,
    )
    toks = (n2p, over_core(n2p))
    shared_fetched = fetch(
        shared_w, ((0, 0), (0, 1)), 1, core * per_core, DEAR, (first_w[1], first_w[3], second_w[0])
    )
    second_w = (second_w[0], over_y(second_w[0]), second_w[1], second_w[2])
    combs = jnp.stack([comb, over_core(comb)])

    near = [[h * 16 + r for r in range(16)] for h in range(reps // 16)]
    distant = [[h * 16 + g for h in range(reps // 16)] for g in range(16)]

    def distant_sum(piece):
        if reps > 16:
            flat = piece.reshape(-1, piece.shape[-1])
            flat = lax.psum_scatter(flat, "rep", scatter_dimension=0, tiled=True, axis_index_groups=distant)
            flat = lax.all_gather(flat, "rep", axis=0, tiled=True, axis_index_groups=distant)
            piece = flat.reshape(piece.shape)
        return piece

    def finish(piece):
        return lax.all_gather(distant_sum(piece), "rep", axis=0, tiled=False, axis_index_groups=near)

    def first(pair, cost=CHEAP):
        pair["sums"] = in_turn(functools.partial(pair_first, cost=cost), where, pair["keep"], pair["got"], pair["hold"], pair["got_y"])
        pair["got"] = (over_y(pair["sums"][0]), over_x(pair["sums"][2]))

    def second(pair, cost=CHEAP):
        call = functools.partial(pair_second, cost=cost)
        pair["sums"] = in_turn(call, where, pair["sums"][1], pair["got"][0], pair["sums"][3], pair["got"][1])
        pair["got"] = [pair["sums"][0]] + [over_z(pair["sums"][n], n) for n in range(1, 4)]

    def third(pair, cost=CHEAP):
        pair["piece"] = in_turn(functools.partial(pair_third, cost=cost), where, pair["got"])

    def new_pair(keep, send, hold, push):
        return {"keep": keep, "got": over_x(send), "hold": hold, "got_y": over_y(push)}

    def routing(j):
        expert = core * per_core + j
        slot_row = lax.dynamic_index_in_dim(slots, expert, 1, keepdims=False)
        gate_row = lax.dynamic_index_in_dim(combs, expert, 1, keepdims=False)
        return where_of(expert), (slot_row, slot_row.reshape(-1, 1), gate_row)

    def after_held(values):
        return [later(v, held[0]) for v in values]

    def add_pair(a, b):
        return ((a.astype(F32) + b.astype(F32)).astype(BF),)

    place_a, route_a = routing(0)
    place_b, route_b = routing(1)
    res_a = in_turn(functools.partial(ffn, route=route_a), place_a, toks, dys, *experts_w, first_w)
    pair_a = new_pair(*res_a[3:])
    res_b = in_turn(
        functools.partial(ffn, route=route_b, only=0), place_b, toks, dys, *experts_w, second_w[:2],
        need=tuple(shared_fetched),
    )
    first(pair_a)
    from_early = over_core(in_turn(add_pair, res_a[1], res_b[1])[0])
    pair_b = new_pair(*after_held(res_b[3:]))
    res_c = in_turn(functools.partial(ffn, route=route_b, only=1), place_b, toks, dys, *experts_w, second_w[2:])
    sums = pair_a["sums"]
    scattered = in_turn(pair_scatter, where, sums[1], pair_a["got"][0], sums[3], pair_a["got"][1])
    z_groups = [[h * 16 + z * 4 + g for z in range(4)] for h in range(reps // 16) for g in range(4)]
    piece_a = lax.psum_scatter(scattered, "rep", scatter_dimension=0, tiled=False, axis_index_groups=z_groups)
    gathered = finish(piece_a)
    first(pair_b)
    pair_c = new_pair(*after_held(res_c[3:]))
    res_s = in_turn(functools.partial(ffn, before=res_c[1]), where, toks, dys, *shared_w, shared_fetched)
    parts = [res_a[0], res_b[0], res_c[0], res_s[0], from_early, over_core(res_s[1])]
    dgates = jnp.stack([res_a[2], res_b[2] + res_c[2]])
    dgates_oth = over_core(dgates[:, 1])
    first(pair_c, DEAR)
    dgate = in_order(core, dgates[:, 0], dgates_oth, 0)
    comb_e = comb[:experts]
    dlog_t = (comb_e * (dgate - jnp.sum(comb_e * dgate, axis=0, keepdims=True))).astype(BF)
    dlog = jnp.pad(dlog_t.T, ((0, 0), (0, 128 - experts)))
    output, d_resid, d_low, ggain_two = in_turn(
        join, where, cotangent, resid, gain_two, dlog, router_t128, parts
    )
    grad_router = jnp.dot(dlog_t, n2, preferred_element_type=F32)
    second(pair_b)
    first_keep, first_send, gout_low, d_normed = in_turn(
        attend_backward, where, pic_block, tokens, gain_one, wqkv, wout, tables, q, k, v, mixed, lse, d_low
    )
    third(pair_b)
    second(pair_c)
    pair_s = new_pair(*after_held(res_s[2:]))
    last_keep, last_send, gout_high, input_grad, ggain_one = in_turn(
        attend_backward,
        where, pic_block, tokens, gain_one, wqkv, wout, tables, q, k, v, mixed, lse, d_low, (d_resid, d_normed),
    )

    for_other, for_me = in_turn(
        attention_pack, where, first_keep, first_send, last_keep, last_send, gout_low, gout_high,
        ggain_one, ggain_two, grad_router,
    )
    att_got = over_core(for_other)
    shared_shapes = [shared_gate.shape, shared_up.shape, shared_down.shape]
    expert_shapes = [expert_gate.shape, expert_up.shape, expert_down.shape]
    third(pair_c)
    piece_b = jnp.stack([pair_b["piece"], pair_c["piece"]])
    gathered_b = finish(piece_b.reshape((2, 6) + piece_b.shape[3:]))
    first(pair_s, FAIR)
    expert_grads = in_turn(lambda f: place(where, 0, f, expert_shapes, None, HUGE), gathered)
    att_keep, att_send = in_turn(attention_sum, where, for_me, att_got)
    x_got = over_x(att_send)
    second(pair_s, FAIR)
    y_send, y_keep = in_turn(functools.partial(sum_x, cost=FAIR), where, att_keep, x_got)
    y_got = over_y(y_send)
    third(pair_s, FAIR)
    shared_full = finish(pair_s["piece"])
    quarter_rows = in_turn(functools.partial(sum_y, cost=FAIR), where, y_keep, y_got)
    quarter_rows = [quarter_rows[0]] + [over_z(quarter_rows[n], n) for n in range(1, 4)]
    piece = distant_sum(in_turn(functools.partial(sum_z, cost=FAIR), where, quarter_rows))
    att = [piece] + [over_z(piece, n) for n in range(1, 4)]
    att = att + [over_y(p) for p in att]
    expert_grads = in_turn(
        lambda f, *old: place(where, 1, f, expert_shapes, old, HUGE), gathered_b, *expert_grads
    )
    att = in_turn(assemble, where, att)
    att_oth = over_core(att)
    shared_grads = in_turn(
        lambda f: place(where, None, f, shared_shapes, None),
        shared_full.reshape((16, 1, 6) + shared_full.shape[3:]),
    )
    gq, gk, gv, gout, small_grads = in_turn(attention_unpack, where, att, att_oth)
    return (
        output,
        input_grad,
        small_grads[:, 0],
        gq,
        gk,
        gv,
        gout,
        small_grads[:, 1],
        small_grads[:, 2 : 2 + experts],
        *expert_grads,
        *shared_grads,
    )


def solution(mesh):
    both = P(("rep", "shard"), None)
    rows = P("shard", None)
    vec = P("shard")
    mid = P(None, "shard", None)
    return jax.shard_map(
        on_device,
        mesh=mesh,
        in_specs=(
            both, both, P(("rep", "shard")),
            vec, rows, rows, rows, rows, vec, rows, mid, mid, mid, rows, rows, rows,
            both,
        ),
        out_specs=(both, both, vec, rows, rows, rows, rows, vec, rows, mid, mid, mid, rows, rows, rows),
        check_vma=False,
    )
```

```python
import functools

import jax
import jax.numpy as jnp
from jax import lax
from jax.experimental import pallas as pl
from jax.experimental.pallas import tpu as pltpu
from jax.sharding import PartitionSpec as P

D = 768
HEADS = 12
HEAD_DIM = 64
PIC = 256
CAP = 640
PAIR = 2 * HEAD_DIM
PAIRS = HEADS // 2
QB = 256
EPS = 1e-05
BF = jnp.bfloat16
F32 = jnp.float32
ALL = ("rep", "shard")
MIB = 1 << 20
CHEAP = pl.CostEstimate(flops=1, transcendentals=0, bytes_accessed=1)
DEAR = pl.CostEstimate(flops=1 << 36, transcendentals=0, bytes_accessed=1)
HUGE = pl.CostEstimate(flops=1 << 38, transcendentals=0, bytes_accessed=1)
FAIR = pl.CostEstimate(flops=1 << 34, transcendentals=0, bytes_accessed=1)


def nn(a, b):
    return lax.dot_general(a, b, (((1,), (0,)), ((), ())), preferred_element_type=F32)


def nt(a, b):
    return lax.dot_general(a, b, (((1,), (1,)), ((), ())), preferred_element_type=F32)


def resident(shape):
    zeros = (0,) * len(shape)
    return pl.BlockSpec(shape, lambda *_: zeros, pipeline_mode=pl.Buffered(1))


def rotary_tables(length):
    halfway = HEAD_DIM // 2
    freqs_base = 10000.0 ** (-jnp.arange(halfway, dtype=F32) / halfway)
    angles = jnp.arange(length, dtype=F32)[:, None] * freqs_base[None, :]
    cosine = jnp.cos(angles)
    sine = jnp.sin(angles)
    zero = jnp.zeros_like(sine)
    cos_t = jnp.concatenate([cosine] * 4, axis=1)
    left = jnp.concatenate([-sine, zero, -sine, zero], axis=1)
    right = jnp.concatenate([zero, sine, zero, sine], axis=1)
    return cos_t, left, right


def turned(v, left, right):
    return pltpu.roll(v, 96, 1) * left + pltpu.roll(v, 32, 1) * right


def head_masks(rows):
    lane = lax.broadcasted_iota(jnp.int32, (rows, PAIR), 1)
    return lane < HEAD_DIM, lane >= HEAD_DIM


def attend_forward_body(
    where, pic, tok, gain, wq, wk, wv, mine, theirs, cos_t, left, right,
    q_o, k_o, v_o, mix_o, lse_o, w_o,
    xn,
):
    length = tok.shape[0]
    half = D // 2
    step = pl.program_id(0)

    @pl.when(step == 0)
    def _():
        for lo in range(0, length, QB):
            x = tok[lo : lo + QB, :].astype(F32)
            inv = lax.rsqrt(jnp.mean(x * x, axis=1, keepdims=True) + EPS)
            xn[lo : lo + QB, :] = (x * inv * gain[...]).astype(BF)

    own = pl.ds(pl.multiple_of(where[0] * half, half), half)
    quarter = half // 2
    first = pl.ds(pl.multiple_of((1 - where[0]) * half + where[1] * quarter, quarter), quarter)
    second = pl.ds(pl.multiple_of((1 - where[0]) * half + (1 - where[1]) * quarter, quarter), quarter)
    for m, w in enumerate((wq, wk, wv)):
        cols = slice(m * PAIR, (m + 1) * PAIR)
        w_o[own, cols] = w[...]
        w_o[first, cols] = mine[m]
        w_o[second, cols] = theirs[m]
    for lo in range(0, length, QB):
        rows = slice(lo, lo + QB)
        qkv = nn(xn[rows, :], w_o[...])
        q, k = qkv[:, :PAIR], qkv[:, PAIR : 2 * PAIR]
        c_, l_, r_ = cos_t[rows, :], left[rows, :], right[rows, :]
        q_o[rows, :] = (q * c_ + turned(q, l_, r_)).astype(BF) * jnp.asarray(0.125, BF)
        k_o[rows, :] = (k * c_ + turned(k, l_, r_)).astype(BF)
        v_o[rows, :] = qkv[:, 2 * PAIR :].astype(BF)
    masks = head_masks(QB)
    row = lax.broadcasted_iota(jnp.int32, (QB, QB), 0)
    col = lax.broadcasted_iota(jnp.int32, (QB, QB), 1)
    causal = col <= row
    for block in range(length // QB):
        rows = slice(block * QB, (block + 1) * QB)
        allowed = causal | (pic[0] == block)
        q = q_o[rows, :]
        outs = []
        for head in range(2):
            qm = jnp.where(masks[head], q, jnp.zeros_like(q))
            s_d = jnp.where(allowed, nt(qm, k_o[rows, :]), -1e30)
            top = jnp.max(s_d, axis=1, keepdims=True)
            if block:
                s_o = nt(qm, k_o[: block * QB, :])
                top = jnp.maximum(top, jnp.max(s_o, axis=1, keepdims=True))
            p_d = jnp.exp(s_d - top)
            total = jnp.sum(p_d, axis=1, keepdims=True)
            acc = nn(p_d.astype(BF), v_o[rows, :])
            if block:
                p_o = jnp.exp(s_o - top)
                total = total + jnp.sum(p_o, axis=1, keepdims=True)
                acc = acc + nn(p_o.astype(BF), v_o[: block * QB, :])
            outs.append(acc / total)
            lse = jnp.broadcast_to(top + jnp.log(total), (QB, PAIR))
            lse_o[0, head : head + 1, rows] = jnp.transpose(lse)[0:1, :]
        mix_o[rows, :] = jnp.where(masks[0], outs[0], outs[1]).astype(BF)


def attend_forward(where, pic_block, tokens, gain, weights, mine, theirs, tables):
    length = tokens.shape[0]
    half = D // 2
    pair = pl.BlockSpec((length, PAIR), lambda p: (0, p))
    wide = jax.ShapeDtypeStruct((length, D), BF)
    weight = pl.BlockSpec((half, PAIR), lambda p: (0, p))
    part = pl.BlockSpec((4, half // 2, PAIR), lambda p: (0, 0, p))
    return pl.pallas_call(
        attend_forward_body,
        cost_estimate=DEAR,
        grid=(PAIRS,),
        in_specs=[
            pl.BlockSpec(memory_space=pltpu.SMEM),
            pl.BlockSpec(memory_space=pltpu.SMEM),
            resident((length, D)),
            resident((1, D)),
            weight,
            weight,
            weight,
            part,
            part,
            resident((length, PAIR)),
            resident((length, PAIR)),
            resident((length, PAIR)),
        ],
        out_specs=[
            pair, pair, pair, pair,
            pl.BlockSpec((1, 8, length), lambda p: (p, 0, 0)),
            pl.BlockSpec((D, 3 * PAIR), lambda p: (0, p)),
        ],
        out_shape=[
            wide, wide, wide, wide,
            jax.ShapeDtypeStruct((PAIRS, 8, length), F32),
            jax.ShapeDtypeStruct((D, 3 * D), BF),
        ],
        scratch_shapes=[pltpu.VMEM((length, D), BF)],
        compiler_params=pltpu.CompilerParams(vmem_limit_bytes=48 * MIB),
        name="attend_forward",
    )(where, pic_block, tokens, gain, *weights, mine, theirs, *tables)


def attend_backward_body(
    last, where, pic, tok, gain, wqkv, wout, cos_t, left, right, q_i, k_i, v_i, mix_i, lse_i, dres, *refs
):
    if last:
        dres_f, dxn_i, keep_o, send_o, gout_o, igrad_o, ggain_o = refs[:7]
        refs = refs[7:]
    else:
        keep_o, send_o, gout_o, dxn_o = refs[:4]
        refs = refs[4:]
    xn_t, dxn, dmix, dqkv, dk_s, dv_s, k_t = refs
    length = tok.shape[0]
    half = D // 2
    step = pl.program_id(0)

    @pl.when(step == 0)
    def _():
        for lo in range(0, length, QB):
            x = tok[lo : lo + QB, :].astype(F32)
            inv = lax.rsqrt(jnp.mean(x * x, axis=1, keepdims=True) + EPS)
            n_t = jnp.transpose((x * inv * gain[...]).astype(BF))
            spot = pl.multiple_of(where[0] * half, half)
            xn_t[pl.ds(spot, half), lo : lo + QB] = n_t[:half, :]
            xn_t[pl.ds(half - spot, half), lo : lo + QB] = n_t[half:, :]

    dm = nt(dres[...], wout[...]).astype(BF)
    dmix[...] = dm
    mixed = mix_i[...]
    gout_o[...] = nn(jnp.transpose(mixed), dres[...]).astype(BF)
    prod = jnp.transpose(dm.astype(F32) * mixed.astype(F32))
    delta = (
        jnp.sum(prod[:HEAD_DIM, :], axis=0, keepdims=True),
        jnp.sum(prod[HEAD_DIM:, :], axis=0, keepdims=True),
    )
    k_t[...] = jnp.transpose(k_i[...])
    masks = head_masks(QB)
    key_row = lax.broadcasted_iota(jnp.int32, (QB, QB), 0)
    query_col = lax.broadcasted_iota(jnp.int32, (QB, QB), 1)
    causal = key_row <= query_col
    for block in reversed(range(length // QB)):
        rows = slice(block * QB, (block + 1) * QB)
        first = block == length // QB - 1
        allowed = causal | (pic[0] == block)
        q = q_i[rows, :]
        dm = dmix[rows, :]
        dq_t = []
        parts = {"d": [], "o": []}
        for head in range(2):
            qm = jnp.where(masks[head], q, jnp.zeros_like(q))
            dmm = jnp.where(masks[head], dm, jnp.zeros_like(dm))
            lse = lse_i[0, head : head + 1, rows]
            cent = delta[head][:, rows]
            lanes = slice(head * HEAD_DIM, (head + 1) * HEAD_DIM)
            dq = None
            for part, keys in (("d", rows), ("o", slice(0, block * QB))):
                if part == "o" and block == 0:
                    continue
                st = nt(k_i[keys, :], qm)
                pt = jnp.exp(st - lse)
                if part == "d":
                    pt = jnp.where(allowed, pt, 0.0)
                dpt = nt(v_i[keys, :], dmm)
                dst = (pt * (dpt - cent)).astype(BF)
                parts[part].append((nn(dst, qm), nn(pt.astype(BF), dmm)))
                add = nn(k_t[lanes, keys], dst)
                dq = add if dq is None else dq + add
            dq_t.append(dq)
        for part, keys in (("d", rows), ("o", slice(0, block * QB))):
            if not parts[part]:
                continue
            dk = parts[part][0][0] + parts[part][1][0]
            dv = parts[part][0][1] + parts[part][1][1]
            if first:
                dk_s[keys, :] = dk
                dv_s[keys, :] = dv
            else:
                dk_s[keys, :] = dk_s[keys, :] + dk
                dv_s[keys, :] = dv_s[keys, :] + dv
        dq = jnp.transpose(jnp.concatenate(dq_t, axis=0)) * 0.125
        c_, l_, r_ = cos_t[rows, :], left[rows, :], right[rows, :]
        dqkv[rows, :PAIR] = (dq * c_ - turned(dq, l_, r_)).astype(BF)
        dk = dk_s[rows, :]
        dqkv[rows, PAIR : 2 * PAIR] = (dk * c_ - turned(dk, l_, r_)).astype(BF)
        dqkv[rows, 2 * PAIR :] = dv_s[rows, :].astype(BF)
    gqkv = nn(xn_t[...], dqkv[...]).astype(BF)
    keep_o[...] = gqkv[:half, :]
    send_o[...] = gqkv[half:, :]
    add = nt(dqkv[...], wqkv[...])

    @pl.when(step == 0)
    def _():
        if last:
            dxn[...] = dxn_i[...] + add
        else:
            dxn[...] = add

    @pl.when(step > 0)
    def _():
        dxn[...] = dxn[...] + add

    @pl.when(step == pl.num_programs(0) - 1)
    def _():
        if not last:
            dxn_o[...] = dxn[...]
            return
        total = jnp.zeros((1, D), F32)
        for lo in range(0, length, QB):
            rows = slice(lo, lo + QB)
            x = tok[rows, :].astype(F32)
            inv = lax.rsqrt(jnp.mean(x * x, axis=1, keepdims=True) + EPS)
            n = x * inv
            up = dxn[rows, :]
            total = total + jnp.sum(up * n, axis=0, keepdims=True)
            u = up * gain[...]
            igrad_o[rows, :] = dres_f[rows, :] + inv * (u - n * jnp.mean(u * n, axis=1, keepdims=True))
        ggain_o[...] = total


def attend_backward(where, pic_block, tokens, gain, wqkv, wout, tables, q, k, v, mixed, lse, dres, more=None):
    length = tokens.shape[0]
    half = D // 2
    last = more is not None
    early = 2 * PAIRS // 3
    count = PAIRS - early if last else early
    off = early if last else 0
    pair = pl.BlockSpec((length, PAIR), lambda p: (0, p + off))
    grad = pl.BlockSpec((half, 3 * PAIR), lambda p: (0, p))
    wide = jax.ShapeDtypeStruct((length, D), F32)
    out_specs = [grad, grad, pl.BlockSpec((PAIR, D), lambda p: (p, 0)), resident((length, D))]
    out_shape = [
        jax.ShapeDtypeStruct((half, 3 * PAIR * count), BF),
        jax.ShapeDtypeStruct((half, 3 * PAIR * count), BF),
        jax.ShapeDtypeStruct((PAIR * count, D), BF),
        wide,
    ]
    if last:
        out_specs.append(resident((1, D)))
        out_shape.append(jax.ShapeDtypeStruct((1, D), F32))
    return pl.pallas_call(
        functools.partial(attend_backward_body, last),
        cost_estimate=DEAR,
        grid=(count,),
        in_specs=[
            pl.BlockSpec(memory_space=pltpu.SMEM),
            pl.BlockSpec(memory_space=pltpu.SMEM),
            resident((length, D)),
            resident((1, D)),
            pl.BlockSpec((D, 3 * PAIR), lambda p: (0, p + off)),
            pl.BlockSpec((PAIR, D), lambda p: (p + off, 0)),
            resident((length, PAIR)),
            resident((length, PAIR)),
            resident((length, PAIR)),
            pair, pair, pair, pair,
            pl.BlockSpec((1, 8, length), lambda p: (p + off, 0, 0)),
            resident((length, D)),
        ]
        + ([resident((length, D))] * 2 if last else []),
        out_specs=out_specs,
        out_shape=out_shape,
        scratch_shapes=[
            pltpu.VMEM((D, length), BF),
            pltpu.VMEM((length, D), F32),
            pltpu.VMEM((length, PAIR), BF),
            pltpu.VMEM((length, 3 * PAIR), BF),
            pltpu.VMEM((length, PAIR), F32),
            pltpu.VMEM((length, PAIR), F32),
            pltpu.VMEM((PAIR, length), BF),
        ],
        compiler_params=pltpu.CompilerParams(vmem_limit_bytes=56 * MIB),
        name="attend_backward_2" if last else "attend_backward_1",
    )(where, pic_block, tokens, gain, wqkv, wout, *tables, q, k, v, mixed, lse, dres, *(more or ()))


def middle_body(
    shard, tok, mixed, w_own, w_mine, w_theirs, gain, router_t, routes_t,
    resid_o, n2_o, n2p_o, comb_o, wout,
):
    @pl.when(pl.program_id(0) == 0)
    def _():
        half = D // 2
        quarter = half // 2
        other = (1 - shard[0]) * half
        wout[pl.ds(pl.multiple_of(shard[0] * half, half), half), :] = w_own[...]
        first = pl.multiple_of(other + shard[1] * quarter, quarter)
        second = pl.multiple_of(other + (1 - shard[1]) * quarter, quarter)
        wout[pl.ds(first, quarter), :] = w_mine[...]
        wout[pl.ds(second, quarter), :] = w_theirs[...]

    r = tok[...].astype(F32) + nn(mixed[...], wout[...])
    resid_o[...] = r
    inv = lax.rsqrt(jnp.mean(r * r, axis=1, keepdims=True) + EPS)
    n2 = (r * inv * gain[...]).astype(BF)
    n2_o[...] = n2
    half = D // 2
    swapped = jnp.concatenate([n2[:, half:], n2[:, :half]], axis=1)
    n2p_o[...] = jnp.where(shard[0] == 0, n2, swapped)
    logits = nt(router_t[...], n2)
    expert = lax.broadcasted_iota(jnp.int32, logits.shape, 0)
    picks = [expert == routes_t[k : k + 1, :] for k in range(2)]
    chosen = [jnp.sum(jnp.where(p, logits, 0.0), axis=0, keepdims=True) for p in picks]
    top = jnp.maximum(chosen[0], chosen[1])
    weights = [jnp.exp(v - top) for v in chosen]
    total = weights[0] + weights[1]
    gates = [w / total for w in weights]
    comb_o[...] = jnp.where(picks[0], gates[0], 0.0) + jnp.where(picks[1], gates[1], 0.0)


def middle(where, tokens, mixed, w_own, w_mine, w_theirs, gain, router_t, routes_t):
    length = tokens.shape[0]
    block = 256
    rows = pl.BlockSpec((block, D), lambda i: (i, 0))
    cols = pl.BlockSpec((8, block), lambda i: (0, i))
    return pl.pallas_call(
        middle_body,
        cost_estimate=CHEAP,
        grid=(length // block,),
        in_specs=[
            pl.BlockSpec(memory_space=pltpu.SMEM),
            rows,
            rows,
            resident((D // 2, D)),
            pl.BlockSpec((None, D // 4, D), lambda i: (3, 0, 0), pipeline_mode=pl.Buffered(1)),
            pl.BlockSpec((None, D // 4, D), lambda i: (3, 0, 0), pipeline_mode=pl.Buffered(1)),
            resident((1, D)),
            resident((8, D)),
            cols,
        ],
        out_specs=[rows, rows, rows, cols, resident((D, D))],
        out_shape=[
            jax.ShapeDtypeStruct((length, D), F32),
            jax.ShapeDtypeStruct((length, D), BF),
            jax.ShapeDtypeStruct((length, D), BF),
            jax.ShapeDtypeStruct((8, length), F32),
            jax.ShapeDtypeStruct((D, D), BF),
        ],
        compiler_params=pltpu.CompilerParams(vmem_limit_bytes=40 * MIB),
        name="middle",
    )(where, tokens, mixed, w_own, w_mine, w_theirs, gain, router_t, routes_t)


def join_body(shard, dy, resid, gain, dlog, router_t, *refs):
    parts = refs[:-4]
    out_o, dres_o, dlow_o, ggain_o = refs[-4:]
    r = resid[...]
    total = r
    for part in parts:
        total = total + part[0].astype(F32)
    out_o[...] = total.astype(BF)
    up = parts[0][1].astype(F32)
    for part in parts[1:]:
        up = up + part[1].astype(F32)
    half = D // 2
    swapped = jnp.concatenate([up[:, half:], up[:, :half]], axis=1)
    up = jnp.where(shard[0] == 0, up, swapped)
    up = up + nn(dlog[...], router_t[...])
    inv = lax.rsqrt(jnp.mean(r * r, axis=1, keepdims=True) + EPS)
    n = r * inv
    add = jnp.sum(up * n, axis=0, keepdims=True)

    @pl.when(pl.program_id(0) == 0)
    def _():
        ggain_o[...] = add

    @pl.when(pl.program_id(0) > 0)
    def _():
        ggain_o[...] = ggain_o[...] + add

    u = up * gain[...]
    d = dy[...].astype(F32) + inv * (u - n * jnp.mean(u * n, axis=1, keepdims=True))
    dres_o[...] = d
    dlow_o[...] = d.astype(BF)


def join(shard, dy, resid, gain, dlog, router_t, parts):
    length = dy.shape[0]
    block = 256
    rows = pl.BlockSpec((block, D), lambda i: (i, 0))

    return pl.pallas_call(
        join_body,
        cost_estimate=CHEAP,
        grid=(length // block,),
        in_specs=[
            pl.BlockSpec(memory_space=pltpu.SMEM),
            rows,
            rows,
            resident((1, D)),
            pl.BlockSpec((block, 128), lambda i: (i, 0)),
            resident((128, D)),
        ]
        + [pl.BlockSpec((2, block, D), lambda i: (0, i, 0))] * len(parts),
        out_specs=[rows, rows, rows, pl.BlockSpec((1, D), lambda i: (0, 0))],
        out_shape=[
            jax.ShapeDtypeStruct((length, D), BF),
            jax.ShapeDtypeStruct((length, D), F32),
            jax.ShapeDtypeStruct((length, D), BF),
            jax.ShapeDtypeStruct((1, D), F32),
        ],
        compiler_params=pltpu.CompilerParams(vmem_limit_bytes=40 * MIB),
        name="join",
    )(shard, dy, resid, gain, dlog, router_t, *parts)


def ffn_body(routed, steps, chunk, before, where, tok_a, tok_b, dy_a, dy_b, *refs):
    tok, dy = (tok_a, tok_b), (dy_a, dy_b)
    if routed:
        slot_row, slot_col, gate_row = refs[:3]
        refs = refs[3:]
    g_own, u_own, d_own = refs[:3]
    per = steps // 2
    gu_oth = refs[3 : 3 + 2 * per]
    d_oth = refs[3 + 2 * per : 3 + 4 * per]
    refs = refs[3 + 4 * per :]
    if before:
        theirs_i = refs[0]
        refs = refs[1:]
    sides = refs[:2]
    refs = refs[2:]
    if routed:
        dgate_o = refs[0]
        refs = refs[1:]
    keep, send, hold_y, push_y = refs[:4]
    refs = refs[4:]
    wg, wu, wd, y_acc, dx_acc, hid_s, dg_s, du_s, x_t, de_t = refs[:10]
    refs = refs[10:]
    i = pl.program_id(0)
    srcs, length = 2, tok_a.shape[0]
    rows_all = y_acc.shape[0]
    hold = rows_all // srcs
    half = D // 2
    if routed:
        x_s, de_s, dys, gate_s = refs
    tile = 128

    @pl.when(i == 0)
    def _():
        for src in range(srcs):
            if routed:
                for lo in range(0, hold, tile):
                    slot = lax.broadcasted_iota(jnp.int32, (tile, length), 0) + lo
                    mine = slot == slot_row[src : src + 1, :]
                    pick = jnp.where(mine, 1.0, 0.0).astype(BF)
                    rows = slice(src * hold + lo, src * hold + lo + tile)
                    x = nn(pick, tok[src][...]).astype(BF)
                    d_raw = nn(pick, dy[src][...])
                    gate = jnp.sum(jnp.where(mine, gate_row[src : src + 1, :], 0.0), axis=1, keepdims=True)
                    gate_s[rows, :] = jnp.broadcast_to(gate, (tile, 128))
                    d_e = (d_raw * gate).astype(BF)
                    x_s[rows, :] = x
                    dys[rows, :] = d_raw.astype(BF)
                    de_s[rows, :] = d_e
                    x_t[:, rows] = jnp.transpose(x)
                    de_t[:, rows] = jnp.transpose(d_e)
            else:
                for lo in range(0, hold, 256):
                    rows = slice(src * hold + lo, src * hold + lo + 256)
                    x_t[:, rows] = jnp.transpose(tok[src][lo : lo + 256, :])
                    de_t[:, rows] = jnp.transpose(dy[src][lo : lo + 256, :])

    wg[:half, :] = g_own[...]
    wu[:half, :] = u_own[...]
    part = half // 2
    block = wd.shape[0]
    for p in range(per):

        @pl.when(i // 2 == p)
        def _(p=p):
            for k in range(2):
                spot = pl.ds(pl.multiple_of(half + (where[3] ^ k) * part, part), part)
                ref = gu_oth[2 * p + k]
                for h in range(2):
                    lanes = slice(h * 256, (h + 1) * 256)
                    wg[spot, lanes] = ref[2 * h * part : (2 * h + 1) * part, :]
                    wu[spot, lanes] = ref[(2 * h + 1) * part : (2 * h + 2) * part, :]

    @pl.when(i % 2 == 0)
    def _():
        wd[...] = d_own[...]

    for p in range(per):

        @pl.when(i == 2 * p + 1)
        def _(p=p):
            for k in range(2):
                spot = pl.ds(pl.multiple_of((where[3] ^ k) * (block // 2), block // 2), block // 2)
                for h in range(3):
                    wd[spot, h * 256 : (h + 1) * 256] = d_oth[2 * p + k][h * 256 : (h + 1) * 256, :]

    def piece(j, src, first):
        inner = pl.ds(pl.multiple_of(j * chunk, chunk), chunk)
        if routed:
            rows = inner
            x, de = x_s[rows, :], de_s[rows, :]
        else:
            rows = pl.ds(pl.multiple_of(src * length + j * chunk, chunk), chunk)
            x, de = tok[src][inner, :], dy[src][inner, :]
        g = nn(x, wg[...])
        u = nn(x, wu[...])
        dh = nt(de, wd[...])
        s = 1.0 / (1.0 + jnp.exp(-g))
        act = g * s
        hid = (act * u).astype(BF)
        du = (dh * act).astype(BF)
        dg = (dh * u * s * (1.0 + g * (1.0 - s))).astype(BF)
        hid_s[rows, :] = hid
        dg_s[rows, :] = dg
        du_s[rows, :] = du
        y = nn(hid, wd[...])
        dx = nt(dg, wg[...]) + nt(du, wu[...])
        if first:
            y_acc[rows, :] = y
            dx_acc[rows, :] = dx
        else:
            y_acc[rows, :] = y_acc[rows, :] + y
            dx_acc[rows, :] = dx_acc[rows, :] + dx

    for first in (True, False):

        @pl.when((i == 0) == first)
        def _(first=first):
            for src in range(1 if routed else srcs):

                @pl.loop(0, (rows_all if routed else length) // chunk)
                def _(j, src=src, first=first):
                    piece(j, src, first)

    gg = nn(x_t[...], dg_s[...]).astype(BF)
    gu = nn(x_t[...], du_s[...]).astype(BF)
    gd = nn(de_t[...], hid_s[...]).astype(BF)
    for p in range(per):

        def put(side, tile, value, p=p):
            count = keep.shape[0]
            number = 6 * p + tile
            if number < count:
                (keep, send)[side][number] = value
            else:
                top, low = value[: half // 2, :], value[half // 2 :, :]
                hold_y[side, number - count] = jnp.where(where[4] == 0, top, low)
                push_y[side, number - count] = jnp.where(where[4] == 0, low, top)

        @pl.when(i == 2 * p)
        def _(put=put):
            put(0, 0, gg[:half, :])
            put(0, 1, gu[:half, :])
            put(0, 2, gd[:half, :])
            put(0, 3, gd[half:, :])
            put(1, 4, gg[half:, :])
            put(1, 5, gu[half:, :])

        @pl.when(i == 2 * p + 1)
        def _(put=put):
            put(0, 4, gg[:half, :])
            put(0, 5, gu[:half, :])
            put(1, 0, gg[half:, :])
            put(1, 1, gu[half:, :])
            put(1, 2, gd[:half, :])
            put(1, 3, gd[half:, :])

    @pl.when(i == steps - 1)
    def _():
        for src in range(srcs):
            if routed:
                total = jnp.zeros((1, length), F32)
                for lo in range(0, hold, tile):
                    rows = slice(src * hold + lo, src * hold + lo + tile)
                    y = y_acc[rows, :]
                    dgate = jnp.sum(dys[rows, :].astype(F32) * y, axis=1, keepdims=True)
                    slot = lax.broadcasted_iota(jnp.int32, (tile, length), 0) + lo
                    mine = slot == slot_row[src : src + 1, :]
                    total = total + jnp.sum(jnp.where(mine, dgate, 0.0), axis=0, keepdims=True)
                    x_s[rows, :] = (y * gate_s[rows, 0:1]).astype(BF)
                    de_s[rows, :] = dx_acc[rows, :].astype(BF)
                dgate_o[src : src + 1, :] = total
                held = slice(src * hold, (src + 1) * hold)
                for lo in range(0, length, tile):
                    slot = lax.broadcasted_iota(jnp.int32, (tile, hold), 1)
                    mine = slot == slot_col[src * length + lo : src * length + lo + tile, :]
                    pick = jnp.where(mine, 1.0, 0.0).astype(BF)
                    sides[src][0, lo : lo + tile, :] = nn(pick, x_s[held, :]).astype(BF)
                    sides[src][1, lo : lo + tile, :] = nn(pick, de_s[held, :]).astype(BF)
            else:
                held = slice(src * hold, (src + 1) * hold)
                for n, acc in enumerate((y_acc, dx_acc)):
                    total = acc[held, :]
                    if before and src == 1:
                        total = total + theirs_i[n].astype(F32)
                    sides[src][n] = total.astype(BF)


def ffn(where, toks, dys, gate, up, down, others, route=None, only=None, before=None):
    routed = route is not None
    srcs, length = 2, toks[0].shape[0]
    block = 512
    half = D // 2
    per = len(others) // 2
    total, start = (2, only) if only is not None else (per, 0)
    steps = 2 * per
    rows_all = srcs * (CAP if routed else length)
    chunk = 256

    def column(i, w):
        return (i % 2 + w[0] - 2 * w[0] * (i % 2)) * total + i // 2 + start

    if routed:
        gate_spec = pl.BlockSpec((None, half, block), lambda i, w: (w[2], 0, column(i, w)))
        down_spec = pl.BlockSpec((None, block, D), lambda i, w: (w[2], i // 2 + start, 0))
    else:
        gate_spec = pl.BlockSpec((half, block), lambda i, w: (0, column(i, w) * 2 + w[1]))
        down_spec = pl.BlockSpec((block, D), lambda i, w: (w[1], 0))
    def shard_block(i, w):
        return i % 2 + w[0] - 2 * w[0] * (i % 2)

    def gu_spec(p):
        first, last = 2 * p, 2 * p + 1
        return pl.BlockSpec((2 * half, 256), lambda i, w: (shard_block(jnp.clip(i, first, last), w), 0))

    d_spec = pl.BlockSpec((2 * half, 256), lambda i, w: (2, 0), pipeline_mode=pl.Buffered(1))
    in_specs = [resident((length, D))] * 4
    operands = [*toks, *dys]
    if routed:
        in_specs += [resident(r.shape) for r in route]
        operands += list(route)
    in_specs += [gate_spec, gate_spec, down_spec] + [gu_spec(n // 2) for n in range(2 * per)] + [d_spec] * (2 * per)
    operands += [gate, up, down, *others, *others]
    if before is not None:
        in_specs.append(resident(before.shape))
        operands.append(before)
    wide = jax.ShapeDtypeStruct((srcs, length, D), BF)
    out_specs = [resident((srcs, length, D)), resident((srcs, length, D))]
    out_shape = [wide, wide]
    if routed:
        out_specs.append(resident((srcs, length)))
        out_shape.append(jax.ShapeDtypeStruct((srcs, length), F32))
    for shape in ((3 * per, half, block), (2, 3 * per, half // 2, block)):
        out_specs += [resident(shape)] * 2
        out_shape += [jax.ShapeDtypeStruct(shape, BF)] * 2
    scratch = [
        pltpu.VMEM((D, block), BF),
        pltpu.VMEM((D, block), BF),
        pltpu.VMEM((block, D), BF),
        pltpu.VMEM((rows_all, D), F32),
        pltpu.VMEM((rows_all, D), F32),
        pltpu.VMEM((rows_all, block), BF),
        pltpu.VMEM((rows_all, block), BF),
        pltpu.VMEM((rows_all, block), BF),
        pltpu.VMEM((D, rows_all), BF),
        pltpu.VMEM((D, rows_all), BF),
    ]
    if routed:
        scratch += [
            pltpu.VMEM((rows_all, D), BF),
            pltpu.VMEM((rows_all, D), BF),
            pltpu.VMEM((rows_all, D), BF),
            pltpu.VMEM((rows_all, 128), F32),
        ]
    return pl.pallas_call(
        functools.partial(ffn_body, routed, steps, chunk, before is not None),
        cost_estimate=DEAR,
        grid_spec=pltpu.PrefetchScalarGridSpec(
            num_scalar_prefetch=1,
            grid=(steps,),
            in_specs=in_specs,
            out_specs=out_specs,
            scratch_shapes=scratch,
        ),
        out_shape=out_shape,
        compiler_params=pltpu.CompilerParams(vmem_limit_bytes=63 * MIB),
        name="ffn_routed" if routed else "ffn_shared",
    )(where, *operands)


def add(a, b):
    return a[...].astype(F32) + b[...].astype(F32)


def small_call(body, name, where, grid, ins, outs, cost=CHEAP):
    return pl.pallas_call(
        body,
        cost_estimate=cost,
        grid_spec=pltpu.PrefetchScalarGridSpec(
            num_scalar_prefetch=1,
            grid=grid,
            in_specs=[pl.BlockSpec(block, index) for _, block, index in ins],
            out_specs=[pl.BlockSpec(block, index) for _, block, index in outs],
        ),
        out_shape=[jax.ShapeDtypeStruct(shape, BF) for shape, _, _ in outs],
        compiler_params=pltpu.CompilerParams(vmem_limit_bytes=32 * MIB),
        name=name,
    )(where, *[array for array, _, _ in ins])


def sum_x(where, keep, got, cost=CHEAP):
    tiles, rows, cols = keep.shape
    block = (1, rows // 2, cols)

    def mine(t, w):
        return (t, w[4], 0)

    def other(t, w):
        return (t, 1 - w[4], 0)

    def body(w, k_m, g_m, k_o, g_o, send, hold):
        hold[...] = add(k_m, g_m).astype(BF)
        send[...] = add(k_o, g_o).astype(BF)

    ins = [(keep, block, mine), (got, block, mine), (keep, block, other), (got, block, other)]
    shape = (tiles, rows // 2, cols)
    here = (shape, block, lambda t, w: (t, 0, 0))
    return small_call(body, "sum_x", where, (tiles,), ins, [here, here], cost)


def sum_y(where, keep, got, cost=CHEAP):
    tiles, rows, cols = keep.shape
    step = 3 if tiles % 3 == 0 else 1
    block = (step, rows // 4, cols)

    def body(w, *refs):
        for k in range(4):
            refs[8 + k][...] = add(refs[k], refs[4 + k]).astype(BF)

    spots = [lambda t, w, k=k: (t, w[5] ^ k, 0) for k in range(4)]
    ins = [(keep, block, s) for s in spots] + [(got, block, s) for s in spots]
    here = ((tiles, rows // 4, cols), block, lambda t, w: (t, 0, 0))
    return small_call(body, "sum_y", where, (tiles // step,), ins, [here] * 4, cost)


def sum_z(where, parts, cost=CHEAP):
    shape = parts[0].shape
    step = 3 if shape[0] % 3 == 0 else 1
    block = (step,) + shape[1:]

    def body(w, a, b, c, d, out):
        out[...] = (add(a, b) + add(c, d)).astype(BF)

    def at(t, w):
        return (t, 0, 0)

    ins = [(p, block, at) for p in parts]
    return small_call(body, "sum_z", where, (shape[0] // step,), ins, [(shape, block, at)], cost)[0]


def pack(where, gate, up, down, units, per, cost=CHEAP):
    half = D // 2
    part = half // 2
    routed = gate.ndim == 3

    def body(w, *refs):
        for n in range(len(units)):
            g, u, d = refs[3 * n : 3 * n + 3]
            out = refs[3 * len(units) + n]

            @pl.when(pl.program_id(0) < 2)
            def _(g=g, u=u, out=out):
                for h in range(2):
                    for m, ref in enumerate((g, u)):
                        spot = (2 * h + m) * part
                        out[spot : spot + part, :] = ref[:, h * 256 : (h + 1) * 256]

            @pl.when(pl.program_id(0) == 2)
            def _(d=d, out=out):
                for h in range(3):
                    out[h * 256 : (h + 1) * 256, :] = d[:, h * 256 : (h + 1) * 256]

    in_specs = []
    for p, flip in units:

        def col_block(b, p=p):
            return jnp.minimum(b, 1) * per + p

        if routed:
            col = pl.BlockSpec((None, part, 512), lambda b, w, c=col_block, f=flip: (w[2], w[3] ^ f, c(b)))
            row = pl.BlockSpec((None, 256, D), lambda b, w, p=p, f=flip: (w[2], p * 2 + (w[3] ^ f), 0))
        else:
            col = pl.BlockSpec((part, 512), lambda b, w, c=col_block, f=flip: (w[3] ^ f, c(b) * 2 + w[1]))
            row = pl.BlockSpec((256, D), lambda b, w, f=flip: (w[1] * 2 + (w[3] ^ f), 0))
        in_specs += [col, col, row]
    out = pl.BlockSpec((2 * half, 256), lambda b, w: (b, 0))
    return pl.pallas_call(
        body,
        cost_estimate=cost,
        grid_spec=pltpu.PrefetchScalarGridSpec(
            num_scalar_prefetch=1, grid=(3,), in_specs=in_specs, out_specs=[out] * len(units)
        ),
        out_shape=[jax.ShapeDtypeStruct((6 * half, 256), BF)] * len(units),
        name="pack",
    )(where, *[gate, up, down] * len(units))


def pair_first(where, keep, got, hold, got_y, cost=CHEAP):
    tiles, rows, cols = keep.shape
    block = (1, rows // 2, cols)
    both = (2, 1, rows // 2, cols)

    def mine(t, w):
        return (t, w[4], 0)

    def other(t, w):
        return (t, 1 - w[4], 0)

    def two(t, w):
        return (0, t, 0, 0)

    def body(w, k_m, g_m, k_o, g_o, h, g, y_send, y_keep, x_send, x_keep):
        y_keep[...] = add(k_m, g_m).astype(BF)
        y_send[...] = add(k_o, g_o).astype(BF)
        total = add(h, g).astype(BF)
        x_keep[...] = total[0]
        x_send[...] = total[1]

    ins = [(keep, block, mine), (got, block, mine), (keep, block, other), (got, block, other)]
    ins += [(hold, both, two), (got_y, both, two)]
    here = ((tiles, rows // 2, cols), block, lambda t, w: (t, 0, 0))
    return small_call(body, "pair_first", where, (tiles,), ins, [here] * 4, cost)


def pair_second(where, a, b, c, d, cost=CHEAP):
    tiles, rows, cols = a.shape
    block = (3, rows // 4, cols)

    def body(w, *refs):
        for k in range(4):
            a_, b_, c_, d_ = refs[4 * k : 4 * k + 4]
            refs[16 + k][0] = add(a_, b_).astype(BF)
            refs[16 + k][1] = add(c_, d_).astype(BF)

    ins = []
    for k in range(4):
        ins += [(x, block, lambda t, w, k=k: (t, w[5] ^ k, 0)) for x in (a, b, c, d)]
    out = ((2, tiles) + block[1:], (2,) + block, lambda t, w: (0, t, 0, 0))
    return small_call(body, "pair_second", where, (tiles // 3,), ins, [out] * 4, cost)


def pair_scatter(where, a, b, c, d):
    tiles, rows, cols = a.shape
    block = (tiles, rows // 4, cols)

    def body(w, a_, b_, c_, d_, out):
        out[0] = add(a_, b_).astype(BF)
        out[1] = add(c_, d_).astype(BF)

    ins = [(x, block, lambda t, w: (0, t, 0)) for x in (a, b, c, d)]
    out = ((4, 2) + block, (None, 2) + block, lambda t, w: (t, 0, 0, 0, 0))
    return small_call(body, "pair_scatter", where, (4,), ins, [out])[0]


def pair_third(where, parts, cost=CHEAP):
    shape = parts[0].shape
    block = (None,) + shape[1:]

    def body(w, a, b, c, d, out):
        out[...] = (add(a, b) + add(c, d)).astype(BF)

    def at(n, w):
        return (n, 0, 0, 0)

    return small_call(body, "pair_third", where, (2,), [(p, block, at) for p in parts], [(shape, block, at)], cost)[0]


def attention_pack(where, first_keep, first_send, last_keep, last_send, gout_low, gout_high, gain_a, gain_b, router_g):
    half = D // 2
    wide = 2 * D + 128

    def body(w, lk, ls, hk, hs, gl, gh, ga, gb, gr, other, mine, rows, turned_rows):
        rows[...] = jnp.zeros(rows.shape, F32)
        rows[0:1, :] = ga[...]
        rows[1:2, :] = gb[...]
        rows[2 : 2 + gr.shape[0], :] = gr[...]
        turned_rows[...] = jnp.transpose(rows[...]).astype(BF)
        split = lk.shape[1]
        cut = wide - split
        rest = hk.shape[1] - cut
        for side, (low, high) in enumerate(((lk, hk), (ls, hs))):
            spot = pl.multiple_of((w[0] ^ side) * half, half)
            more = turned_rows[pl.ds(spot, half), :]
            for core in range(2):

                @pl.when(w[1] == core)
                def _(core=core, low=low, high=high, side=side, more=more):
                    first, last = (mine, other) if core == 0 else (other, mine)
                    first[side, :, :split] = low[...]
                    first[side, :, split:] = high[:, :cut]
                    last[side, :, :rest] = high[:, cut:]
                    last[side, :, rest + D : rest + D + 128] = more
                    last[side, :, rest + D + 128 :] = jnp.zeros((half, wide - rest - D - 128), BF)

            for core in range(2):
                for part in range(2):

                    @pl.when((w[1] == core) & ((w[0] ^ side) == part))
                    def _(core=core, part=part, side=side):
                        last = (other, mine)[core]
                        if part == 0:
                            last[side, :, rest : rest + D] = gl[:half, :]
                        else:
                            count = gl.shape[0] - half
                            last[side, :count, rest : rest + D] = gl[half:, :]
                            last[side, count:, rest : rest + D] = gh[...]

    last_core = (first_keep, first_send, last_keep, last_send, gout_low, gout_high, gain_a, gain_b, router_g)
    out = resident((2, half, wide))
    return pl.pallas_call(
        body,
        cost_estimate=CHEAP,
        grid_spec=pltpu.PrefetchScalarGridSpec(
            num_scalar_prefetch=1,
            grid=(1,),
            in_specs=[resident(v.shape) for v in last_core],
            out_specs=[out, out],
            scratch_shapes=[pltpu.VMEM((128, D), F32), pltpu.VMEM((D, 128), BF)],
        ),
        out_shape=[jax.ShapeDtypeStruct((2, half, wide), BF)] * 2,
        compiler_params=pltpu.CompilerParams(vmem_limit_bytes=40 * MIB),
        name="attention_pack",
    )(where, *last_core)


def attention_sum(where, mine, got):
    block = (1,) + mine.shape[1:]

    def body(w, a, b, c, d, keep, send):
        keep[...] = add(a, b).astype(BF)
        send[...] = add(c, d).astype(BF)

    ins = [(v, block, lambda t, w, n=n: (n, 0, 0)) for n in range(2) for v in (mine, got)]
    out = (block, block, lambda t, w: (0, 0, 0))
    return small_call(body, "attention_sum", where, (1,), ins, [out, out])


def attention_unpack(where, mine, theirs):
    half, wide = mine.shape[1:]

    def body(w, m, t, *outs):
        for core in range(2):

            @pl.when(w[1] == core)
            def _(core=core):
                both = (m, t) if core == 0 else (t, m)

                def cols(lo):
                    return both[lo // wide][0, :, lo % wide : lo % wide + 128].astype(F32)

                for pair in range(PAIRS):
                    for n in range(3):
                        outs[n][:, pair * PAIR : (pair + 1) * PAIR] = cols((3 * pair + n) * PAIR)
                for n in range(D // 128):
                    outs[3][:, n * 128 : (n + 1) * 128] = cols(3 * D + n * 128)
                outs[4][...] = cols(4 * D)

    shapes = [(half, D)] * 4 + [(half, 128)]
    return pl.pallas_call(
        body,
        cost_estimate=CHEAP,
        grid_spec=pltpu.PrefetchScalarGridSpec(
            num_scalar_prefetch=1,
            grid=(1,),
            in_specs=[resident(mine.shape)] * 2,
            out_specs=[resident(v) for v in shapes],
        ),
        out_shape=[jax.ShapeDtypeStruct(v, F32) for v in shapes],
        compiler_params=pltpu.CompilerParams(vmem_limit_bytes=40 * MIB),
        name="attention_unpack",
    )(where, mine, theirs)


def assemble(where, pieces):
    tiles, rows, cols = pieces[0].shape
    block = (tiles, rows, cols)

    def body(w, *refs):
        for k in range(8):

            @pl.when(pl.program_id(0) == k)
            def _(k=k):
                refs[8][...] = refs[k][...]

    ins = [(p, block, lambda t, w: (0, 0, 0)) for p in pieces]
    out = ((tiles, 8 * rows, cols), block, lambda t, w: (0, t ^ (w[4] * 4 + w[5]), 0))
    return small_call(body, "assemble", where, (8,), ins, [out])[0]


def place(where, j, full, shapes, before, cost=CHEAP):
    paired = isinstance(full, (list, tuple))
    count, _, rows, block = (full[0] if paired else full).shape[1:]
    half = 8 * rows
    routed = j is not None

    def core(t, w):
        return t + w[1] - 2 * t * w[1]

    def column(o, w):
        o = jnp.minimum(o, 1)
        return o + w[0] - 2 * o * w[0]

    def pick(o):
        return jnp.where(o == 0, 0, 3 - o)

    if paired:
        operands = list(full)

        def mine(t, p, o, w):
            return (0, jnp.where(t == 0, p, count - 1), jnp.where(t == 0, pick(o), 1), 0, 0)

        def theirs(t, p, o, w):
            return (0, jnp.where(t == 0, 0, p), jnp.where(t == 0, 0, pick(o)), 0, 0)

        tiles = [pl.BlockSpec((8, None, 2, rows, block), index) for index in (mine, theirs)]
    else:
        operands = [full.reshape((8, 2) + full.shape[1:])]
        tiles = [
            pl.BlockSpec((8, None, None, 2, rows, block), lambda t, p, o, w: (0, core(t, w), p, pick(o), 0, 0))
        ]

    def body(w, *refs):
        for which in range(len(tiles)):
            if paired:

                @pl.when(pl.program_id(0) == which)
                def _(which=which):
                    write(refs[which], *refs[-3:])

            else:
                write(refs[which], *refs[-3:])

    def write(tile, g_o, u_o, d_o):
        step = pl.program_id(2)

        @pl.when(step < 2)
        def _():
            for r in range(8):
                spot = ((r % 2) * 4 + r // 2) * rows
                g_o[spot : spot + rows, :] = tile[r, 0].astype(F32)
                u_o[spot : spot + rows, :] = tile[r, 1].astype(F32)

        @pl.when(step == 2)
        def _():
            for m in range(2):
                parts = [tile[(n % 4) * 2 + n // 4, m] for n in range(8)]
                d_o[:, m * half : (m + 1) * half] = jnp.transpose(jnp.concatenate(parts, axis=0)).astype(F32)

    if routed:
        col = pl.BlockSpec((None, half, block), lambda t, p, o, w: (core(t, w) * 2 + j, 0, column(o, w) * count + p))
        row = pl.BlockSpec((None, block, D), lambda t, p, o, w: (core(t, w) * 2 + j, p, 0))
    else:
        col = pl.BlockSpec((half, block), lambda t, p, o, w: (0, column(o, w) * 2 + core(t, w)))
        row = pl.BlockSpec((block, D), lambda t, p, o, w: (core(t, w), 0))
    before = before or ()
    return pl.pallas_call(
        body,
        cost_estimate=cost,
        grid_spec=pltpu.PrefetchScalarGridSpec(
            num_scalar_prefetch=1,
            grid=(2, count, 3),
            in_specs=tiles + [pl.BlockSpec(memory_space=pl.ANY)] * len(before),
            out_specs=[col, col, row],
        ),
        out_shape=[jax.ShapeDtypeStruct(s, F32) for s in shapes],
        input_output_aliases={1 + len(tiles) + k: k for k in range(len(before))},
        compiler_params=pltpu.CompilerParams(vmem_limit_bytes=40 * MIB),
        name="place",
    )(where, *operands, *before)


def on_device(
    tokens,
    routes,
    pic_block,
    norm1_gain,
    w_query,
    w_key,
    w_value,
    w_out,
    norm2_gain,
    router,
    expert_gate,
    expert_up,
    expert_down,
    shared_gate,
    shared_up,
    shared_down,
    cotangent,
):
    reps = lax.axis_size("rep")
    shards = lax.axis_size("shard")
    rep = lax.axis_index("rep")
    shard = lax.axis_index("shard")
    core = rep % 2
    quarter = (rep // 2) % 4
    length = tokens.shape[0]
    half = D // 2
    experts = router.shape[1]
    per_core = experts // 2

    def swap(value, rep_bit, shard_bit):
        perm = [
            (r * shards + s, (r ^ rep_bit) * shards + (s ^ shard_bit))
            for r in range(reps)
            for s in range(shards)
        ]
        return lax.ppermute(value, ALL, perm)

    def over_core(value):
        return swap(value, 1, 0)

    def over_x(value):
        return swap(value, 0, 1)

    def over_y(value):
        return swap(value, 2, 0)

    def over_z(value, bits):
        return swap(value, 4 * bits, 0)

    def in_order(index, mine, theirs, axis):
        return jnp.where(
            index == 0,
            jnp.concatenate([mine, theirs], axis=axis),
            jnp.concatenate([theirs, mine], axis=axis),
        )

    def later(value, after):
        return lax.optimization_barrier((value, after))[0]

    held = [None]

    def in_turn(call, *args, need=()):
        if held[0] is not None or need:
            args, _, _ = lax.optimization_barrier((args, held[0], need))
        result = call(*args)
        held[0] = result[0] if isinstance(result, (list, tuple)) else result
        return result

    def where_of(expert):
        return jnp.stack(
            [shard, core, expert, (quarter ^ (quarter // 2)) % 2, quarter % 2, (rep // 4) % 4]
        ).astype(jnp.int32)

    where = where_of(core * per_core)

    rows_c = functools.partial(lax.dynamic_slice_in_dim, start_index=core * (half // 2), slice_size=half // 2, axis=0)
    tiny = jnp.concatenate([norm1_gain[None], norm2_gain[None], router.T], axis=0)
    tiny = jnp.pad(tiny, ((0, 8 - tiny.shape[0]), (0, 0)))
    tiny_got = over_x(tiny)
    small_mine = over_x(later(jnp.stack([rows_c(w_query), rows_c(w_key), rows_c(w_value), rows_c(w_out)]), tiny_got))
    tiny_full = in_order(shard, tiny, tiny_got, 1)
    gain_one = tiny_full[0:1].astype(F32)
    gain_two = tiny_full[1:2].astype(F32)
    router_t = tiny_full[2 : 2 + experts]
    router_t8 = jnp.pad(router_t, ((0, 8 - experts), (0, 0)))
    router_t128 = jnp.pad(router_t, ((0, 128 - experts), (0, 0)))

    experts_w = (expert_gate, expert_up, expert_down)
    shared_w = (shared_gate, shared_up, shared_down)

    def fetch(weights, units, per, expert, cost=CHEAP, need=()):
        call = functools.partial(pack, units=units, per=per, cost=cost)
        return [over_x(v) for v in in_turn(call, where_of(expert), *weights, need=need)]

    def slot_tables(picks):
        expert_ids = jnp.arange(8)[:, None, None]
        picked = jnp.any(picks.T[None] == expert_ids, axis=1)
        earlier = jnp.arange(length)[:, None] < jnp.arange(length)[None, :]
        rank = jnp.dot(picked.astype(BF), earlier.astype(BF), preferred_element_type=F32)
        return jnp.where(picked, rank.astype(jnp.int32), -1)

    routes_oth = over_core(routes)
    slots = jnp.stack([slot_tables(routes), slot_tables(routes_oth)])
    dys = (cotangent, over_core(cotangent))
    tables = rotary_tables(length)
    routes_t = jnp.pad(routes.T, ((0, 6), (0, 0)))

    first_w = fetch(experts_w, ((0, 0), (1, 0)), 2, core * per_core)
    small_theirs = over_core(later(small_mine, held[0]))
    q, k, v, mixed, lse, wqkv = in_turn(
        attend_forward, where, pic_block, tokens, gain_one, (w_query, w_key, w_value), small_mine, small_theirs, tables,
    )
    first_w = [later(v, q) for v in first_w]
    first_w = (first_w[0], over_y(first_w[0]), first_w[1], over_z(first_w[1], 1))
    second_w = fetch(experts_w, ((0, 0), (1, 0)), 2, core * per_core + 1)
    resid, n2, n2p, comb, wout = in_turn(
        middle, where, tokens, mixed, w_out, small_mine, small_theirs, gain_two, router_t8, routes_t,
    )
    toks = (n2p, over_core(n2p))
    shared_fetched = fetch(
        shared_w, ((0, 0), (0, 1)), 1, core * per_core, DEAR, (first_w[1], first_w[3], second_w[0])
    )
    second_w = (second_w[0], over_y(second_w[0]), second_w[1])
    combs = jnp.stack([comb, over_core(comb)])

    near = [[h * 16 + r for r in range(16)] for h in range(reps // 16)]
    distant = [[h * 16 + g for h in range(reps // 16)] for g in range(16)]

    def distant_sum(piece):
        if reps > 16:
            flat = piece.reshape(-1, piece.shape[-1])
            flat = lax.psum_scatter(flat, "rep", scatter_dimension=0, tiled=True, axis_index_groups=distant)
            flat = lax.all_gather(flat, "rep", axis=0, tiled=True, axis_index_groups=distant)
            piece = flat.reshape(piece.shape)
        return piece

    def finish(piece):
        return lax.all_gather(distant_sum(piece), "rep", axis=0, tiled=False, axis_index_groups=near)

    def first(pair, cost=CHEAP):
        pair["sums"] = in_turn(functools.partial(pair_first, cost=cost), where, pair["keep"], pair["got"], pair["hold"], pair["got_y"])
        pair["got"] = (over_y(pair["sums"][0]), over_x(pair["sums"][2]))

    def second(pair, cost=CHEAP):
        call = functools.partial(pair_second, cost=cost)
        pair["sums"] = in_turn(call, where, pair["sums"][1], pair["got"][0], pair["sums"][3], pair["got"][1])
        pair["got"] = [pair["sums"][0]] + [over_z(pair["sums"][n], n) for n in range(1, 4)]

    def third(pair, cost=CHEAP):
        pair["piece"] = in_turn(functools.partial(pair_third, cost=cost), where, pair["got"])

    def new_pair(keep, send, hold, push):
        return {"keep": keep, "got": over_x(send), "hold": hold, "got_y": over_y(push)}

    def routing(j):
        expert = core * per_core + j
        slot_row = lax.dynamic_index_in_dim(slots, expert, 1, keepdims=False)
        gate_row = lax.dynamic_index_in_dim(combs, expert, 1, keepdims=False)
        return where_of(expert), (slot_row, slot_row.reshape(-1, 1), gate_row)

    def after_held(values):
        return [later(v, held[0]) for v in values]

    def add_pair(a, b):
        return ((a.astype(F32) + b.astype(F32)).astype(BF),)

    place_a, route_a = routing(0)
    place_b, route_b = routing(1)
    res_a = in_turn(functools.partial(ffn, route=route_a), place_a, toks, dys, *experts_w, first_w)
    pair_a = new_pair(*res_a[3:])
    second_w += (over_z(later(second_w[2], res_a[0]), 1),)
    res_b = in_turn(
        functools.partial(ffn, route=route_b, only=0), place_b, toks, dys, *experts_w, second_w[:2],
        need=tuple(shared_fetched),
    )
    first(pair_a)
    from_early = over_core(in_turn(add_pair, res_a[1], res_b[1])[0])
    pair_b = new_pair(*after_held(res_b[3:]))
    res_c = in_turn(functools.partial(ffn, route=route_b, only=1), place_b, toks, dys, *experts_w, second_w[2:])
    sums = pair_a["sums"]
    scattered = in_turn(pair_scatter, where, sums[1], pair_a["got"][0], sums[3], pair_a["got"][1])
    z_groups = [[h * 16 + z * 4 + g for z in range(4)] for h in range(reps // 16) for g in range(4)]
    piece_a = lax.psum_scatter(scattered, "rep", scatter_dimension=0, tiled=False, axis_index_groups=z_groups)
    gathered = finish(piece_a)
    first(pair_b)
    pair_c = new_pair(*after_held(res_c[3:]))
    res_s = in_turn(functools.partial(ffn, before=res_c[1]), where, toks, dys, *shared_w, shared_fetched)
    parts = [res_a[0], res_b[0], res_c[0], res_s[0], from_early, over_core(res_s[1])]
    dgates = jnp.stack([res_a[2], res_b[2] + res_c[2]])
    dgates_oth = over_core(dgates[:, 1])
    first(pair_c, DEAR)
    dgate = in_order(core, dgates[:, 0], dgates_oth, 0)
    comb_e = comb[:experts]
    dlog_t = (comb_e * (dgate - jnp.sum(comb_e * dgate, axis=0, keepdims=True))).astype(BF)
    dlog = jnp.pad(dlog_t.T, ((0, 0), (0, 128 - experts)))
    output, d_resid, d_low, ggain_two = in_turn(
        join, where, cotangent, resid, gain_two, dlog, router_t128, parts
    )
    grad_router = jnp.dot(dlog_t, n2, preferred_element_type=F32)
    second(pair_b)
    first_keep, first_send, gout_low, d_normed = in_turn(
        attend_backward, where, pic_block, tokens, gain_one, wqkv, wout, tables, q, k, v, mixed, lse, d_low
    )
    third(pair_b)
    second(pair_c)
    pair_s = new_pair(*after_held(res_s[2:]))
    last_keep, last_send, gout_high, input_grad, ggain_one = in_turn(
        attend_backward,
        where, pic_block, tokens, gain_one, wqkv, wout, tables, q, k, v, mixed, lse, d_low, (d_resid, d_normed),
    )

    for_other, for_me = in_turn(
        attention_pack, where, first_keep, first_send, last_keep, last_send, gout_low, gout_high,
        ggain_one, ggain_two, grad_router,
    )
    att_got = over_core(for_other)
    shared_shapes = [shared_gate.shape, shared_up.shape, shared_down.shape]
    expert_shapes = [expert_gate.shape, expert_up.shape, expert_down.shape]
    third(pair_c)
    piece_b = jnp.stack([pair_b["piece"], pair_c["piece"]])
    gathered_b = finish(piece_b.reshape((2, 6) + piece_b.shape[3:]))
    first(pair_s, DEAR)
    att_keep, att_send = in_turn(attention_sum, where, for_me, att_got)
    x_got = over_x(att_send)
    expert_grads = in_turn(lambda f: place(where, 0, f, expert_shapes, None, HUGE), gathered)
    second(pair_s, FAIR)
    y_send, y_keep = in_turn(sum_x, where, att_keep, x_got)
    y_got = over_y(y_send)
    third(pair_s, FAIR)
    shared_full = finish(pair_s["piece"])
    quarter_rows = in_turn(functools.partial(sum_y, cost=FAIR), where, y_keep, y_got)
    quarter_rows = [quarter_rows[0]] + [over_z(quarter_rows[n], n) for n in range(1, 4)]
    piece = distant_sum(in_turn(functools.partial(sum_z, cost=FAIR), where, quarter_rows))
    att = [piece] + [over_z(piece, n) for n in range(1, 4)]
    att = att + [over_y(p) for p in att]
    expert_grads = in_turn(
        lambda f, *old: place(where, 1, f, expert_shapes, old, HUGE), gathered_b, *expert_grads
    )
    att = in_turn(assemble, where, att)
    att_oth = over_core(att)
    gq, gk, gv, gout, small_grads = in_turn(attention_unpack, where, att, att_oth)
    shared_grads = in_turn(
        lambda f: place(where, None, f, shared_shapes, None),
        shared_full.reshape((16, 1, 6) + shared_full.shape[3:]),
    )
    return (
        output,
        input_grad,
        small_grads[:, 0],
        gq,
        gk,
        gv,
        gout,
        small_grads[:, 1],
        small_grads[:, 2 : 2 + experts],
        *expert_grads,
        *shared_grads,
    )


def solution(mesh):
    both = P(("rep", "shard"), None)
    rows = P("shard", None)
    vec = P("shard")
    mid = P(None, "shard", None)
    return jax.shard_map(
        on_device,
        mesh=mesh,
        in_specs=(
            both, both, P(("rep", "shard")),
            vec, rows, rows, rows, rows, vec, rows, mid, mid, mid, rows, rows, rows,
            both,
        ),
        out_specs=(both, both, vec, rows, rows, rows, rows, vec, rows, mid, mid, mid, rows, rows, rows),
        check_vma=False,
    )
```

```python
import functools

import jax
import jax.numpy as jnp
from jax import lax
from jax.experimental import pallas as pl
from jax.experimental.pallas import tpu as pltpu
from jax.sharding import PartitionSpec as P

D = 768
HEADS = 12
HEAD_DIM = 64
PIC = 256
CAP = 640
PAIR = 2 * HEAD_DIM
PAIRS = HEADS // 2
QB = 256
EPS = 1e-05
BF = jnp.bfloat16
F32 = jnp.float32
ALL = ("rep", "shard")
MIB = 1 << 20
CHEAP = pl.CostEstimate(flops=1, transcendentals=0, bytes_accessed=1)
DEAR = pl.CostEstimate(flops=1 << 36, transcendentals=0, bytes_accessed=1)
HUGE = pl.CostEstimate(flops=1 << 38, transcendentals=0, bytes_accessed=1)
FAIR = pl.CostEstimate(flops=1 << 34, transcendentals=0, bytes_accessed=1)


def nn(a, b):
    return lax.dot_general(a, b, (((1,), (0,)), ((), ())), preferred_element_type=F32)


def nt(a, b):
    return lax.dot_general(a, b, (((1,), (1,)), ((), ())), preferred_element_type=F32)


def resident(shape):
    zeros = (0,) * len(shape)
    return pl.BlockSpec(shape, lambda *_: zeros, pipeline_mode=pl.Buffered(1))


def rotary_tables(length):
    halfway = HEAD_DIM // 2
    freqs_base = 10000.0 ** (-jnp.arange(halfway, dtype=F32) / halfway)
    angles = jnp.arange(length, dtype=F32)[:, None] * freqs_base[None, :]
    cosine = jnp.cos(angles)
    sine = jnp.sin(angles)
    zero = jnp.zeros_like(sine)
    cos_t = jnp.concatenate([cosine] * 4, axis=1)
    left = jnp.concatenate([-sine, zero, -sine, zero], axis=1)
    right = jnp.concatenate([zero, sine, zero, sine], axis=1)
    return cos_t, left, right


def turned(v, left, right):
    return pltpu.roll(v, 96, 1) * left + pltpu.roll(v, 32, 1) * right


def head_masks(rows):
    lane = lax.broadcasted_iota(jnp.int32, (rows, PAIR), 1)
    return lane < HEAD_DIM, lane >= HEAD_DIM


def attend_forward_body(
    where, pic, tok, gain, wq, wk, wv, mine, theirs, cos_t, left, right,
    q_o, k_o, v_o, mix_o, lse_o, w_o,
    xn,
):
    length = tok.shape[0]
    half = D // 2
    step = pl.program_id(0)

    @pl.when(step == 0)
    def _():
        for lo in range(0, length, QB):
            x = tok[lo : lo + QB, :].astype(F32)
            inv = lax.rsqrt(jnp.mean(x * x, axis=1, keepdims=True) + EPS)
            xn[lo : lo + QB, :] = (x * inv * gain[...]).astype(BF)

    own = pl.ds(pl.multiple_of(where[0] * half, half), half)
    quarter = half // 2
    first = pl.ds(pl.multiple_of((1 - where[0]) * half + where[1] * quarter, quarter), quarter)
    second = pl.ds(pl.multiple_of((1 - where[0]) * half + (1 - where[1]) * quarter, quarter), quarter)
    for m, w in enumerate((wq, wk, wv)):
        cols = slice(m * PAIR, (m + 1) * PAIR)
        w_o[own, cols] = w[...]
        w_o[first, cols] = mine[m]
        w_o[second, cols] = theirs[m]
    for lo in range(0, length, QB):
        rows = slice(lo, lo + QB)
        qkv = nn(xn[rows, :], w_o[...])
        q, k = qkv[:, :PAIR], qkv[:, PAIR : 2 * PAIR]
        c_, l_, r_ = cos_t[rows, :], left[rows, :], right[rows, :]
        q_o[rows, :] = (q * c_ + turned(q, l_, r_)).astype(BF) * jnp.asarray(0.125, BF)
        k_o[rows, :] = (k * c_ + turned(k, l_, r_)).astype(BF)
        v_o[rows, :] = qkv[:, 2 * PAIR :].astype(BF)
    masks = head_masks(QB)
    row = lax.broadcasted_iota(jnp.int32, (QB, QB), 0)
    col = lax.broadcasted_iota(jnp.int32, (QB, QB), 1)
    causal = col <= row
    for block in range(length // QB):
        rows = slice(block * QB, (block + 1) * QB)
        allowed = causal | (pic[0] == block)
        q = q_o[rows, :]
        outs = []
        for head in range(2):
            qm = jnp.where(masks[head], q, jnp.zeros_like(q))
            s_d = jnp.where(allowed, nt(qm, k_o[rows, :]), -1e30)
            top = jnp.max(s_d, axis=1, keepdims=True)
            if block:
                s_o = nt(qm, k_o[: block * QB, :])
                top = jnp.maximum(top, jnp.max(s_o, axis=1, keepdims=True))
            p_d = jnp.exp(s_d - top)
            total = jnp.sum(p_d, axis=1, keepdims=True)
            acc = nn(p_d.astype(BF), v_o[rows, :])
            if block:
                p_o = jnp.exp(s_o - top)
                total = total + jnp.sum(p_o, axis=1, keepdims=True)
                acc = acc + nn(p_o.astype(BF), v_o[: block * QB, :])
            outs.append(acc / total)
            lse = jnp.broadcast_to(top + jnp.log(total), (QB, PAIR))
            lse_o[0, head : head + 1, rows] = jnp.transpose(lse)[0:1, :]
        mix_o[rows, :] = jnp.where(masks[0], outs[0], outs[1]).astype(BF)


def attend_forward(where, pic_block, tokens, gain, weights, mine, theirs, tables):
    length = tokens.shape[0]
    half = D // 2
    pair = pl.BlockSpec((length, PAIR), lambda p: (0, p))
    wide = jax.ShapeDtypeStruct((length, D), BF)
    weight = pl.BlockSpec((half, PAIR), lambda p: (0, p))
    part = pl.BlockSpec((3, half // 2, PAIR), lambda p: (0, 0, p))
    return pl.pallas_call(
        attend_forward_body,
        cost_estimate=DEAR,
        grid=(PAIRS,),
        in_specs=[
            pl.BlockSpec(memory_space=pltpu.SMEM),
            pl.BlockSpec(memory_space=pltpu.SMEM),
            resident((length, D)),
            resident((1, D)),
            weight,
            weight,
            weight,
            part,
            part,
            resident((length, PAIR)),
            resident((length, PAIR)),
            resident((length, PAIR)),
        ],
        out_specs=[
            pair, pair, pair, pair,
            pl.BlockSpec((1, 8, length), lambda p: (p, 0, 0)),
            pl.BlockSpec((D, 3 * PAIR), lambda p: (0, p)),
        ],
        out_shape=[
            wide, wide, wide, wide,
            jax.ShapeDtypeStruct((PAIRS, 8, length), F32),
            jax.ShapeDtypeStruct((D, 3 * D), BF),
        ],
        scratch_shapes=[pltpu.VMEM((length, D), BF)],
        compiler_params=pltpu.CompilerParams(vmem_limit_bytes=48 * MIB),
        name="attend_forward",
    )(where, pic_block, tokens, gain, *weights, mine, theirs, *tables)


def attend_backward_body(
    last, where, pic, tok, gain, wqkv, wout, cos_t, left, right, q_i, k_i, v_i, mix_i, lse_i, dres, *refs
):
    if last:
        dres_f, dxn_i, keep_o, send_o, gout_o, igrad_o, ggain_o = refs[:7]
        refs = refs[7:]
    else:
        keep_o, send_o, gout_o, dxn_o = refs[:4]
        refs = refs[4:]
    xn_t, dxn, dmix, dqkv, dk_s, dv_s, k_t = refs
    length = tok.shape[0]
    half = D // 2
    step = pl.program_id(0)

    @pl.when(step == 0)
    def _():
        for lo in range(0, length, QB):
            x = tok[lo : lo + QB, :].astype(F32)
            inv = lax.rsqrt(jnp.mean(x * x, axis=1, keepdims=True) + EPS)
            n_t = jnp.transpose((x * inv * gain[...]).astype(BF))
            spot = pl.multiple_of(where[0] * half, half)
            xn_t[pl.ds(spot, half), lo : lo + QB] = n_t[:half, :]
            xn_t[pl.ds(half - spot, half), lo : lo + QB] = n_t[half:, :]

    dm = nt(dres[...], wout[...]).astype(BF)
    dmix[...] = dm
    mixed = mix_i[...]
    gout_o[...] = nn(jnp.transpose(mixed), dres[...]).astype(BF)
    prod = jnp.transpose(dm.astype(F32) * mixed.astype(F32))
    delta = (
        jnp.sum(prod[:HEAD_DIM, :], axis=0, keepdims=True),
        jnp.sum(prod[HEAD_DIM:, :], axis=0, keepdims=True),
    )
    k_t[...] = jnp.transpose(k_i[...])
    masks = head_masks(QB)
    key_row = lax.broadcasted_iota(jnp.int32, (QB, QB), 0)
    query_col = lax.broadcasted_iota(jnp.int32, (QB, QB), 1)
    causal = key_row <= query_col
    for block in reversed(range(length // QB)):
        rows = slice(block * QB, (block + 1) * QB)
        first = block == length // QB - 1
        allowed = causal | (pic[0] == block)
        q = q_i[rows, :]
        dm = dmix[rows, :]
        dq_t = []
        parts = {"d": [], "o": []}
        for head in range(2):
            qm = jnp.where(masks[head], q, jnp.zeros_like(q))
            dmm = jnp.where(masks[head], dm, jnp.zeros_like(dm))
            lse = lse_i[0, head : head + 1, rows]
            cent = delta[head][:, rows]
            lanes = slice(head * HEAD_DIM, (head + 1) * HEAD_DIM)
            dq = None
            for part, keys in (("d", rows), ("o", slice(0, block * QB))):
                if part == "o" and block == 0:
                    continue
                st = nt(k_i[keys, :], qm)
                pt = jnp.exp(st - lse)
                if part == "d":
                    pt = jnp.where(allowed, pt, 0.0)
                dpt = nt(v_i[keys, :], dmm)
                dst = (pt * (dpt - cent)).astype(BF)
                parts[part].append((nn(dst, qm), nn(pt.astype(BF), dmm)))
                add = nn(k_t[lanes, keys], dst)
                dq = add if dq is None else dq + add
            dq_t.append(dq)
        for part, keys in (("d", rows), ("o", slice(0, block * QB))):
            if not parts[part]:
                continue
            dk = parts[part][0][0] + parts[part][1][0]
            dv = parts[part][0][1] + parts[part][1][1]
            if first:
                dk_s[keys, :] = dk
                dv_s[keys, :] = dv
            else:
                dk_s[keys, :] = dk_s[keys, :] + dk
                dv_s[keys, :] = dv_s[keys, :] + dv
        dq = jnp.transpose(jnp.concatenate(dq_t, axis=0)) * 0.125
        c_, l_, r_ = cos_t[rows, :], left[rows, :], right[rows, :]
        dqkv[rows, :PAIR] = (dq * c_ - turned(dq, l_, r_)).astype(BF)
        dk = dk_s[rows, :]
        dqkv[rows, PAIR : 2 * PAIR] = (dk * c_ - turned(dk, l_, r_)).astype(BF)
        dqkv[rows, 2 * PAIR :] = dv_s[rows, :].astype(BF)
    gqkv = nn(xn_t[...], dqkv[...]).astype(BF)
    keep_o[...] = gqkv[:half, :]
    send_o[...] = gqkv[half:, :]
    add = nt(dqkv[...], wqkv[...])

    @pl.when(step == 0)
    def _():
        if last:
            dxn[...] = dxn_i[...] + add
        else:
            dxn[...] = add

    @pl.when(step > 0)
    def _():
        dxn[...] = dxn[...] + add

    @pl.when(step == pl.num_programs(0) - 1)
    def _():
        if not last:
            dxn_o[...] = dxn[...]
            return
        total = jnp.zeros((1, D), F32)
        for lo in range(0, length, QB):
            rows = slice(lo, lo + QB)
            x = tok[rows, :].astype(F32)
            inv = lax.rsqrt(jnp.mean(x * x, axis=1, keepdims=True) + EPS)
            n = x * inv
            up = dxn[rows, :]
            total = total + jnp.sum(up * n, axis=0, keepdims=True)
            u = up * gain[...]
            igrad_o[rows, :] = dres_f[rows, :] + inv * (u - n * jnp.mean(u * n, axis=1, keepdims=True))
        ggain_o[...] = total


def attend_backward(where, pic_block, tokens, gain, wqkv, wout, tables, q, k, v, mixed, lse, dres, more=None):
    length = tokens.shape[0]
    half = D // 2
    last = more is not None
    early = 2 * PAIRS // 3
    count = PAIRS - early if last else early
    off = early if last else 0
    pair = pl.BlockSpec((length, PAIR), lambda p: (0, p + off))
    grad = pl.BlockSpec((half, 3 * PAIR), lambda p: (0, p))
    wide = jax.ShapeDtypeStruct((length, D), F32)
    out_specs = [grad, grad, pl.BlockSpec((PAIR, D), lambda p: (p, 0)), resident((length, D))]
    out_shape = [
        jax.ShapeDtypeStruct((half, 3 * PAIR * count), BF),
        jax.ShapeDtypeStruct((half, 3 * PAIR * count), BF),
        jax.ShapeDtypeStruct((PAIR * count, D), BF),
        wide,
    ]
    if last:
        out_specs.append(resident((1, D)))
        out_shape.append(jax.ShapeDtypeStruct((1, D), F32))
    return pl.pallas_call(
        functools.partial(attend_backward_body, last),
        cost_estimate=DEAR,
        grid=(count,),
        in_specs=[
            pl.BlockSpec(memory_space=pltpu.SMEM),
            pl.BlockSpec(memory_space=pltpu.SMEM),
            resident((length, D)),
            resident((1, D)),
            pl.BlockSpec((D, 3 * PAIR), lambda p: (0, p + off)),
            pl.BlockSpec((PAIR, D), lambda p: (p + off, 0)),
            resident((length, PAIR)),
            resident((length, PAIR)),
            resident((length, PAIR)),
            pair, pair, pair, pair,
            pl.BlockSpec((1, 8, length), lambda p: (p + off, 0, 0)),
            resident((length, D)),
        ]
        + ([resident((length, D))] * 2 if last else []),
        out_specs=out_specs,
        out_shape=out_shape,
        scratch_shapes=[
            pltpu.VMEM((D, length), BF),
            pltpu.VMEM((length, D), F32),
            pltpu.VMEM((length, PAIR), BF),
            pltpu.VMEM((length, 3 * PAIR), BF),
            pltpu.VMEM((length, PAIR), F32),
            pltpu.VMEM((length, PAIR), F32),
            pltpu.VMEM((PAIR, length), BF),
        ],
        compiler_params=pltpu.CompilerParams(vmem_limit_bytes=56 * MIB),
        name="attend_backward_2" if last else "attend_backward_1",
    )(where, pic_block, tokens, gain, wqkv, wout, *tables, q, k, v, mixed, lse, dres, *(more or ()))


def middle_body(
    shard, tok, mixed, w_own, w_mine, w_theirs, gain, router_t, routes_t,
    resid_o, n2_o, n2p_o, comb_o, wout,
):
    @pl.when(pl.program_id(0) == 0)
    def _():
        half = D // 2
        quarter = half // 2
        other = (1 - shard[0]) * half
        wout[pl.ds(pl.multiple_of(shard[0] * half, half), half), :] = w_own[...]
        first = pl.multiple_of(other + shard[1] * quarter, quarter)
        second = pl.multiple_of(other + (1 - shard[1]) * quarter, quarter)
        wout[pl.ds(first, quarter), :] = w_mine[...]
        wout[pl.ds(second, quarter), :] = w_theirs[...]

    r = tok[...].astype(F32) + nn(mixed[...], wout[...])
    resid_o[...] = r
    inv = lax.rsqrt(jnp.mean(r * r, axis=1, keepdims=True) + EPS)
    n2 = (r * inv * gain[...]).astype(BF)
    n2_o[...] = n2
    half = D // 2
    swapped = jnp.concatenate([n2[:, half:], n2[:, :half]], axis=1)
    n2p_o[...] = jnp.where(shard[0] == 0, n2, swapped)
    logits = nt(router_t[...], n2)
    expert = lax.broadcasted_iota(jnp.int32, logits.shape, 0)
    picks = [expert == routes_t[k : k + 1, :] for k in range(2)]
    chosen = [jnp.sum(jnp.where(p, logits, 0.0), axis=0, keepdims=True) for p in picks]
    top = jnp.maximum(chosen[0], chosen[1])
    weights = [jnp.exp(v - top) for v in chosen]
    total = weights[0] + weights[1]
    gates = [w / total for w in weights]
    comb_o[...] = jnp.where(picks[0], gates[0], 0.0) + jnp.where(picks[1], gates[1], 0.0)


def middle(where, tokens, mixed, w_own, w_mine, w_theirs, gain, router_t, routes_t):
    length = tokens.shape[0]
    block = 256
    rows = pl.BlockSpec((block, D), lambda i: (i, 0))
    cols = pl.BlockSpec((8, block), lambda i: (0, i))
    return pl.pallas_call(
        middle_body,
        cost_estimate=CHEAP,
        grid=(length // block,),
        in_specs=[
            pl.BlockSpec(memory_space=pltpu.SMEM),
            rows,
            rows,
            resident((D // 2, D)),
            resident((D // 4, D)),
            resident((D // 4, D)),
            resident((1, D)),
            resident((8, D)),
            cols,
        ],
        out_specs=[rows, rows, rows, cols, resident((D, D))],
        out_shape=[
            jax.ShapeDtypeStruct((length, D), F32),
            jax.ShapeDtypeStruct((length, D), BF),
            jax.ShapeDtypeStruct((length, D), BF),
            jax.ShapeDtypeStruct((8, length), F32),
            jax.ShapeDtypeStruct((D, D), BF),
        ],
        compiler_params=pltpu.CompilerParams(vmem_limit_bytes=40 * MIB),
        name="middle",
    )(where, tokens, mixed, w_own, w_mine, w_theirs, gain, router_t, routes_t)


def join_body(shard, dy, resid, gain, dlog, router_t, *refs):
    parts = refs[:-4]
    out_o, dres_o, dlow_o, ggain_o = refs[-4:]
    r = resid[...]
    total = r
    for part in parts:
        total = total + part[0].astype(F32)
    out_o[...] = total.astype(BF)
    up = parts[0][1].astype(F32)
    for part in parts[1:]:
        up = up + part[1].astype(F32)
    half = D // 2
    swapped = jnp.concatenate([up[:, half:], up[:, :half]], axis=1)
    up = jnp.where(shard[0] == 0, up, swapped)
    up = up + nn(dlog[...], router_t[...])
    inv = lax.rsqrt(jnp.mean(r * r, axis=1, keepdims=True) + EPS)
    n = r * inv
    add = jnp.sum(up * n, axis=0, keepdims=True)

    @pl.when(pl.program_id(0) == 0)
    def _():
        ggain_o[...] = add

    @pl.when(pl.program_id(0) > 0)
    def _():
        ggain_o[...] = ggain_o[...] + add

    u = up * gain[...]
    d = dy[...].astype(F32) + inv * (u - n * jnp.mean(u * n, axis=1, keepdims=True))
    dres_o[...] = d
    dlow_o[...] = d.astype(BF)


def join(shard, dy, resid, gain, dlog, router_t, parts):
    length = dy.shape[0]
    block = 256
    rows = pl.BlockSpec((block, D), lambda i: (i, 0))

    return pl.pallas_call(
        join_body,
        cost_estimate=CHEAP,
        grid=(length // block,),
        in_specs=[
            pl.BlockSpec(memory_space=pltpu.SMEM),
            rows,
            rows,
            resident((1, D)),
            pl.BlockSpec((block, 128), lambda i: (i, 0)),
            resident((128, D)),
        ]
        + [pl.BlockSpec((2, block, D), lambda i: (0, i, 0))] * len(parts),
        out_specs=[rows, rows, rows, pl.BlockSpec((1, D), lambda i: (0, 0))],
        out_shape=[
            jax.ShapeDtypeStruct((length, D), BF),
            jax.ShapeDtypeStruct((length, D), F32),
            jax.ShapeDtypeStruct((length, D), BF),
            jax.ShapeDtypeStruct((1, D), F32),
        ],
        compiler_params=pltpu.CompilerParams(vmem_limit_bytes=40 * MIB),
        name="join",
    )(shard, dy, resid, gain, dlog, router_t, *parts)


def ffn_body(routed, steps, chunk, before, where, tok_a, tok_b, dy_a, dy_b, *refs):
    tok, dy = (tok_a, tok_b), (dy_a, dy_b)
    if routed:
        slot_row, slot_col, gate_row = refs[:3]
        refs = refs[3:]
    g_own, u_own, d_own = refs[:3]
    per = steps // 2
    gu_oth = refs[3 : 3 + 2 * per]
    d_oth = refs[3 + 2 * per : 3 + 4 * per]
    refs = refs[3 + 4 * per :]
    if before:
        theirs_i = refs[0]
        refs = refs[1:]
    sides = refs[:2]
    refs = refs[2:]
    if routed:
        dgate_o = refs[0]
        refs = refs[1:]
    keep, send, hold_y, push_y = refs[:4]
    refs = refs[4:]
    wg, wu, wd, y_acc, dx_acc, hid_s, dg_s, du_s, x_t, de_t = refs[:10]
    refs = refs[10:]
    i = pl.program_id(0)
    srcs, length = 2, tok_a.shape[0]
    rows_all = y_acc.shape[0]
    hold = rows_all // srcs
    half = D // 2
    if routed:
        x_s, de_s, dys, gate_s = refs
    tile = 128

    @pl.when(i == 0)
    def _():
        for src in range(srcs):
            if routed:
                for lo in range(0, hold, tile):
                    slot = lax.broadcasted_iota(jnp.int32, (tile, length), 0) + lo
                    mine = slot == slot_row[src : src + 1, :]
                    pick = jnp.where(mine, 1.0, 0.0).astype(BF)
                    rows = slice(src * hold + lo, src * hold + lo + tile)
                    x = nn(pick, tok[src][...]).astype(BF)
                    d_raw = nn(pick, dy[src][...])
                    gate = jnp.sum(jnp.where(mine, gate_row[src : src + 1, :], 0.0), axis=1, keepdims=True)
                    gate_s[rows, :] = jnp.broadcast_to(gate, (tile, 128))
                    d_e = (d_raw * gate).astype(BF)
                    x_s[rows, :] = x
                    dys[rows, :] = d_raw.astype(BF)
                    de_s[rows, :] = d_e
                    x_t[:, rows] = jnp.transpose(x)
                    de_t[:, rows] = jnp.transpose(d_e)
            else:
                for lo in range(0, hold, 256):
                    rows = slice(src * hold + lo, src * hold + lo + 256)
                    x_t[:, rows] = jnp.transpose(tok[src][lo : lo + 256, :])
                    de_t[:, rows] = jnp.transpose(dy[src][lo : lo + 256, :])

    wg[:half, :] = g_own[...]
    wu[:half, :] = u_own[...]
    part = half // 2
    block = wd.shape[0]
    for p in range(per):

        @pl.when(i // 2 == p)
        def _(p=p):
            for k in range(2):
                spot = pl.ds(pl.multiple_of(half + (where[3] ^ k) * part, part), part)
                ref = gu_oth[2 * p + k]
                for h in range(2):
                    lanes = slice(h * 256, (h + 1) * 256)
                    wg[spot, lanes] = ref[2 * h * part : (2 * h + 1) * part, :]
                    wu[spot, lanes] = ref[(2 * h + 1) * part : (2 * h + 2) * part, :]

    @pl.when(i % 2 == 0)
    def _():
        wd[...] = d_own[...]

    for p in range(per):

        @pl.when(i == 2 * p + 1)
        def _(p=p):
            for k in range(2):
                spot = pl.ds(pl.multiple_of((where[3] ^ k) * (block // 2), block // 2), block // 2)
                for h in range(3):
                    wd[spot, h * 256 : (h + 1) * 256] = d_oth[2 * p + k][h * 256 : (h + 1) * 256, :]

    def piece(j, src, first):
        inner = pl.ds(pl.multiple_of(j * chunk, chunk), chunk)
        if routed:
            rows = inner
            x, de = x_s[rows, :], de_s[rows, :]
        else:
            rows = pl.ds(pl.multiple_of(src * length + j * chunk, chunk), chunk)
            x, de = tok[src][inner, :], dy[src][inner, :]
        g = nn(x, wg[...])
        u = nn(x, wu[...])
        dh = nt(de, wd[...])
        s = 1.0 / (1.0 + jnp.exp(-g))
        act = g * s
        hid = (act * u).astype(BF)
        du = (dh * act).astype(BF)
        dg = (dh * u * s * (1.0 + g * (1.0 - s))).astype(BF)
        hid_s[rows, :] = hid
        dg_s[rows, :] = dg
        du_s[rows, :] = du
        y = nn(hid, wd[...])
        dx = nt(dg, wg[...]) + nt(du, wu[...])
        if first:
            y_acc[rows, :] = y
            dx_acc[rows, :] = dx
        else:
            y_acc[rows, :] = y_acc[rows, :] + y
            dx_acc[rows, :] = dx_acc[rows, :] + dx

    for first in (True, False):

        @pl.when((i == 0) == first)
        def _(first=first):
            for src in range(1 if routed else srcs):

                @pl.loop(0, (rows_all if routed else length) // chunk)
                def _(j, src=src, first=first):
                    piece(j, src, first)

    gg = nn(x_t[...], dg_s[...]).astype(BF)
    gu = nn(x_t[...], du_s[...]).astype(BF)
    gd = nn(de_t[...], hid_s[...]).astype(BF)
    for p in range(per):

        def put(side, tile, value, p=p):
            count = keep.shape[0]
            number = 6 * p + tile
            if number < count:
                (keep, send)[side][number] = value
            else:
                top, low = value[: half // 2, :], value[half // 2 :, :]
                hold_y[side, number - count] = jnp.where(where[4] == 0, top, low)
                push_y[side, number - count] = jnp.where(where[4] == 0, low, top)

        @pl.when(i == 2 * p)
        def _(put=put):
            put(0, 0, gg[:half, :])
            put(0, 1, gu[:half, :])
            put(0, 2, gd[:half, :])
            put(0, 3, gd[half:, :])
            put(1, 4, gg[half:, :])
            put(1, 5, gu[half:, :])

        @pl.when(i == 2 * p + 1)
        def _(put=put):
            put(0, 4, gg[:half, :])
            put(0, 5, gu[:half, :])
            put(1, 0, gg[half:, :])
            put(1, 1, gu[half:, :])
            put(1, 2, gd[:half, :])
            put(1, 3, gd[half:, :])

    @pl.when(i == steps - 1)
    def _():
        for src in range(srcs):
            if routed:
                total = jnp.zeros((1, length), F32)
                for lo in range(0, hold, tile):
                    rows = slice(src * hold + lo, src * hold + lo + tile)
                    y = y_acc[rows, :]
                    dgate = jnp.sum(dys[rows, :].astype(F32) * y, axis=1, keepdims=True)
                    slot = lax.broadcasted_iota(jnp.int32, (tile, length), 0) + lo
                    mine = slot == slot_row[src : src + 1, :]
                    total = total + jnp.sum(jnp.where(mine, dgate, 0.0), axis=0, keepdims=True)
                    x_s[rows, :] = (y * gate_s[rows, 0:1]).astype(BF)
                    de_s[rows, :] = dx_acc[rows, :].astype(BF)
                dgate_o[src : src + 1, :] = total
                held = slice(src * hold, (src + 1) * hold)
                for lo in range(0, length, tile):
                    slot = lax.broadcasted_iota(jnp.int32, (tile, hold), 1)
                    mine = slot == slot_col[src * length + lo : src * length + lo + tile, :]
                    pick = jnp.where(mine, 1.0, 0.0).astype(BF)
                    sides[src][0, lo : lo + tile, :] = nn(pick, x_s[held, :]).astype(BF)
                    sides[src][1, lo : lo + tile, :] = nn(pick, de_s[held, :]).astype(BF)
            else:
                held = slice(src * hold, (src + 1) * hold)
                for n, acc in enumerate((y_acc, dx_acc)):
                    total = acc[held, :]
                    if before and src == 1:
                        total = total + theirs_i[n].astype(F32)
                    sides[src][n] = total.astype(BF)


def ffn(where, toks, dys, gate, up, down, others, route=None, only=None, before=None):
    routed = route is not None
    srcs, length = 2, toks[0].shape[0]
    block = 512
    half = D // 2
    per = len(others) // 2
    total, start = (2, only) if only is not None else (per, 0)
    steps = 2 * per
    rows_all = srcs * (CAP if routed else length)
    chunk = 256

    def column(i, w):
        return (i % 2 + w[0] - 2 * w[0] * (i % 2)) * total + i // 2 + start

    if routed:
        gate_spec = pl.BlockSpec((None, half, block), lambda i, w: (w[2], 0, column(i, w)))
        down_spec = pl.BlockSpec((None, block, D), lambda i, w: (w[2], i // 2 + start, 0))
    else:
        gate_spec = pl.BlockSpec((half, block), lambda i, w: (0, column(i, w) * 2 + w[1]))
        down_spec = pl.BlockSpec((block, D), lambda i, w: (w[1], 0))
    def shard_block(i, w):
        return i % 2 + w[0] - 2 * w[0] * (i % 2)

    def gu_spec(p):
        first, last = 2 * p, 2 * p + 1
        return pl.BlockSpec((2 * half, 256), lambda i, w: (shard_block(jnp.clip(i, first, last), w), 0))

    d_spec = pl.BlockSpec((2 * half, 256), lambda i, w: (2, 0), pipeline_mode=pl.Buffered(1))
    in_specs = [resident((length, D))] * 4
    operands = [*toks, *dys]
    if routed:
        in_specs += [resident(r.shape) for r in route]
        operands += list(route)
    in_specs += [gate_spec, gate_spec, down_spec] + [gu_spec(n // 2) for n in range(2 * per)] + [d_spec] * (2 * per)
    operands += [gate, up, down, *others, *others]
    if before is not None:
        in_specs.append(resident(before.shape))
        operands.append(before)
    wide = jax.ShapeDtypeStruct((srcs, length, D), BF)
    out_specs = [resident((srcs, length, D)), resident((srcs, length, D))]
    out_shape = [wide, wide]
    if routed:
        out_specs.append(resident((srcs, length)))
        out_shape.append(jax.ShapeDtypeStruct((srcs, length), F32))
    for shape in ((3 * per, half, block), (2, 3 * per, half // 2, block)):
        out_specs += [resident(shape)] * 2
        out_shape += [jax.ShapeDtypeStruct(shape, BF)] * 2
    scratch = [
        pltpu.VMEM((D, block), BF),
        pltpu.VMEM((D, block), BF),
        pltpu.VMEM((block, D), BF),
        pltpu.VMEM((rows_all, D), F32),
        pltpu.VMEM((rows_all, D), F32),
        pltpu.VMEM((rows_all, block), BF),
        pltpu.VMEM((rows_all, block), BF),
        pltpu.VMEM((rows_all, block), BF),
        pltpu.VMEM((D, rows_all), BF),
        pltpu.VMEM((D, rows_all), BF),
    ]
    if routed:
        scratch += [
            pltpu.VMEM((rows_all, D), BF),
            pltpu.VMEM((rows_all, D), BF),
            pltpu.VMEM((rows_all, D), BF),
            pltpu.VMEM((rows_all, 128), F32),
        ]
    return pl.pallas_call(
        functools.partial(ffn_body, routed, steps, chunk, before is not None),
        cost_estimate=DEAR,
        grid_spec=pltpu.PrefetchScalarGridSpec(
            num_scalar_prefetch=1,
            grid=(steps,),
            in_specs=in_specs,
            out_specs=out_specs,
            scratch_shapes=scratch,
        ),
        out_shape=out_shape,
        compiler_params=pltpu.CompilerParams(vmem_limit_bytes=63 * MIB),
        name="ffn_routed" if routed else "ffn_shared",
    )(where, *operands)


def add(a, b):
    return a[...].astype(F32) + b[...].astype(F32)


def small_call(body, name, where, grid, ins, outs, cost=CHEAP):
    return pl.pallas_call(
        body,
        cost_estimate=cost,
        grid_spec=pltpu.PrefetchScalarGridSpec(
            num_scalar_prefetch=1,
            grid=grid,
            in_specs=[pl.BlockSpec(block, index) for _, block, index in ins],
            out_specs=[pl.BlockSpec(block, index) for _, block, index in outs],
        ),
        out_shape=[jax.ShapeDtypeStruct(shape, BF) for shape, _, _ in outs],
        compiler_params=pltpu.CompilerParams(vmem_limit_bytes=32 * MIB),
        name=name,
    )(where, *[array for array, _, _ in ins])


def sum_x(where, keep, got, cost=CHEAP):
    tiles, rows, cols = keep.shape
    block = (1, rows // 2, cols)

    def mine(t, w):
        return (t, w[4], 0)

    def other(t, w):
        return (t, 1 - w[4], 0)

    def body(w, k_m, g_m, k_o, g_o, send, hold):
        hold[...] = add(k_m, g_m).astype(BF)
        send[...] = add(k_o, g_o).astype(BF)

    ins = [(keep, block, mine), (got, block, mine), (keep, block, other), (got, block, other)]
    shape = (tiles, rows // 2, cols)
    here = (shape, block, lambda t, w: (t, 0, 0))
    return small_call(body, "sum_x", where, (tiles,), ins, [here, here], cost)


def sum_y(where, keep, got, cost=CHEAP):
    tiles, rows, cols = keep.shape
    step = 3 if tiles % 3 == 0 else 1
    block = (step, rows // 4, cols)

    def body(w, *refs):
        for k in range(4):
            refs[8 + k][...] = add(refs[k], refs[4 + k]).astype(BF)

    spots = [lambda t, w, k=k: (t, w[5] ^ k, 0) for k in range(4)]
    ins = [(keep, block, s) for s in spots] + [(got, block, s) for s in spots]
    here = ((tiles, rows // 4, cols), block, lambda t, w: (t, 0, 0))
    return small_call(body, "sum_y", where, (tiles // step,), ins, [here] * 4, cost)


def sum_z(where, parts, cost=CHEAP):
    shape = parts[0].shape
    step = 3 if shape[0] % 3 == 0 else 1
    block = (step,) + shape[1:]

    def body(w, a, b, c, d, out):
        out[...] = (add(a, b) + add(c, d)).astype(BF)

    def at(t, w):
        return (t, 0, 0)

    ins = [(p, block, at) for p in parts]
    return small_call(body, "sum_z", where, (shape[0] // step,), ins, [(shape, block, at)], cost)[0]


def pack(where, gate, up, down, units, per, cost=CHEAP):
    half = D // 2
    part = half // 2
    routed = gate.ndim == 3

    def body(w, *refs):
        for n in range(len(units)):
            g, u, d = refs[3 * n : 3 * n + 3]
            out = refs[3 * len(units) + n]

            @pl.when(pl.program_id(0) < 2)
            def _(g=g, u=u, out=out):
                for h in range(2):
                    for m, ref in enumerate((g, u)):
                        spot = (2 * h + m) * part
                        out[spot : spot + part, :] = ref[:, h * 256 : (h + 1) * 256]

            @pl.when(pl.program_id(0) == 2)
            def _(d=d, out=out):
                for h in range(3):
                    out[h * 256 : (h + 1) * 256, :] = d[:, h * 256 : (h + 1) * 256]

    in_specs = []
    for p, flip in units:

        def col_block(b, p=p):
            return jnp.minimum(b, 1) * per + p

        if routed:
            col = pl.BlockSpec((None, part, 512), lambda b, w, c=col_block, f=flip: (w[2], w[3] ^ f, c(b)))
            row = pl.BlockSpec((None, 256, D), lambda b, w, p=p, f=flip: (w[2], p * 2 + (w[3] ^ f), 0))
        else:
            col = pl.BlockSpec((part, 512), lambda b, w, c=col_block, f=flip: (w[3] ^ f, c(b) * 2 + w[1]))
            row = pl.BlockSpec((256, D), lambda b, w, f=flip: (w[1] * 2 + (w[3] ^ f), 0))
        in_specs += [col, col, row]
    out = pl.BlockSpec((2 * half, 256), lambda b, w: (b, 0))
    return pl.pallas_call(
        body,
        cost_estimate=cost,
        grid_spec=pltpu.PrefetchScalarGridSpec(
            num_scalar_prefetch=1, grid=(3,), in_specs=in_specs, out_specs=[out] * len(units)
        ),
        out_shape=[jax.ShapeDtypeStruct((6 * half, 256), BF)] * len(units),
        name="pack",
    )(where, *[gate, up, down] * len(units))


def pair_first(where, keep, got, hold, got_y, cost=CHEAP):
    tiles, rows, cols = keep.shape
    block = (1, rows // 2, cols)
    both = (2, 1, rows // 2, cols)

    def mine(t, w):
        return (t, w[4], 0)

    def other(t, w):
        return (t, 1 - w[4], 0)

    def two(t, w):
        return (0, t, 0, 0)

    def body(w, k_m, g_m, k_o, g_o, h, g, y_send, y_keep, x_send, x_keep):
        y_keep[...] = add(k_m, g_m).astype(BF)
        y_send[...] = add(k_o, g_o).astype(BF)
        total = add(h, g).astype(BF)
        x_keep[...] = total[0]
        x_send[...] = total[1]

    ins = [(keep, block, mine), (got, block, mine), (keep, block, other), (got, block, other)]
    ins += [(hold, both, two), (got_y, both, two)]
    here = ((tiles, rows // 2, cols), block, lambda t, w: (t, 0, 0))
    return small_call(body, "pair_first", where, (tiles,), ins, [here] * 4, cost)


def pair_second(where, a, b, c, d, cost=CHEAP):
    tiles, rows, cols = a.shape
    block = (3, rows // 4, cols)

    def body(w, *refs):
        for k in range(4):
            a_, b_, c_, d_ = refs[4 * k : 4 * k + 4]
            refs[16 + k][0] = add(a_, b_).astype(BF)
            refs[16 + k][1] = add(c_, d_).astype(BF)

    ins = []
    for k in range(4):
        ins += [(x, block, lambda t, w, k=k: (t, w[5] ^ k, 0)) for x in (a, b, c, d)]
    out = ((2, tiles) + block[1:], (2,) + block, lambda t, w: (0, t, 0, 0))
    return small_call(body, "pair_second", where, (tiles // 3,), ins, [out] * 4, cost)


def pair_scatter(where, a, b, c, d):
    tiles, rows, cols = a.shape
    block = (tiles, rows // 4, cols)

    def body(w, a_, b_, c_, d_, out):
        out[0] = add(a_, b_).astype(BF)
        out[1] = add(c_, d_).astype(BF)

    ins = [(x, block, lambda t, w: (0, t, 0)) for x in (a, b, c, d)]
    out = ((4, 2) + block, (None, 2) + block, lambda t, w: (t, 0, 0, 0, 0))
    return small_call(body, "pair_scatter", where, (4,), ins, [out])[0]


def pair_third(where, parts, cost=CHEAP):
    shape = parts[0].shape
    block = (None,) + shape[1:]

    def body(w, a, b, c, d, out):
        out[...] = (add(a, b) + add(c, d)).astype(BF)

    def at(n, w):
        return (n, 0, 0, 0)

    return small_call(body, "pair_third", where, (2,), [(p, block, at) for p in parts], [(shape, block, at)], cost)[0]


def attention_pack(where, first_keep, first_send, last_keep, last_send, gout_low, gout_high, gain_a, gain_b, router_g):
    half = D // 2
    wide = 2 * D + 128

    def body(w, lk, ls, hk, hs, gl, gh, ga, gb, gr, other, mine, rows, turned_rows):
        rows[...] = jnp.zeros(rows.shape, F32)
        rows[0:1, :] = ga[...]
        rows[1:2, :] = gb[...]
        rows[2 : 2 + gr.shape[0], :] = gr[...]
        turned_rows[...] = jnp.transpose(rows[...]).astype(BF)
        split = lk.shape[1]
        cut = wide - split
        rest = hk.shape[1] - cut
        for side, (low, high) in enumerate(((lk, hk), (ls, hs))):
            spot = pl.multiple_of((w[0] ^ side) * half, half)
            more = turned_rows[pl.ds(spot, half), :]
            for core in range(2):

                @pl.when(w[1] == core)
                def _(core=core, low=low, high=high, side=side, more=more):
                    first, last = (mine, other) if core == 0 else (other, mine)
                    first[side, :, :split] = low[...]
                    first[side, :, split:] = high[:, :cut]
                    last[side, :, :rest] = high[:, cut:]
                    last[side, :, rest + D : rest + D + 128] = more
                    last[side, :, rest + D + 128 :] = jnp.zeros((half, wide - rest - D - 128), BF)

            for core in range(2):
                for part in range(2):

                    @pl.when((w[1] == core) & ((w[0] ^ side) == part))
                    def _(core=core, part=part, side=side):
                        last = (other, mine)[core]
                        if part == 0:
                            last[side, :, rest : rest + D] = gl[:half, :]
                        else:
                            count = gl.shape[0] - half
                            last[side, :count, rest : rest + D] = gl[half:, :]
                            last[side, count:, rest : rest + D] = gh[...]

    last_core = (first_keep, first_send, last_keep, last_send, gout_low, gout_high, gain_a, gain_b, router_g)
    out = resident((2, half, wide))
    return pl.pallas_call(
        body,
        cost_estimate=CHEAP,
        grid_spec=pltpu.PrefetchScalarGridSpec(
            num_scalar_prefetch=1,
            grid=(1,),
            in_specs=[resident(v.shape) for v in last_core],
            out_specs=[out, out],
            scratch_shapes=[pltpu.VMEM((128, D), F32), pltpu.VMEM((D, 128), BF)],
        ),
        out_shape=[jax.ShapeDtypeStruct((2, half, wide), BF)] * 2,
        compiler_params=pltpu.CompilerParams(vmem_limit_bytes=40 * MIB),
        name="attention_pack",
    )(where, *last_core)


def attention_sum(where, mine, got):
    block = (1,) + mine.shape[1:]

    def body(w, a, b, c, d, keep, send):
        keep[...] = add(a, b).astype(BF)
        send[...] = add(c, d).astype(BF)

    ins = [(v, block, lambda t, w, n=n: (n, 0, 0)) for n in range(2) for v in (mine, got)]
    out = (block, block, lambda t, w: (0, 0, 0))
    return small_call(body, "attention_sum", where, (1,), ins, [out, out])


def attention_unpack(where, mine, theirs):
    half, wide = mine.shape[1:]

    def body(w, m, t, *outs):
        for core in range(2):

            @pl.when(w[1] == core)
            def _(core=core):
                both = (m, t) if core == 0 else (t, m)

                def cols(lo):
                    return both[lo // wide][0, :, lo % wide : lo % wide + 128].astype(F32)

                for pair in range(PAIRS):
                    for n in range(3):
                        outs[n][:, pair * PAIR : (pair + 1) * PAIR] = cols((3 * pair + n) * PAIR)
                for n in range(D // 128):
                    outs[3][:, n * 128 : (n + 1) * 128] = cols(3 * D + n * 128)
                outs[4][...] = cols(4 * D)

    shapes = [(half, D)] * 4 + [(half, 128)]
    return pl.pallas_call(
        body,
        cost_estimate=CHEAP,
        grid_spec=pltpu.PrefetchScalarGridSpec(
            num_scalar_prefetch=1,
            grid=(1,),
            in_specs=[resident(mine.shape)] * 2,
            out_specs=[resident(v) for v in shapes],
        ),
        out_shape=[jax.ShapeDtypeStruct(v, F32) for v in shapes],
        compiler_params=pltpu.CompilerParams(vmem_limit_bytes=40 * MIB),
        name="attention_unpack",
    )(where, mine, theirs)


def assemble(where, pieces):
    tiles, rows, cols = pieces[0].shape
    block = (tiles, rows, cols)

    def body(w, *refs):
        for k in range(8):

            @pl.when(pl.program_id(0) == k)
            def _(k=k):
                refs[8][...] = refs[k][...]

    ins = [(p, block, lambda t, w: (0, 0, 0)) for p in pieces]
    out = ((tiles, 8 * rows, cols), block, lambda t, w: (0, t ^ (w[4] * 4 + w[5]), 0))
    return small_call(body, "assemble", where, (8,), ins, [out])[0]


def place(where, j, full, shapes, before, cost=CHEAP):
    paired = isinstance(full, (list, tuple))
    count, _, rows, block = (full[0] if paired else full).shape[1:]
    half = 8 * rows
    routed = j is not None

    def core(t, w):
        return t + w[1] - 2 * t * w[1]

    def column(o, w):
        o = jnp.minimum(o, 1)
        return o + w[0] - 2 * o * w[0]

    def pick(o):
        return jnp.where(o == 0, 0, 3 - o)

    if paired:
        operands = list(full)

        def mine(t, p, o, w):
            return (0, jnp.where(t == 0, p, count - 1), jnp.where(t == 0, pick(o), 1), 0, 0)

        def theirs(t, p, o, w):
            return (0, jnp.where(t == 0, 0, p), jnp.where(t == 0, 0, pick(o)), 0, 0)

        tiles = [pl.BlockSpec((8, None, 2, rows, block), index) for index in (mine, theirs)]
    else:
        operands = [full.reshape((8, 2) + full.shape[1:])]
        tiles = [
            pl.BlockSpec((8, None, None, 2, rows, block), lambda t, p, o, w: (0, core(t, w), p, pick(o), 0, 0))
        ]

    def body(w, *refs):
        for which in range(len(tiles)):
            if paired:

                @pl.when(pl.program_id(0) == which)
                def _(which=which):
                    write(refs[which], *refs[-3:])

            else:
                write(refs[which], *refs[-3:])

    def write(tile, g_o, u_o, d_o):
        step = pl.program_id(2)

        @pl.when(step < 2)
        def _():
            for r in range(8):
                spot = ((r % 2) * 4 + r // 2) * rows
                g_o[spot : spot + rows, :] = tile[r, 0].astype(F32)
                u_o[spot : spot + rows, :] = tile[r, 1].astype(F32)

        @pl.when(step == 2)
        def _():
            for m in range(2):
                parts = [tile[(n % 4) * 2 + n // 4, m] for n in range(8)]
                d_o[:, m * half : (m + 1) * half] = jnp.transpose(jnp.concatenate(parts, axis=0)).astype(F32)

    if routed:
        col = pl.BlockSpec((None, half, block), lambda t, p, o, w: (core(t, w) * 2 + j, 0, column(o, w) * count + p))
        row = pl.BlockSpec((None, block, D), lambda t, p, o, w: (core(t, w) * 2 + j, p, 0))
    else:
        col = pl.BlockSpec((half, block), lambda t, p, o, w: (0, column(o, w) * 2 + core(t, w)))
        row = pl.BlockSpec((block, D), lambda t, p, o, w: (core(t, w), 0))
    before = before or ()
    return pl.pallas_call(
        body,
        cost_estimate=cost,
        grid_spec=pltpu.PrefetchScalarGridSpec(
            num_scalar_prefetch=1,
            grid=(2, count, 3),
            in_specs=tiles + [pl.BlockSpec(memory_space=pl.ANY)] * len(before),
            out_specs=[col, col, row],
        ),
        out_shape=[jax.ShapeDtypeStruct(s, F32) for s in shapes],
        input_output_aliases={1 + len(tiles) + k: k for k in range(len(before))},
        compiler_params=pltpu.CompilerParams(vmem_limit_bytes=40 * MIB),
        name="place",
    )(where, *operands, *before)


def on_device(
    tokens,
    routes,
    pic_block,
    norm1_gain,
    w_query,
    w_key,
    w_value,
    w_out,
    norm2_gain,
    router,
    expert_gate,
    expert_up,
    expert_down,
    shared_gate,
    shared_up,
    shared_down,
    cotangent,
):
    reps = lax.axis_size("rep")
    shards = lax.axis_size("shard")
    rep = lax.axis_index("rep")
    shard = lax.axis_index("shard")
    core = rep % 2
    quarter = (rep // 2) % 4
    length = tokens.shape[0]
    half = D // 2
    experts = router.shape[1]
    per_core = experts // 2

    def swap(value, rep_bit, shard_bit):
        perm = [
            (r * shards + s, (r ^ rep_bit) * shards + (s ^ shard_bit))
            for r in range(reps)
            for s in range(shards)
        ]
        return lax.ppermute(value, ALL, perm)

    def over_core(value):
        return swap(value, 1, 0)

    def over_x(value):
        return swap(value, 0, 1)

    def over_y(value):
        return swap(value, 2, 0)

    def over_z(value, bits):
        return swap(value, 4 * bits, 0)

    def in_order(index, mine, theirs, axis):
        return jnp.where(
            index == 0,
            jnp.concatenate([mine, theirs], axis=axis),
            jnp.concatenate([theirs, mine], axis=axis),
        )

    def later(value, after):
        return lax.optimization_barrier((value, after))[0]

    held = [None]

    def in_turn(call, *args, need=()):
        if held[0] is not None or need:
            args, _, _ = lax.optimization_barrier((args, held[0], need))
        result = call(*args)
        held[0] = result[0] if isinstance(result, (list, tuple)) else result
        return result

    def where_of(expert):
        return jnp.stack(
            [shard, core, expert, (quarter ^ (quarter // 2)) % 2, quarter % 2, (rep // 4) % 4]
        ).astype(jnp.int32)

    where = where_of(core * per_core)

    rows_c = functools.partial(lax.dynamic_slice_in_dim, start_index=core * (half // 2), slice_size=half // 2, axis=0)
    tiny = jnp.concatenate([norm1_gain[None], norm2_gain[None], router.T], axis=0)
    tiny = jnp.pad(tiny, ((0, 8 - tiny.shape[0]), (0, 0)))
    tiny_got = over_x(tiny)
    small_mine = over_x(later(jnp.stack([rows_c(w_query), rows_c(w_key), rows_c(w_value)]), tiny_got))
    tiny_full = in_order(shard, tiny, tiny_got, 1)
    gain_one = tiny_full[0:1].astype(F32)
    gain_two = tiny_full[1:2].astype(F32)
    router_t = tiny_full[2 : 2 + experts]
    router_t8 = jnp.pad(router_t, ((0, 8 - experts), (0, 0)))
    router_t128 = jnp.pad(router_t, ((0, 128 - experts), (0, 0)))

    experts_w = (expert_gate, expert_up, expert_down)
    shared_w = (shared_gate, shared_up, shared_down)

    def fetch(weights, units, per, expert, cost=CHEAP, need=()):
        call = functools.partial(pack, units=units, per=per, cost=cost)
        return [over_x(v) for v in in_turn(call, where_of(expert), *weights, need=need)]

    def slot_tables(picks):
        expert_ids = jnp.arange(8)[:, None, None]
        picked = jnp.any(picks.T[None] == expert_ids, axis=1)
        earlier = jnp.arange(length)[:, None] < jnp.arange(length)[None, :]
        rank = jnp.dot(picked.astype(BF), earlier.astype(BF), preferred_element_type=F32)
        return jnp.where(picked, rank.astype(jnp.int32), -1)

    routes_oth = over_core(routes)
    slots = jnp.stack([slot_tables(routes), slot_tables(routes_oth)])
    dys = (cotangent, over_core(cotangent))
    tables = rotary_tables(length)
    routes_t = jnp.pad(routes.T, ((0, 6), (0, 0)))

    out_mine = over_x(rows_c(w_out))
    first_w = fetch(experts_w, ((0, 0), (1, 0)), 2, core * per_core)
    small_theirs = over_core(later(small_mine, held[0]))
    out_theirs = over_core(out_mine)
    q, k, v, mixed, lse, wqkv = in_turn(
        attend_forward, where, pic_block, tokens, gain_one, (w_query, w_key, w_value), small_mine, small_theirs, tables,
        need=(out_mine,),
    )
    first_w = [later(v, q) for v in first_w]
    first_w = (first_w[0], over_y(first_w[0]), first_w[1], over_z(first_w[1], 1))
    second_w = fetch(experts_w, ((0, 0), (1, 0)), 2, core * per_core + 1)
    resid, n2, n2p, comb, wout = in_turn(
        middle, where, tokens, mixed, w_out, out_mine, out_theirs, gain_two, router_t8, routes_t,
    )
    toks = (n2p, over_core(n2p))
    shared_fetched = fetch(
        shared_w, ((0, 0), (0, 1)), 1, core * per_core, DEAR, (first_w[1], first_w[3], second_w[0])
    )
    second_w = (second_w[0], over_y(second_w[0]), second_w[1])
    combs = jnp.stack([comb, over_core(comb)])

    near = [[h * 16 + r for r in range(16)] for h in range(reps // 16)]
    distant = [[h * 16 + g for h in range(reps // 16)] for g in range(16)]

    def distant_sum(piece):
        if reps > 16:
            flat = piece.reshape(-1, piece.shape[-1])
            flat = lax.psum_scatter(flat, "rep", scatter_dimension=0, tiled=True, axis_index_groups=distant)
            flat = lax.all_gather(flat, "rep", axis=0, tiled=True, axis_index_groups=distant)
            piece = flat.reshape(piece.shape)
        return piece

    def finish(piece):
        return lax.all_gather(distant_sum(piece), "rep", axis=0, tiled=False, axis_index_groups=near)

    def first(pair, cost=CHEAP):
        pair["sums"] = in_turn(functools.partial(pair_first, cost=cost), where, pair["keep"], pair["got"], pair["hold"], pair["got_y"])
        pair["got"] = (over_y(pair["sums"][0]), over_x(pair["sums"][2]))

    def second(pair, cost=CHEAP):
        call = functools.partial(pair_second, cost=cost)
        pair["sums"] = in_turn(call, where, pair["sums"][1], pair["got"][0], pair["sums"][3], pair["got"][1])
        pair["got"] = [pair["sums"][0]] + [over_z(pair["sums"][n], n) for n in range(1, 4)]

    def third(pair, cost=CHEAP):
        pair["piece"] = in_turn(functools.partial(pair_third, cost=cost), where, pair["got"])

    def new_pair(keep, send, hold, push):
        return {"keep": keep, "got": over_x(send), "hold": hold, "got_y": over_y(push)}

    def routing(j):
        expert = core * per_core + j
        slot_row = lax.dynamic_index_in_dim(slots, expert, 1, keepdims=False)
        gate_row = lax.dynamic_index_in_dim(combs, expert, 1, keepdims=False)
        return where_of(expert), (slot_row, slot_row.reshape(-1, 1), gate_row)

    def after_held(values):
        return [later(v, held[0]) for v in values]

    def add_pair(a, b):
        return ((a.astype(F32) + b.astype(F32)).astype(BF),)

    place_a, route_a = routing(0)
    place_b, route_b = routing(1)
    res_a = in_turn(functools.partial(ffn, route=route_a), place_a, toks, dys, *experts_w, first_w)
    pair_a = new_pair(*res_a[3:])
    second_w += (over_z(later(second_w[2], res_a[0]), 1),)
    res_b = in_turn(
        functools.partial(ffn, route=route_b, only=0), place_b, toks, dys, *experts_w, second_w[:2],
        need=tuple(shared_fetched),
    )
    first(pair_a)
    from_early = over_core(in_turn(add_pair, res_a[1], res_b[1])[0])
    pair_b = new_pair(*after_held(res_b[3:]))
    res_c = in_turn(functools.partial(ffn, route=route_b, only=1), place_b, toks, dys, *experts_w, second_w[2:])
    sums = pair_a["sums"]
    scattered = in_turn(pair_scatter, where, sums[1], pair_a["got"][0], sums[3], pair_a["got"][1])
    z_groups = [[h * 16 + z * 4 + g for z in range(4)] for h in range(reps // 16) for g in range(4)]
    piece_a = lax.psum_scatter(scattered, "rep", scatter_dimension=0, tiled=False, axis_index_groups=z_groups)
    gathered = finish(piece_a)
    first(pair_b)
    pair_c = new_pair(*after_held(res_c[3:]))
    res_s = in_turn(functools.partial(ffn, before=res_c[1]), where, toks, dys, *shared_w, shared_fetched)
    parts = [res_a[0], res_b[0], res_c[0], res_s[0], from_early, over_core(res_s[1])]
    dgates = jnp.stack([res_a[2], res_b[2] + res_c[2]])
    dgates_oth = over_core(dgates[:, 1])
    first(pair_c, DEAR)
    dgate = in_order(core, dgates[:, 0], dgates_oth, 0)
    comb_e = comb[:experts]
    dlog_t = (comb_e * (dgate - jnp.sum(comb_e * dgate, axis=0, keepdims=True))).astype(BF)
    dlog = jnp.pad(dlog_t.T, ((0, 0), (0, 128 - experts)))
    output, d_resid, d_low, ggain_two = in_turn(
        join, where, cotangent, resid, gain_two, dlog, router_t128, parts
    )
    grad_router = jnp.dot(dlog_t, n2, preferred_element_type=F32)
    second(pair_b)
    first_keep, first_send, gout_low, d_normed = in_turn(
        attend_backward, where, pic_block, tokens, gain_one, wqkv, wout, tables, q, k, v, mixed, lse, d_low
    )
    third(pair_b)
    second(pair_c)
    pair_s = new_pair(*after_held(res_s[2:]))
    last_keep, last_send, gout_high, input_grad, ggain_one = in_turn(
        attend_backward,
        where, pic_block, tokens, gain_one, wqkv, wout, tables, q, k, v, mixed, lse, d_low, (d_resid, d_normed),
    )

    for_other, for_me = in_turn(
        attention_pack, where, first_keep, first_send, last_keep, last_send, gout_low, gout_high,
        ggain_one, ggain_two, grad_router,
    )
    att_got = over_core(for_other)
    shared_shapes = [shared_gate.shape, shared_up.shape, shared_down.shape]
    expert_shapes = [expert_gate.shape, expert_up.shape, expert_down.shape]
    third(pair_c)
    piece_b = jnp.stack([pair_b["piece"], pair_c["piece"]])
    gathered_b = finish(piece_b.reshape((2, 6) + piece_b.shape[3:]))
    first(pair_s, DEAR)
    att_keep, att_send = in_turn(attention_sum, where, for_me, att_got)
    x_got = over_x(att_send)
    expert_grads = in_turn(lambda f: place(where, 0, f, expert_shapes, None, HUGE), gathered)
    second(pair_s, FAIR)
    y_send, y_keep = in_turn(sum_x, where, att_keep, x_got)
    y_got = over_y(y_send)
    third(pair_s, FAIR)
    shared_full = finish(pair_s["piece"])
    quarter_rows = in_turn(functools.partial(sum_y, cost=FAIR), where, y_keep, y_got)
    quarter_rows = [quarter_rows[0]] + [over_z(quarter_rows[n], n) for n in range(1, 4)]
    piece = distant_sum(in_turn(functools.partial(sum_z, cost=FAIR), where, quarter_rows))
    att = [piece] + [over_z(piece, n) for n in range(1, 4)]
    att = att + [over_y(p) for p in att]
    expert_grads = in_turn(
        lambda f, *old: place(where, 1, f, expert_shapes, old, HUGE), gathered_b, *expert_grads
    )
    att = in_turn(assemble, where, att)
    att_oth = over_core(att)
    gq, gk, gv, gout, small_grads = in_turn(attention_unpack, where, att, att_oth)
    shared_grads = in_turn(
        lambda f: place(where, None, f, shared_shapes, None),
        shared_full.reshape((16, 1, 6) + shared_full.shape[3:]),
    )
    return (
        output,
        input_grad,
        small_grads[:, 0],
        gq,
        gk,
        gv,
        gout,
        small_grads[:, 1],
        small_grads[:, 2 : 2 + experts],
        *expert_grads,
        *shared_grads,
    )


def solution(mesh):
    both = P(("rep", "shard"), None)
    rows = P("shard", None)
    vec = P("shard")
    mid = P(None, "shard", None)
    return jax.shard_map(
        on_device,
        mesh=mesh,
        in_specs=(
            both, both, P(("rep", "shard")),
            vec, rows, rows, rows, rows, vec, rows, mid, mid, mid, rows, rows, rows,
            both,
        ),
        out_specs=(both, both, vec, rows, rows, rows, rows, vec, rows, mid, mid, mid, rows, rows, rows),
        check_vma=False,
    )
```
